32 devices in a mesh: dp: 4 (over y, x), ctx: 8 (over z, core).
Axes of the slice: x: 2, y: 2, z: 4, core: 2. Of those that a mesh axis runs over, the one named last changes fastest.
Arguments:
- inputs: bfloat16 [4, 16, 128, 2048], P('dp', 'ctx'), may hold values from -6 to 6
- block_of: int32 [4, 16], P('dp', 'ctx'), may hold values from 0 to 15, as said below
- first_gain: float32 [2048], P('dp'), may hold values from 0.5 to 1.5
- first_shift: float32 [2048], P('dp'), may hold values from -3 to 3
- w_qkv: bfloat16 [2048, 6144], P('dp'), may hold values from -8 to 8
- qkv_bias: float32 [6144], P('dp'), may hold values from -3 to 3
- w_out: bfloat16 [2048, 2048], P('dp'), may hold values from -0.75 to 0.75
- second_gain: float32 [2048], P('dp'), may hold values from 0.5 to 1.5
- second_shift: float32 [2048], P('dp'), may hold values from -3 to 3
- w_gateup: bfloat16 [2048, 11264], P('dp'), may hold values from -0.125 to 0.125
- w_down: bfloat16 [5632, 2048], P('dp'), may hold values from -0.078125 to 0.078125
- cotangent: bfloat16 [4, 16, 128, 2048], P('dp', 'ctx'), may hold values from -6 to 6
Outputs:
- outputs: bfloat16 [4, 16, 128, 2048], P('dp', 'ctx')
- grad_inputs: float32 [4, 16, 128, 2048], P('dp', 'ctx')
- grad_first_gain: float32 [2048], P('dp')
- grad_first_shift: float32 [2048], P('dp')
- grad_w_qkv: float32 [2048, 6144], P('dp')
- grad_qkv_bias: float32 [6144], P('dp')
- grad_w_out: float32 [2048, 2048], P('dp')
- grad_second_gain: float32 [2048], P('dp')
- grad_second_shift: float32 [2048], P('dp')
- grad_w_gateup: float32 [2048, 11264], P('dp')
- grad_w_down: float32 [5632, 2048], P('dp')
The draws below stay inside these ranges and needn't reach their ends.
Inputs may be any that keep to these rules, and one draw needn't show every extreme that they name: `block_of`: for each sequence the 16 entries are a permutation of the blocks, and the two slots of one index of ctx hold blocks b and 15 - b, in either order.
All inputs are finite; a program needn't handle non-finite values.
Results may differ from the reference program's by a relative error of at most 0.035.
Values may be sent and summed in bfloat16 or wider, within the bound.
A program may use at most 640 MiB of HBM per device.

```python
import jax
import jax.numpy as jnp
from jax import lax

D = 2048
HEADS = 32
HEAD_DIM = 64
ROT = 16
FF = 5632
BLK = 128
BLOCKS = 16
SEQS = 4


def draw_block_of(key, part):
    pair_count = BLOCKS // 2
    seq_keys = jax.random.split(key, SEQS)

    def draw_sequence(seq_key):
        order_key, flip_key = jax.random.split(seq_key)
        pair_order = jax.random.permutation(order_key, pair_count)
        flip_bits = jax.random.randint(flip_key, (pair_count,), 0, 2)
        low_block = jnp.where(flip_bits == 1, BLOCKS - 1 - pair_order, pair_order)
        high_block = BLOCKS - 1 - low_block
        return jnp.stack([low_block, high_block], axis=1).reshape(BLOCKS)
    return jax.vmap(draw_sequence)(seq_keys).astype(jnp.int32)


def draw_w_qkv(key, part):
    query_key, keys_key, values_key = jax.random.split(key, 3)
    spread_std = D ** (-0.5)
    w_query = jnp.clip(jax.random.normal(query_key, (D, D), jnp.float32), -6.0, 6.0) * spread_std
    w_keys = jnp.clip(jax.random.normal(keys_key, (D, D), jnp.float32), -6.0, 6.0) * spread_std
    w_values = jnp.clip(jax.random.normal(values_key, (D, D), jnp.float32), -6.0, 6.0) * spread_std
    return jnp.clip(jnp.concatenate([w_query, w_keys, w_values], axis=1), -8.0, 8.0).astype(jnp.bfloat16)


def level_of(own_key, shape, cuts, low, largest):
    gain = 1.0
    for axis_at, blocks in cuts:
        heights = jax.random.uniform(jax.random.fold_in(jax.random.fold_in(own_key, 6), axis_at), (blocks,), jnp.float32, low / len(cuts), largest / len(cuts))
        gain = gain * jnp.repeat(jnp.exp(heights), shape[axis_at] // blocks).reshape((-1,) + (1,) * (len(shape) - 1 - axis_at))
    return gain


def scatter_about(stream_key, dims, scale, reach, shards=(), kind=jnp.bfloat16):
    level = level_of(stream_key, dims, shards, -0.22, 0.18) if shards else 1.0
    array = jax.random.normal(stream_key, dims, jnp.float32) * scale * level
    return jnp.minimum(jnp.maximum(array, -reach), reach).astype(kind)


def setup_inputs(seed: int = 0) -> dict:
    key_of = jax.random.split(jax.random.key(seed), 13)
    return {
        "inputs": scatter_about(key_of[0], (SEQS, BLOCKS, BLK, D), 1.0, 6.0, ((0, 4), (1, 8))),
        "block_of": draw_block_of(jax.random.fold_in(key_of[12], 71), 0),
        "first_gain": jnp.clip(1.0 + 0.1 * jax.random.normal(key_of[2], (D,), jnp.float32), 0.5, 1.5),
        "first_shift": scatter_about(key_of[3], (D,), 0.3, 3.0, ((0, 4),), jnp.float32),
        "w_qkv": draw_w_qkv(jax.random.fold_in(key_of[12], 71), 0),
        "qkv_bias": scatter_about(key_of[5], (3 * D,), 0.5, 3.0, ((0, 4),), jnp.float32),
        "w_out": scatter_about(key_of[6], (D, D), 64 ** -0.5, 0.75, ((0, 4),)),
        "second_gain": jnp.clip(1.0 + 0.1 * jax.random.normal(key_of[7], (D,), jnp.float32), 0.5, 1.5),
        "second_shift": scatter_about(key_of[8], (D,), 0.3, 3.0, ((0, 4),), jnp.float32),
        "w_gateup": scatter_about(key_of[9], (D, 2 * FF), D ** -0.5, 0.125, ((0, 4),)),
        "w_down": scatter_about(key_of[10], (FF, D), FF ** -0.5, 0.078125, ((0, 4),)),
        "cotangent": scatter_about(key_of[11], (SEQS, BLOCKS, BLK, D), 1.0, 6.0, ((0, 4), (1, 8))),
    }


epsilon = 1e-05

def layer_norm(token_rows, gain_vec, shift_vec):
    centre = lax.optimization_barrier(jnp.mean(token_rows, axis=-1, keepdims=True))
    centred = token_rows - centre
    spread = lax.optimization_barrier(jnp.mean(centred * centred, axis=-1, keepdims=True))
    inverse = lax.rsqrt(spread + epsilon)
    normed = centred * inverse
    return (normed * gain_vec + shift_vec, normed, inverse)

def norm_back(grad_rows, normed, inverse, gain_vec):
    scaled = grad_rows * gain_vec
    mean_plain = lax.optimization_barrier(jnp.mean(scaled, axis=-1, keepdims=True))
    mean_cross = lax.optimization_barrier(jnp.mean(scaled * normed, axis=-1, keepdims=True))
    return inverse * (scaled - mean_plain - normed * mean_cross)

def rotary_tables(positions):
    half_rot = ROT // 2
    frequency = 10000.0 ** (-2.0 * jnp.arange(half_rot, dtype=jnp.float32) / ROT)
    angles = positions.astype(jnp.float32)[:, None] * frequency[None, :]
    return (jnp.cos(angles), jnp.sin(angles))

def rotate_heads(head_rows, cosine, sine_part, direction_sign):
    half_rot = ROT // 2
    first_half = head_rows[..., :half_rot]
    second_half = head_rows[..., half_rot:ROT]
    cos_rows = cosine[:, None, :]
    sin_rows = sine_part[:, None, :] * direction_sign
    return jnp.concatenate([first_half * cos_rows - second_half * sin_rows, second_half * cos_rows + first_half * sin_rows, head_rows[..., ROT:]], axis=-1)

def attend(query, keys_all, values_all, query_pos, key_pos):
    tok_count, head_count, head_width = query.shape
    per_group = min(4, head_count)
    score_scale = head_width ** (-0.5)
    allowed = key_pos[None, :] <= query_pos[:, None]
    highest = lax.Precision.HIGHEST

    def group_step(group_index, carry):
        output_all, lse_all = carry
        first_head = jnp.asarray(group_index).astype(jnp.int32) * per_group
        query_part = lax.dynamic_slice_in_dim(query, first_head, per_group, 1).astype(jnp.float32)
        keys_part = lax.dynamic_slice_in_dim(keys_all, first_head, per_group, 1).astype(jnp.float32)
        values_part = lax.dynamic_slice_in_dim(values_all, first_head, per_group, 1).astype(jnp.float32)
        scores = jnp.einsum('thd,shd->hts', query_part, keys_part, precision=highest) * score_scale
        scores = jnp.where(allowed[None], scores, -jnp.inf)
        row_max = lax.optimization_barrier(jnp.max(scores, axis=-1, keepdims=True))
        log_total = row_max + jnp.log(lax.optimization_barrier(jnp.sum(jnp.exp(scores - row_max), axis=-1, keepdims=True)))
        weights = jnp.exp(scores - log_total).astype(jnp.bfloat16)
        mixed = jnp.einsum('hts,shd->thd', weights.astype(jnp.float32), values_part, precision=highest).astype(jnp.bfloat16)
        output_all = lax.dynamic_update_slice_in_dim(output_all, mixed, first_head, 1)
        lse_all = lax.dynamic_update_slice_in_dim(lse_all, log_total[..., 0], first_head, 0)
        return (output_all, lse_all)
    init = (jnp.zeros(query.shape, jnp.bfloat16), jnp.zeros((head_count, tok_count), jnp.float32))
    return lax.fori_loop(0, head_count // per_group, group_step, init)

def attend_back(query, keys_all, values_all, output, grad_output, lse_all, query_pos, key_pos):
    tok_count, head_count, head_width = query.shape
    per_group = min(4, head_count)
    score_scale = head_width ** (-0.5)
    allowed = key_pos[None, :] <= query_pos[:, None]
    highest = lax.Precision.HIGHEST
    delta_all = jnp.einsum('thd,thd->ht', output.astype(jnp.float32), grad_output.astype(jnp.float32), precision=highest)

    def group_step(group_index, carry):
        grad_q_all, grad_k_all, grad_v_all = carry
        first_head = jnp.asarray(group_index).astype(jnp.int32) * per_group
        query_part = lax.dynamic_slice_in_dim(query, first_head, per_group, 1).astype(jnp.float32)
        keys_part = lax.dynamic_slice_in_dim(keys_all, first_head, per_group, 1).astype(jnp.float32)
        values_part = lax.dynamic_slice_in_dim(values_all, first_head, per_group, 1).astype(jnp.float32)
        dout_part = lax.dynamic_slice_in_dim(grad_output, first_head, per_group, 1).astype(jnp.float32)
        lse_part = lax.dynamic_slice_in_dim(lse_all, first_head, per_group, 0)
        delta_part = lax.dynamic_slice_in_dim(delta_all, first_head, per_group, 0)
        scores = jnp.einsum('thd,shd->hts', query_part, keys_part, precision=highest) * score_scale
        scores = jnp.where(allowed[None], scores, -jnp.inf)
        probs = jnp.exp(scores - lse_part[..., None])
        probs_low = probs.astype(jnp.bfloat16).astype(jnp.float32)
        grad_v_part = jnp.einsum('hts,thd->shd', probs_low, dout_part, precision=highest)
        grad_p = jnp.einsum('thd,shd->hts', dout_part, values_part, precision=highest)
        grad_s = (probs * (grad_p - delta_part[..., None])).astype(jnp.bfloat16).astype(jnp.float32)
        grad_q_part = jnp.einsum('hts,shd->thd', grad_s, keys_part, precision=highest) * score_scale
        grad_k_part = jnp.einsum('hts,thd->shd', grad_s, query_part, precision=highest) * score_scale
        grad_q_all = lax.dynamic_update_slice_in_dim(grad_q_all, grad_q_part, first_head, 1)
        grad_k_all = lax.dynamic_update_slice_in_dim(grad_k_all, grad_k_part, first_head, 1)
        grad_v_all = lax.dynamic_update_slice_in_dim(grad_v_all, grad_v_part, first_head, 1)
        return (grad_q_all, grad_k_all, grad_v_all)
    init = (jnp.zeros(query.shape, jnp.float32), jnp.zeros(keys_all.shape, jnp.float32), jnp.zeros(values_all.shape, jnp.float32))
    return lax.fori_loop(0, head_count // per_group, group_step, init)

def one_sequence(seq_inputs, seq_blocks, seq_cot, params):
    first_gain, first_shift, w_qkv, qkv_bias, w_out, second_gain, second_shift, w_gateup, w_down = params
    token_rows = seq_inputs.reshape(-1, D).astype(jnp.float32)
    count_rows = token_rows.shape[0]
    positions = (seq_blocks[:, None] * BLK + jnp.arange(BLK, dtype=jnp.int32)[None, :]).reshape(-1).astype(jnp.int32)
    cosine, sine_part = rotary_tables(positions)
    head_shape = (count_rows, HEADS, HEAD_DIM)
    normed_out, normed_one, inverse_one = layer_norm(token_rows, first_gain, first_shift)
    hidden_one = normed_out.astype(jnp.bfloat16)
    projected = jnp.dot(hidden_one, w_qkv, preferred_element_type=jnp.float32) + qkv_bias
    query = rotate_heads(projected[:, :D].reshape(head_shape), cosine, sine_part, 1.0).astype(jnp.bfloat16)
    keys_rot = rotate_heads(projected[:, D:2 * D].reshape(head_shape), cosine, sine_part, 1.0).astype(jnp.bfloat16)
    values_heads = projected[:, 2 * D:].reshape(head_shape).astype(jnp.bfloat16)
    attended, log_totals = attend(query, keys_rot, values_heads, positions, positions)
    attended_flat = attended.reshape(count_rows, D)
    middle = token_rows + jnp.dot(attended_flat, w_out, preferred_element_type=jnp.float32)
    normed_out_two, normed_two, inverse_two = layer_norm(middle, second_gain, second_shift)
    hidden_two = normed_out_two.astype(jnp.bfloat16)
    gate_up = jnp.dot(hidden_two, w_gateup, preferred_element_type=jnp.float32)
    gate_part = gate_up[:, :FF]
    up_part = gate_up[:, FF:]
    sigmoid_gate = jax.nn.sigmoid(gate_part)
    activation = (gate_part * sigmoid_gate * up_part).astype(jnp.bfloat16)
    result = middle + jnp.dot(activation, w_down, preferred_element_type=jnp.float32)
    seq_out = result.astype(jnp.bfloat16).reshape(seq_inputs.shape)
    grad_rows = seq_cot.reshape(count_rows, D)
    grad_down = jnp.dot(activation.T, grad_rows, preferred_element_type=jnp.float32)
    grad_act = jnp.dot(grad_rows, w_down.T, preferred_element_type=jnp.float32)
    grad_gate = grad_act * up_part * sigmoid_gate * (1.0 + gate_part * (1.0 - sigmoid_gate))
    grad_up = grad_act * gate_part * sigmoid_gate
    grad_gu = jnp.concatenate([grad_gate, grad_up], axis=1).astype(jnp.bfloat16)
    grad_gateup = jnp.dot(hidden_two.T, grad_gu, preferred_element_type=jnp.float32)
    grad_hidden_two = jnp.dot(grad_gu, w_gateup.T, preferred_element_type=jnp.float32)
    grad_gain_two = lax.optimization_barrier(jnp.sum(grad_hidden_two * normed_two, axis=0))
    grad_shift_two = lax.optimization_barrier(jnp.sum(grad_hidden_two, axis=0))
    grad_middle = grad_rows.astype(jnp.float32) + norm_back(grad_hidden_two, normed_two, inverse_two, second_gain)
    grad_middle_low = grad_middle.astype(jnp.bfloat16)
    grad_wout = jnp.dot(attended_flat.T, grad_middle_low, preferred_element_type=jnp.float32)
    grad_attended = jnp.dot(grad_middle_low, w_out.T, preferred_element_type=jnp.float32).astype(jnp.bfloat16)
    grad_query, grad_keys, grad_values = attend_back(query, keys_rot, values_heads, attended, grad_attended.reshape(head_shape), log_totals, positions, positions)
    grad_query_plain = rotate_heads(grad_query, cosine, sine_part, -1.0).reshape(count_rows, D)
    grad_keys_plain = rotate_heads(grad_keys, cosine, sine_part, -1.0).reshape(count_rows, D)
    grad_proj = jnp.concatenate([grad_query_plain, grad_keys_plain, grad_values.reshape(count_rows, D)], axis=1)
    grad_bias = lax.optimization_barrier(jnp.sum(grad_proj, axis=0))
    grad_proj_low = grad_proj.astype(jnp.bfloat16)
    grad_wqkv = jnp.dot(hidden_one.T, grad_proj_low, preferred_element_type=jnp.float32)
    grad_hidden_one = jnp.dot(grad_proj_low, w_qkv.T, preferred_element_type=jnp.float32)
    grad_gain_one = lax.optimization_barrier(jnp.sum(grad_hidden_one * normed_one, axis=0))
    grad_shift_one = lax.optimization_barrier(jnp.sum(grad_hidden_one, axis=0))
    grad_in = grad_middle + norm_back(grad_hidden_one, normed_one, inverse_one, first_gain)
    grads = (grad_gain_one, grad_shift_one, grad_wqkv, grad_bias, grad_wout, grad_gain_two, grad_shift_two, grad_gateup, grad_down)
    return (seq_out, grad_in.reshape(seq_inputs.shape), grads)

def reference(inputs, block_of, first_gain, first_shift, w_qkv, qkv_bias, w_out, second_gain, second_shift, w_gateup, w_down, cotangent):
    params = (first_gain, first_shift, w_qkv, qkv_bias, w_out, second_gain, second_shift, w_gateup, w_down)
    shapes = ((D,), (D,), (D, 3 * D), (3 * D,), (D, D), (D,), (D,), (D, 2 * FF), (FF, D))
    zero_grads = tuple((jnp.zeros(shape_now, jnp.float32) for shape_now in shapes))

    def seq_step(carry, slices):
        seq_inputs, seq_blocks, seq_cot = slices
        seq_out, seq_grad, grads = one_sequence(seq_inputs, seq_blocks, seq_cot, params)
        totals = jax.tree.map(lambda total_now, extra_now: total_now + extra_now, carry, grads)
        return (totals, (seq_out, seq_grad))
    totals, (outputs, grad_inputs) = lax.scan(seq_step, zero_grads, (inputs, block_of, cotangent))
    return (outputs, grad_inputs, totals[0], totals[1], totals[2], totals[3], totals[4], totals[5], totals[6], totals[7], totals[8])
```

```python
import functools

import jax
import jax.numpy as jnp
from jax import lax
from jax.experimental import pallas as pl
from jax.experimental.pallas import tpu as pltpu
from jax.sharding import Mesh
from jax.sharding import PartitionSpec as P

HEADS = 32
HEAD_DIM = 64
ROT = 16
PAIR = 2 * HEAD_DIM
SCALE = HEAD_DIM ** (-0.5)
epsilon = 1e-05
F32 = jnp.float32
BF16 = jnp.bfloat16
PLANE = ("dp", "core")
EVERY = ("dp", "pl", "core")


def layer_norm(token_rows, gain_vec, shift_vec):
    centre = jnp.mean(token_rows, axis=-1, keepdims=True)
    centred = token_rows - centre
    spread = jnp.mean(centred * centred, axis=-1, keepdims=True)
    inverse = lax.rsqrt(spread + epsilon)
    normed = centred * inverse
    return (normed * gain_vec + shift_vec, normed, inverse)


def norm_back(grad_rows, normed, inverse, gain_vec):
    scaled = grad_rows * gain_vec
    mean_plain = jnp.mean(scaled, axis=-1, keepdims=True)
    mean_cross = jnp.mean(scaled * normed, axis=-1, keepdims=True)
    return inverse * (scaled - mean_plain - normed * mean_cross)


def rotary_tables(length):
    half = ROT // 2
    lane = jnp.arange(PAIR, dtype=jnp.int32) % HEAD_DIM
    frequency = 10000.0 ** (-2.0 * (lane % half).astype(F32) / ROT)
    angles = jnp.arange(length, dtype=F32)[:, None] * frequency[None, :]
    cosine, sine = jnp.cos(angles), jnp.sin(angles)
    cos_t = jnp.where(lane < ROT, cosine, 1.0)
    low_t = jnp.where(lane < half, -sine, 0.0)
    high_t = jnp.where((lane >= half) & (lane < ROT), sine, 0.0)
    return cos_t, low_t, high_t


def head_mask(shape, head):
    lane = lax.broadcasted_iota(jnp.int32, shape, 1)
    return (lane < HEAD_DIM) if head == 0 else (lane >= HEAD_DIM)


def roll_pair(x, shift):
    return pltpu.roll(x, shift % PAIR, 1)


def nt(a, b):
    return lax.dot_general(a, b, (((1,), (1,)), ((), ())), preferred_element_type=F32)


def nn(a, b):
    return lax.dot_general(a, b, (((1,), (0,)), ((), ())), preferred_element_type=F32)


def tn(a, b):
    return lax.dot_general(a, b, (((0,), (0,)), ((), ())), preferred_element_type=F32)


def attend_kernel(
    blk, tile, slot_ref, pq, pk, pv, bq, bk, bv, cos_t, low_t, high_t, qs, ks, vs, att, lse, acc, top, osc
):
    length = pq.shape[0]

    def sort_block(b, carry):
        src = pl.ds(pl.multiple_of(slot_ref[b] * blk, blk), blk)
        dst = pl.ds(pl.multiple_of(b * blk, blk), blk)
        c, lo, hi = cos_t[dst, :], low_t[dst, :], high_t[dst, :]
        q = pq[src, :] + bq[...]
        k = pk[src, :] + bk[...]
        q = q * c + roll_pair(q, -(ROT // 2)) * lo + roll_pair(q, ROT // 2) * hi
        k = k * c + roll_pair(k, -(ROT // 2)) * lo + roll_pair(k, ROT // 2) * hi
        qs[dst, :] = q.astype(BF16)
        ks[dst, :] = k.astype(BF16)
        vs[dst, :] = (pv[src, :] + bv[...]).astype(BF16)
        return carry

    lax.fori_loop(0, length // blk, sort_block, 0)
    rows = lax.broadcasted_iota(jnp.int32, (tile, tile), 0)
    cols = lax.broadcasted_iota(jnp.int32, (tile, tile), 1)
    masks = [head_mask((tile, PAIR), h) for h in range(2)]

    def q_step(qi, carry):
        q_at = pl.ds(pl.multiple_of(qi * tile, tile), tile)
        q = qs[q_at, :]
        acc[...] = jnp.zeros_like(acc)
        top[...] = jnp.full(top.shape, -1e30, F32)

        def one(kj, diagonal):
            k_at = pl.ds(pl.multiple_of(kj * tile, tile), tile)
            k, v = ks[k_at, :], vs[k_at, :]
            for h in range(2):
                qm = jnp.where(masks[h], q, 0).astype(BF16)
                s = nt(qm, k) * SCALE
                if diagonal:
                    s = jnp.where(cols <= rows, s, -jnp.inf)
                old = top[h]
                new = jnp.maximum(old, jnp.max(s, axis=1, keepdims=True))
                p = jnp.exp(s - new[:, :1]).astype(BF16)
                ve = jnp.where(masks[h], v, 1).astype(BF16)
                acc[h] = acc[h] * jnp.exp(old - new) + nn(p, ve)
                top[h] = new

        def k_step(kj, c):
            one(kj, False)
            return c

        lax.fori_loop(0, qi, k_step, 0)
        one(qi, True)
        a0, a1 = acc[0], acc[1]
        sum0 = roll_pair(a0, HEAD_DIM)
        sum1 = roll_pair(a1, HEAD_DIM)
        total = jnp.where(masks[0], sum0, sum1)
        mixed = jnp.where(masks[0], a0, a1) / total
        osc[q_at, :] = mixed.astype(BF16)
        lse[q_at, :] = jnp.where(masks[0], top[0], top[1]) + jnp.log(total)
        return carry

    lax.fori_loop(0, length // tile, q_step, 0)

    def place_block(b, carry):
        dst = pl.ds(pl.multiple_of(slot_ref[b] * blk, blk), blk)
        att[dst, :] = osc[pl.ds(pl.multiple_of(b * blk, blk), blk), :]
        return carry

    lax.fori_loop(0, length // blk, place_block, 0)


def attend(slot_of, proj, bias, tables, blk):
    length, width = proj.shape
    pairs = width // (3 * PAIR)
    tile = min(512, length)
    whole = lambda f: pl.BlockSpec((length, PAIR), f)
    table = pl.BlockSpec((length, PAIR), lambda p, s: (0, 0), pipeline_mode=pl.Buffered(1))
    in_specs = (
        [whole(lambda p, s, o=o: (0, o * pairs + p)) for o in range(3)]
        + [pl.BlockSpec((1, PAIR), lambda p, s, o=o: (0, o * pairs + p)) for o in range(3)]
        + [table] * 3
    )
    out = jax.ShapeDtypeStruct((length, pairs * PAIR), BF16)
    own = whole(lambda p, s: (0, p))
    return pl.pallas_call(
        functools.partial(attend_kernel, blk, tile),
        out_shape=(out, out, out, out, jax.ShapeDtypeStruct((length, pairs * PAIR), F32)),
        grid_spec=pltpu.PrefetchScalarGridSpec(
            num_scalar_prefetch=1,
            grid=(pairs,),
            in_specs=in_specs,
            out_specs=[own] * 5,
            scratch_shapes=[
                pltpu.VMEM((2, tile, PAIR), F32),
                pltpu.VMEM((2, tile, PAIR), F32),
                pltpu.VMEM((length, PAIR), BF16),
            ],
        ),
        compiler_params=pltpu.CompilerParams(vmem_limit_bytes=56 * 2**20),
        name="attend",
    )(slot_of, proj, proj, proj, bias, bias, bias, *tables)


def attend_back_kernel(
    blk, tile, slot_ref, qs, ks, vs, att, gat, lse, cos_t, low_t, high_t, gq, gk, gv, bias, dos, dlt, dq, dk, dv
):
    length = qs.shape[0]
    bmask = head_mask((blk, PAIR), 0)

    def sort_block(b, carry):
        src = pl.ds(pl.multiple_of(slot_ref[b] * blk, blk), blk)
        dst = pl.ds(pl.multiple_of(b * blk, blk), blk)
        g = gat[src, :]
        dos[dst, :] = g
        prod = g.astype(F32) * att[src, :].astype(F32)
        d0 = jnp.sum(jnp.where(bmask, prod, 0.0), axis=1, keepdims=True)
        d1 = jnp.sum(jnp.where(bmask, 0.0, prod), axis=1, keepdims=True)
        dlt[dst, :] = jnp.where(bmask, d0, d1)
        return carry

    lax.fori_loop(0, length // blk, sort_block, 0)
    dq[...] = jnp.zeros_like(dq)
    rows = lax.broadcasted_iota(jnp.int32, (tile, tile), 0)
    cols = lax.broadcasted_iota(jnp.int32, (tile, tile), 1)
    masks = [head_mask((tile, PAIR), h) for h in range(2)]
    steps = length // tile

    def k_step(kj, carry):
        k_at = pl.ds(pl.multiple_of(kj * tile, tile), tile)
        k, v = ks[k_at, :], vs[k_at, :]
        dk[...] = jnp.zeros_like(dk)
        dv[...] = jnp.zeros_like(dv)

        def one(qi, diagonal):
            q_at = pl.ds(pl.multiple_of(qi * tile, tile), tile)
            q, do = qs[q_at, :], dos[q_at, :]
            ls, dl = lse[q_at, :], dlt[q_at, :]
            for h in range(2):
                at = h * HEAD_DIM
                qm = jnp.where(masks[h], q, 0).astype(BF16)
                dm = jnp.where(masks[h], do, 0).astype(BF16)
                km = jnp.where(masks[h], k, 0).astype(BF16)
                p = jnp.exp(nt(qm, k) * SCALE - ls[:, at : at + 1])
                if diagonal:
                    p = jnp.where(cols <= rows, p, 0.0)
                ds = (p * (nt(dm, v) - dl[:, at : at + 1])).astype(BF16)
                dv[...] += tn(p.astype(BF16), dm)
                dk[...] += tn(ds, qm)
                dq[q_at, :] += nn(ds, km)

        one(kj, True)

        def q_step(qi, c):
            one(qi, False)
            return c

        lax.fori_loop(kj + 1, steps, q_step, 0)
        for part in range(tile // blk):
            b = kj * (tile // blk) + part
            sub = pl.ds(part * blk, blk)
            pos = pl.ds(pl.multiple_of(b * blk, blk), blk)
            dst = pl.ds(pl.multiple_of(slot_ref[b] * blk, blk), blk)
            g = dk[sub, :] * SCALE
            g = g * cos_t[pos, :] - roll_pair(g, -(ROT // 2)) * low_t[pos, :] - roll_pair(g, ROT // 2) * high_t[pos, :]
            gk[dst, :] = g.astype(BF16)
            bias[1:2, :] += jnp.sum(g, axis=0, keepdims=True)
            w = dv[sub, :]
            gv[dst, :] = w.astype(BF16)
            bias[2:3, :] += jnp.sum(w, axis=0, keepdims=True)
        return carry

    bias[...] = jnp.zeros_like(bias)
    lax.fori_loop(0, steps, k_step, 0)

    def place_block(b, carry):
        pos = pl.ds(pl.multiple_of(b * blk, blk), blk)
        dst = pl.ds(pl.multiple_of(slot_ref[b] * blk, blk), blk)
        g = dq[pos, :] * SCALE
        g = g * cos_t[pos, :] - roll_pair(g, -(ROT // 2)) * low_t[pos, :] - roll_pair(g, ROT // 2) * high_t[pos, :]
        gq[dst, :] = g.astype(BF16)
        bias[0:1, :] += jnp.sum(g, axis=0, keepdims=True)
        return carry

    lax.fori_loop(0, length // blk, place_block, 0)


def attend_back(slot_of, qs, ks, vs, att, gat, lse, tables, blk):
    length, width = qs.shape
    pairs = width // PAIR
    tile = min(512, length)
    own = pl.BlockSpec((length, PAIR), lambda p, s: (0, p))
    table = pl.BlockSpec((length, PAIR), lambda p, s: (0, 0), pipeline_mode=pl.Buffered(1))
    out = jax.ShapeDtypeStruct((length, width), BF16)
    return pl.pallas_call(
        functools.partial(attend_back_kernel, blk, tile),
        out_shape=(out, out, out, jax.ShapeDtypeStruct((8, width), F32)),
        grid_spec=pltpu.PrefetchScalarGridSpec(
            num_scalar_prefetch=1,
            grid=(pairs,),
            in_specs=[own] * 6 + [table] * 3,
            out_specs=[own] * 3 + [pl.BlockSpec((8, PAIR), lambda p, s: (0, p))],
            scratch_shapes=[
                pltpu.VMEM((length, PAIR), BF16),
                pltpu.VMEM((length, PAIR), F32),
                pltpu.VMEM((length, PAIR), F32),
                pltpu.VMEM((tile, PAIR), F32),
                pltpu.VMEM((tile, PAIR), F32),
            ],
        ),
        compiler_params=pltpu.CompilerParams(vmem_limit_bytes=56 * 2**20),
        name="attend_back",
    )(slot_of, qs, ks, vs, att, gat, lse, *tables)


def local(
    groups,
    inputs,
    block_of,
    first_gain,
    first_shift,
    w_qkv,
    qkv_bias,
    w_out,
    second_gain,
    second_shift,
    w_gateup,
    w_down,
    cotangent,
):
    n = groups
    blk = inputs.shape[2]
    toks = inputs.shape[1] * blk
    width = inputs.shape[3]
    rows = w_qkv.shape[0]
    me, plane, core = (lax.axis_index(a) for a in EVERY)
    hw = width // (2 * n)
    units = w_down.shape[0] // 2
    swap_pairs = [(s * n + z, z * n + s) for s in range(n) for z in range(n)]
    swap = lambda a: lax.ppermute(a, ("dp", "pl"), swap_pairs)
    gather = lambda a: lax.all_gather(a, PLANE, axis=0, tiled=True)
    scatter = lambda a: lax.psum_scatter(a.astype(BF16), PLANE, scatter_dimension=0, tiled=True).astype(F32)
    pick = lambda a, axis, at: lax.dynamic_index_in_dim(a, at, axis, keepdims=False)

    def columns(w, parts, wide):
        mine = pick(w.reshape(rows, parts, n, 2, wide), 3, core)
        mine = mine.transpose(2, 0, 1, 3).reshape(n * rows, parts * wide)
        return lax.all_to_all(mine, "dp", 0, 0, tiled=True)

    token_rows = swap(inputs.reshape(toks, width)).astype(F32)
    cot = swap(cotangent.reshape(toks, width))
    wq = columns(w_qkv, 3, hw)
    small = jnp.concatenate([first_gain, first_shift, second_gain, second_shift, qkv_bias])
    small = lax.all_gather(small, "dp", axis=0, tiled=False)
    gain_one, shift_one, gain_two, shift_two = (
        small[:, k * rows : (k + 1) * rows].reshape(width) for k in range(4)
    )
    bias = small[:, 4 * rows :].reshape(3, n, 2, hw)
    bias = pick(pick(bias, 1, me), 1, core).reshape(1, 3 * hw)
    blocks = lax.all_gather(block_of.reshape(-1), EVERY, axis=0, tiled=True)
    blocks = pick(blocks.reshape(n, -1), 0, plane)
    order = jnp.arange(blocks.shape[0], dtype=jnp.int32)
    slot_of = jnp.sum(jnp.where(blocks[None, :] == order[:, None], order[None, :], 0), axis=1)
    wgu = columns(w_gateup, 2, units)
    wo = pick(w_out.reshape(2, hw, width), 0, core)
    wd = pick(w_down.reshape(2, units, width), 0, core)
    tables = rotary_tables(blocks.shape[0] * blk)

    normed_out, normed_one, inverse_one = layer_norm(token_rows, gain_one, shift_one)
    hidden_one = gather(normed_out.astype(BF16))
    proj = nn(hidden_one, wq)
    qs, ks, vs, att, lse = attend(slot_of, proj, bias, tables, blk)
    middle = token_rows + scatter(nn(att, wo))
    normed_out_two, normed_two, inverse_two = layer_norm(middle, gain_two, shift_two)
    hidden_two = gather(normed_out_two.astype(BF16))
    cot_all = gather(cot)
    gate_up = nn(hidden_two, wgu)
    gate, upper = gate_up[:, :units], gate_up[:, units:]
    sig = jax.nn.sigmoid(gate)
    act = (gate * sig * upper).astype(BF16)
    grad_act = nt(cot_all, wd)
    grad_gate = grad_act * upper * sig * (1.0 + gate * (1.0 - sig))
    grad_up = grad_act * gate * sig
    grad_gu = jnp.concatenate([grad_gate, grad_up], axis=1).astype(BF16)
    grad_hidden_two = scatter(nt(grad_gu, wgu))
    outputs = (middle + scatter(nn(act, wd))).astype(BF16)
    outputs = swap(outputs)
    gain_two_term = jnp.sum(grad_hidden_two * normed_two, axis=0)
    shift_two_term = jnp.sum(grad_hidden_two, axis=0)
    grad_middle = cot.astype(F32) + norm_back(grad_hidden_two, normed_two, inverse_two, gain_two)
    grad_middle_all = gather(grad_middle.astype(BF16))
    grad_att = nt(grad_middle_all, wo).astype(BF16)
    gq, gk, gv, bias_terms = attend_back(slot_of, qs, ks, vs, att, grad_att, lse, tables, blk)
    grad_proj = jnp.concatenate([gq, gk, gv], axis=1)
    grad_hidden_one = scatter(nt(grad_proj, wq))
    gain_one_term = jnp.sum(grad_hidden_one * normed_one, axis=0)
    shift_one_term = jnp.sum(grad_hidden_one, axis=0)
    grad_inputs = grad_middle + norm_back(grad_hidden_one, normed_one, inverse_one, gain_one)
    grad_inputs = swap(grad_inputs.astype(BF16)).astype(F32)

    def by_rows(g):
        part = lax.psum_scatter(g.astype(BF16), "pl", scatter_dimension=0, tiled=True)
        return lax.all_gather(part, ("core", "pl"), axis=0, tiled=True).astype(F32)

    def by_columns(g, parts, wide):
        sub = rows // n
        g = g.astype(BF16).reshape(n, n, sub, parts * wide).transpose(1, 0, 2, 3).reshape(n * rows, parts * wide)
        part = lax.psum_scatter(g, "pl", scatter_dimension=0, tiled=True)
        part = lax.all_to_all(part, "dp", 0, 0, tiled=True)
        whole = lax.all_gather(part, ("core", "pl"), axis=0, tiled=True)
        whole = whole.reshape(2, n, n, sub, parts, wide).transpose(1, 3, 4, 2, 0, 5)
        return whole.reshape(rows, parts * n * 2 * wide).astype(F32)

    grad_down = by_rows(tn(act, cot_all))
    grad_gateup = by_columns(tn(hidden_two, grad_gu), 2, units)
    grad_out = by_rows(tn(att, grad_middle_all))
    grad_qkv = by_columns(tn(hidden_one, grad_proj), 3, hw)
    bias_term = bias_terms[:3].reshape(3, 1, hw)
    at = me * 2 + core
    spots = (jnp.arange(2 * n, dtype=jnp.int32) == at)[None, :, None]
    bias_term = jnp.where(spots, bias_term, 0.0).reshape(n, -1)
    tiny = jnp.concatenate(
        [a.reshape(n, rows) for a in (gain_one_term, shift_one_term, gain_two_term, shift_two_term)] + [bias_term],
        axis=1,
    )
    tiny = pick(lax.psum(tiny, EVERY), 0, me)
    terms = [tiny[k * rows : (k + 1) * rows] for k in range(4)]
    return (
        outputs.reshape(inputs.shape),
        grad_inputs.reshape(inputs.shape),
        terms[0],
        terms[1],
        grad_qkv,
        tiny[4 * rows :],
        grad_out,
        terms[2],
        terms[3],
        grad_gateup,
        grad_down,
    )


def solution(mesh):
    n = mesh.shape["dp"]
    if mesh.shape["ctx"] != 2 * n:
        raise ValueError("unsupported mesh")
    grid = Mesh(mesh.devices.reshape(n, n, 2), EVERY)
    act = P("dp", ("pl", "core"), None, None)
    mat = P("dp", None)
    vec = P("dp")
    return jax.shard_map(
        functools.partial(local, n),
        mesh=grid,
        in_specs=(act, P("dp", ("pl", "core")), vec, vec, mat, vec, mat, vec, vec, mat, mat, act),
        out_specs=(act, act, vec, vec, mat, vec, mat, vec, vec, mat, mat),
        check_vma=False,
    )
```

```python
import functools

import jax
import jax.numpy as jnp
from jax import lax
from jax.experimental import pallas as pl
from jax.experimental.pallas import tpu as pltpu
from jax.sharding import Mesh
from jax.sharding import PartitionSpec as P

HEADS = 32
HEAD_DIM = 64
ROT = 16
PAIR = 2 * HEAD_DIM
SCALE = HEAD_DIM ** (-0.5)
epsilon = 1e-05
F32 = jnp.float32
BF16 = jnp.bfloat16
PLANE = ("dp", "core")
EVERY = ("dp", "pl", "core")


def layer_norm(token_rows, gain_vec, shift_vec):
    centre = jnp.mean(token_rows, axis=-1, keepdims=True)
    centred = token_rows - centre
    spread = jnp.mean(centred * centred, axis=-1, keepdims=True)
    inverse = lax.rsqrt(spread + epsilon)
    normed = centred * inverse
    return (normed * gain_vec + shift_vec, normed, inverse)


def norm_back(grad_rows, normed, inverse, gain_vec):
    scaled = grad_rows * gain_vec
    mean_plain = jnp.mean(scaled, axis=-1, keepdims=True)
    mean_cross = jnp.mean(scaled * normed, axis=-1, keepdims=True)
    return inverse * (scaled - mean_plain - normed * mean_cross)


def rotary_tables(length):
    half = ROT // 2
    lane = jnp.arange(PAIR, dtype=jnp.int32) % HEAD_DIM
    frequency = 10000.0 ** (-2.0 * (lane % half).astype(F32) / ROT)
    angles = jnp.arange(length, dtype=F32)[:, None] * frequency[None, :]
    cosine, sine = jnp.cos(angles), jnp.sin(angles)
    cos_t = jnp.where(lane < ROT, cosine, 1.0)
    low_t = jnp.where(lane < half, -sine, 0.0)
    high_t = jnp.where((lane >= half) & (lane < ROT), sine, 0.0)
    return cos_t, low_t, high_t


def head_mask(shape, head):
    lane = lax.broadcasted_iota(jnp.int32, shape, 1)
    return (lane < HEAD_DIM) if head == 0 else (lane >= HEAD_DIM)


def roll_pair(x, shift):
    return pltpu.roll(x, shift % PAIR, 1)


def nt(a, b):
    return lax.dot_general(a, b, (((1,), (1,)), ((), ())), preferred_element_type=F32)


def nn(a, b):
    return lax.dot_general(a, b, (((1,), (0,)), ((), ())), preferred_element_type=F32)


def tn(a, b):
    return lax.dot_general(a, b, (((0,), (0,)), ((), ())), preferred_element_type=F32)


def attend_kernel(
    blk, tile, slot_ref, pq, pk, pv, bq, bk, bv, cos_t, low_t, high_t, qs, ks, vs, att, lse, acc, top, osc
):
    length = pq.shape[0]

    def sort_block(b, carry):
        src = pl.ds(pl.multiple_of(slot_ref[b] * blk, blk), blk)
        dst = pl.ds(pl.multiple_of(b * blk, blk), blk)
        c, lo, hi = cos_t[dst, :], low_t[dst, :], high_t[dst, :]
        q = pq[src, :] + bq[...]
        k = pk[src, :] + bk[...]
        q = q * c + roll_pair(q, -(ROT // 2)) * lo + roll_pair(q, ROT // 2) * hi
        k = k * c + roll_pair(k, -(ROT // 2)) * lo + roll_pair(k, ROT // 2) * hi
        qs[dst, :] = q.astype(BF16)
        ks[dst, :] = k.astype(BF16)
        vs[dst, :] = (pv[src, :] + bv[...]).astype(BF16)
        return carry

    lax.fori_loop(0, length // blk, sort_block, 0)
    rows = lax.broadcasted_iota(jnp.int32, (tile, tile), 0)
    cols = lax.broadcasted_iota(jnp.int32, (tile, tile), 1)
    masks = [head_mask((tile, PAIR), h) for h in range(2)]

    def q_step(qi, carry):
        q_at = pl.ds(pl.multiple_of(qi * tile, tile), tile)
        q = qs[q_at, :]
        acc[...] = jnp.zeros_like(acc)
        top[...] = jnp.full(top.shape, -1e30, F32)

        def one(kj, diagonal):
            k_at = pl.ds(pl.multiple_of(kj * tile, tile), tile)
            k, v = ks[k_at, :], vs[k_at, :]
            for h in range(2):
                qm = jnp.where(masks[h], q, 0).astype(BF16)
                s = nt(qm, k) * SCALE
                if diagonal:
                    s = jnp.where(cols <= rows, s, -jnp.inf)
                old = top[h]
                new = jnp.maximum(old, jnp.max(s, axis=1, keepdims=True))
                p = jnp.exp(s - new[:, :1]).astype(BF16)
                ve = jnp.where(masks[h], v, 1).astype(BF16)
                acc[h] = acc[h] * jnp.exp(old - new) + nn(p, ve)
                top[h] = new

        def k_step(kj, c):
            one(kj, False)
            return c

        lax.fori_loop(0, qi, k_step, 0)
        one(qi, True)
        a0, a1 = acc[0], acc[1]
        sum0 = roll_pair(a0, HEAD_DIM)
        sum1 = roll_pair(a1, HEAD_DIM)
        total = jnp.where(masks[0], sum0, sum1)
        mixed = jnp.where(masks[0], a0, a1) / total
        osc[q_at, :] = mixed.astype(BF16)
        lse[q_at, :] = jnp.where(masks[0], top[0], top[1]) + jnp.log(total)
        return carry

    lax.fori_loop(0, length // tile, q_step, 0)

    def place_block(b, carry):
        dst = pl.ds(pl.multiple_of(slot_ref[b] * blk, blk), blk)
        att[dst, :] = osc[pl.ds(pl.multiple_of(b * blk, blk), blk), :]
        return carry

    lax.fori_loop(0, length // blk, place_block, 0)


def attend(slot_of, proj, bias, tables, blk):
    length, width = proj.shape
    pairs = width // (3 * PAIR)
    tile = min(512, length)
    whole = lambda f: pl.BlockSpec((length, PAIR), f)
    table = pl.BlockSpec((length, PAIR), lambda p, s: (0, 0), pipeline_mode=pl.Buffered(1))
    in_specs = (
        [whole(lambda p, s, o=o: (0, o * pairs + p)) for o in range(3)]
        + [pl.BlockSpec((1, PAIR), lambda p, s, o=o: (0, o * pairs + p)) for o in range(3)]
        + [table] * 3
    )
    out = jax.ShapeDtypeStruct((length, pairs * PAIR), BF16)
    own = whole(lambda p, s: (0, p))
    return pl.pallas_call(
        functools.partial(attend_kernel, blk, tile),
        out_shape=(out, out, out, out, jax.ShapeDtypeStruct((length, pairs * PAIR), F32)),
        grid_spec=pltpu.PrefetchScalarGridSpec(
            num_scalar_prefetch=1,
            grid=(pairs,),
            in_specs=in_specs,
            out_specs=[own] * 5,
            scratch_shapes=[
                pltpu.VMEM((2, tile, PAIR), F32),
                pltpu.VMEM((2, tile, PAIR), F32),
                pltpu.VMEM((length, PAIR), BF16),
            ],
        ),
        compiler_params=pltpu.CompilerParams(vmem_limit_bytes=56 * 2**20),
        cost_estimate=cost(41, 0),
        name="attend",
    )(slot_of, proj, proj, proj, bias, bias, bias, *tables)


def attend_back_kernel(
    blk, tile, slot_ref, qs, ks, vs, att, gat, lse, cos_t, low_t, high_t, gq, gk, gv, bias, dos, dlt, dq, dk, dv
):
    length = qs.shape[0]
    bmask = head_mask((blk, PAIR), 0)

    def sort_block(b, carry):
        src = pl.ds(pl.multiple_of(slot_ref[b] * blk, blk), blk)
        dst = pl.ds(pl.multiple_of(b * blk, blk), blk)
        g = gat[src, :]
        dos[dst, :] = g
        prod = g.astype(F32) * att[src, :].astype(F32)
        d0 = jnp.sum(jnp.where(bmask, prod, 0.0), axis=1, keepdims=True)
        d1 = jnp.sum(jnp.where(bmask, 0.0, prod), axis=1, keepdims=True)
        dlt[dst, :] = jnp.where(bmask, d0, d1)
        return carry

    lax.fori_loop(0, length // blk, sort_block, 0)
    dq[...] = jnp.zeros_like(dq)
    rows = lax.broadcasted_iota(jnp.int32, (tile, tile), 0)
    cols = lax.broadcasted_iota(jnp.int32, (tile, tile), 1)
    masks = [head_mask((tile, PAIR), h) for h in range(2)]
    steps = length // tile

    def k_step(kj, carry):
        k_at = pl.ds(pl.multiple_of(kj * tile, tile), tile)
        k, v = ks[k_at, :], vs[k_at, :]
        dk[...] = jnp.zeros_like(dk)
        dv[...] = jnp.zeros_like(dv)

        def one(qi, diagonal):
            q_at = pl.ds(pl.multiple_of(qi * tile, tile), tile)
            q, do = qs[q_at, :], dos[q_at, :]
            ls, dl = lse[q_at, :], dlt[q_at, :]
            for h in range(2):
                at = h * HEAD_DIM
                qm = jnp.where(masks[h], q, 0).astype(BF16)
                dm = jnp.where(masks[h], do, 0).astype(BF16)
                km = jnp.where(masks[h], k, 0).astype(BF16)
                p = jnp.exp(nt(qm, k) * SCALE - ls[:, at : at + 1])
                if diagonal:
                    p = jnp.where(cols <= rows, p, 0.0)
                ds = (p * (nt(dm, v) - dl[:, at : at + 1])).astype(BF16)
                dv[...] += tn(p.astype(BF16), dm)
                dk[...] += tn(ds, qm)
                dq[q_at, :] += nn(ds, km)

        one(kj, True)

        def q_step(qi, c):
            one(qi, False)
            return c

        lax.fori_loop(kj + 1, steps, q_step, 0)
        for part in range(tile // blk):
            b = kj * (tile // blk) + part
            sub = pl.ds(part * blk, blk)
            pos = pl.ds(pl.multiple_of(b * blk, blk), blk)
            dst = pl.ds(pl.multiple_of(slot_ref[b] * blk, blk), blk)
            g = dk[sub, :] * SCALE
            g = g * cos_t[pos, :] - roll_pair(g, -(ROT // 2)) * low_t[pos, :] - roll_pair(g, ROT // 2) * high_t[pos, :]
            gk[dst, :] = g.astype(BF16)
            bias[1:2, :] += jnp.sum(g, axis=0, keepdims=True)
            w = dv[sub, :]
            gv[dst, :] = w.astype(BF16)
            bias[2:3, :] += jnp.sum(w, axis=0, keepdims=True)
        return carry

    bias[...] = jnp.zeros_like(bias)
    lax.fori_loop(0, steps, k_step, 0)

    def place_block(b, carry):
        pos = pl.ds(pl.multiple_of(b * blk, blk), blk)
        dst = pl.ds(pl.multiple_of(slot_ref[b] * blk, blk), blk)
        g = dq[pos, :] * SCALE
        g = g * cos_t[pos, :] - roll_pair(g, -(ROT // 2)) * low_t[pos, :] - roll_pair(g, ROT // 2) * high_t[pos, :]
        gq[dst, :] = g.astype(BF16)
        bias[0:1, :] += jnp.sum(g, axis=0, keepdims=True)
        return carry

    lax.fori_loop(0, length // blk, place_block, 0)


def attend_back(slot_of, qs, ks, vs, att, gat, lse, tables, blk):
    length, width = qs.shape
    pairs = width // PAIR
    tile = min(512, length)
    own = pl.BlockSpec((length, PAIR), lambda p, s: (0, p))
    table = pl.BlockSpec((length, PAIR), lambda p, s: (0, 0), pipeline_mode=pl.Buffered(1))
    out = jax.ShapeDtypeStruct((length, width), BF16)
    return pl.pallas_call(
        functools.partial(attend_back_kernel, blk, tile),
        out_shape=(out, out, out, jax.ShapeDtypeStruct((8, width), F32)),
        grid_spec=pltpu.PrefetchScalarGridSpec(
            num_scalar_prefetch=1,
            grid=(pairs,),
            in_specs=[own] * 6 + [table] * 3,
            out_specs=[own] * 3 + [pl.BlockSpec((8, PAIR), lambda p, s: (0, p))],
            scratch_shapes=[
                pltpu.VMEM((length, PAIR), BF16),
                pltpu.VMEM((length, PAIR), F32),
                pltpu.VMEM((length, PAIR), F32),
                pltpu.VMEM((tile, PAIR), F32),
                pltpu.VMEM((tile, PAIR), F32),
            ],
        ),
        compiler_params=pltpu.CompilerParams(vmem_limit_bytes=56 * 2**20),
        cost_estimate=cost(50, 0),
        name="attend_back",
    )(slot_of, qs, ks, vs, att, gat, lse, *tables)


HBM = pltpu.MemorySpace.HBM
MESH_ID = pl.DeviceIdType.MESH


def ring_pos(dp, n):
    odd, half = dp % 2, dp // 2
    return odd * (half + 1) + (1 - odd) * ((n - half) % n)


def ring_dp(pos, n):
    far = ((pos + n - 1) % n) // (n // 2)
    return (1 - far) * (2 * pos - 1) + far * (2 * ((n - pos) % n))


def plane_ids(n):
    dp, core = lax.axis_index("dp"), lax.axis_index("core")
    pos = ring_pos(dp, n)
    at = lambda off: ring_dp((pos + off + n) % n, n)
    return dp, core, at


def greet(ids):
    barrier = pltpu.get_barrier_semaphore()
    for where in ids:
        pl.semaphore_signal(barrier, inc=1, device_id=where, device_id_type=MESH_ID)
    pl.semaphore_wait(barrier, len(ids))


def remote(src, dst, send, recv, where):
    return pltpu.make_async_remote_copy(
        src_ref=src, dst_ref=dst, send_sem=send, recv_sem=recv, device_id=where, device_id_type=MESH_ID
    )


def col_tile(width):
    for t in (512, 384, 256, 128):
        if width % t == 0:
            return t
    return width


def gather_blocks(n, x_ref, buf, s_in, s_ring, r_ring, s_part, r_part, ready, use):
    dp, core, at = plane_ids(n)
    rows = x_ref.shape[0]
    half = rows // 2
    mid = n // 2
    slot = lambda off, flip: 2 * at(off) + (core if flip == 0 else 1 - core)
    right, left, mate = {"dp": at(1)}, {"dp": at(-1)}, {"core": 1 - core}
    load_x = pltpu.make_async_copy(x_ref, buf.at[slot(0, 0)], s_in)
    load_x.start()
    greet((right, left, mate))
    load_x.wait()
    top, low = pl.ds(0, half), pl.ds(half, half)

    def push(src_slot, part, where, send, recv):
        view = buf.at[src_slot] if part is None else buf.at[src_slot, part]
        remote(view, view, send, recv, where).start()

    def sent(part, send):
        view = buf.at[0] if part is None else buf.at[0, part]
        remote(view, view, send, r_ring.at[0, 0], right).wait_send()

    def arrive(src_slot, part, sem):
        view = buf.at[src_slot] if part is None else buf.at[src_slot, part]
        remote(view, view, s_ring.at[0, 0], sem, right).wait_recv()

    own = slot(0, 0)
    push(own, None, right, s_ring.at[0, 0], r_ring.at[1, 0])
    push(own, None, left, s_ring.at[0, 1], r_ring.at[1, 1])
    push(own, None, mate, s_part.at[0, 0], r_part.at[0, 0])

    def ring_step(d):
        for side, sign in ((0, -1), (1, 1)):
            src = slot(sign * d, 0)
            onward = right if side == 0 else left
            if d < mid:
                arrive(src, None, r_ring.at[d, side])
                if d + 1 < mid:
                    push(src, None, onward, s_ring.at[d, side], r_ring.at[d + 1, side])
                else:
                    push(src, top if side == 0 else low, onward, s_ring.at[d, side], r_ring.at[mid, side])
                push(src, None, mate, s_part.at[d, side], r_part.at[d, side])
            else:
                part = top if side == 0 else low
                arrive(src, part, r_ring.at[mid, side])
                push(src, part, mate, s_part.at[mid, side], r_part.at[mid, side])

    def mate_step(d):
        if d == 0:
            arrive(slot(0, 1), None, r_part.at[0, 0])
        elif d < mid:
            arrive(slot(-d, 1), None, r_part.at[d, 0])
            arrive(slot(d, 1), None, r_part.at[d, 1])
        else:
            arrive(slot(d, 1), top, r_part.at[d, 0])
            arrive(slot(d, 1), low, r_part.at[d, 1])

    ready()

    def body(step, carry):
        for d in range(1, mid + 1):
            first = 2 + 4 * (d - 1)

            @pl.when(step == first)
            def _():
                ring_step(d)

            @pl.when(step == first + (2 if d < mid else 1))
            def _():
                mate_step(d)

        @pl.when(step == 1)
        def _():
            mate_step(0)

        later = jnp.maximum(step - 2, 0)
        d = jnp.where(step < 2, 0, 1 + later // 4)
        kind = jnp.where(step < 2, step, later % 4)
        last = jnp.where(step < 2, 1, d // mid)
        flip = jnp.where(last == 1, kind, kind // 2)
        off = jnp.where(kind % 2 == 0, -d, d)
        use(step, 2 * at(off) + core + flip - 2 * core * flip)
        return carry

    lax.fori_loop(0, 2 * n, body, 0)
    for d in range(mid + 1):
        for side in range(2):
            part = top if side == 0 else low
            if d < mid:
                sent(part if d + 1 == mid and d > 0 else None, s_ring.at[d, side])
            if d > 0 or side == 0:
                sent(part if d == mid else None, s_part.at[d, side])


def gather_dot_kernel(
    n, trans, x_ref, w_ref, all_ref, res_ref, buf, wv, stage, s_ring, r_ring, s_part, r_part, s_in, s_out, s_res
):
    load_w = pltpu.make_async_copy(w_ref, wv, s_in.at[0])
    load_w.start()
    width = res_ref.shape[-1]
    tile = col_tile(width)

    def put(keep, where):
        return pltpu.make_async_copy(stage.at[keep], res_ref.at[where], s_res.at[keep])

    def use(step, where):
        keep = step % 2

        @pl.when(step >= 2)
        def _():
            put(keep, where).wait()

        pltpu.make_async_copy(buf.at[where], all_ref.at[where], s_out.at[step]).start()
        block = buf[where]
        for c in range(width // tile):
            cols = pl.ds(c * tile, tile)
            part = nt(block, wv[cols, :]) if trans else nn(block, wv[:, cols])
            stage[keep, :, cols] = part.astype(stage.dtype)
        put(keep, where).start()

    gather_blocks(n, x_ref, buf, s_in.at[1], s_ring, r_ring, s_part, r_part, load_w.wait, use)
    for keep in range(2):
        put(keep, 0).wait()
    for step in range(2 * n):
        pltpu.make_async_copy(buf.at[0], all_ref.at[0], s_out.at[step]).wait()


def cost(us, flops):
    return pl.CostEstimate(flops=flops, bytes_accessed=int(us * 3.4e6), transcendentals=0)


def ring_sems(n):
    dma = pltpu.SemaphoreType.DMA
    mid = n // 2
    return [dma((mid, 2)), dma((mid + 1, 2)), dma((mid + 1, 2)), dma((mid + 1, 2))]


def gather_dot(n, cid, x, w, trans, dtype):
    rows, depth = x.shape
    width = w.shape[0] if trans else w.shape[1]
    dma = pltpu.SemaphoreType.DMA
    everything, result = pl.pallas_call(
        functools.partial(gather_dot_kernel, n, trans),
        out_shape=(
            jax.ShapeDtypeStruct((2 * n, rows, depth), x.dtype),
            jax.ShapeDtypeStruct((2 * n, rows, width), dtype),
        ),
        in_specs=[pl.BlockSpec(memory_space=HBM)] * 2,
        out_specs=[pl.BlockSpec(memory_space=HBM)] * 2,
        scratch_shapes=[
            pltpu.VMEM((2 * n, rows, depth), x.dtype),
            pltpu.VMEM(w.shape, w.dtype),
            pltpu.VMEM((2, rows, width), dtype),
        ]
        + ring_sems(n)
        + [dma((2,)), dma((2 * n,)), dma((2,))],
        compiler_params=pltpu.CompilerParams(
            collective_id=cid, has_side_effects=True, vmem_limit_bytes=60 * 2**20
        ),
        cost_estimate=cost(42, 4 * n * rows * depth * width),
        name="gather_dot",
    )(x, w)
    return everything.reshape(2 * n * rows, depth), result.reshape(2 * n * rows, width)


def gather_mlp_kernel(
    n, x_ref, w_ref, c_ref, d_ref, all_ref, act_ref, gg_ref, gu_ref, buf, wv, dv, cv, stage, s_ring, r_ring, s_part, r_part, s_in, s_c, s_out, s_res
):
    load_w = pltpu.make_async_copy(w_ref, wv, s_in.at[0])
    load_d = pltpu.make_async_copy(d_ref, dv, s_in.at[2])
    load_w.start()
    load_d.start()
    outs = (act_ref, gg_ref, gu_ref)

    def put(keep, k, where):
        return pltpu.make_async_copy(stage.at[keep, k], outs[k].at[where], s_res.at[keep, k])

    def ready():
        load_w.wait()
        load_d.wait()

    def use(step, where):
        keep = step % 2
        load_c = pltpu.make_async_copy(c_ref.at[where], cv, s_c)
        load_c.start()

        @pl.when(step >= 2)
        def _():
            for k in range(3):
                put(keep, k, where).wait()

        pltpu.make_async_copy(buf.at[where], all_ref.at[where], s_out.at[step]).start()
        block = buf[where]
        gate = nn(block, wv[0])
        upper = nn(block, wv[1])
        load_c.wait()
        back = nt(cv[...], dv[...])
        sig = 1.0 / (1.0 + jnp.exp(-gate))
        swish = gate * sig
        stage[keep, 0] = (swish * upper).astype(BF16)
        stage[keep, 1] = (back * upper * sig * (1.0 + gate * (1.0 - sig))).astype(BF16)
        stage[keep, 2] = (back * swish).astype(BF16)
        for k in range(3):
            put(keep, k, where).start()

    gather_blocks(n, x_ref, buf, s_in.at[1], s_ring, r_ring, s_part, r_part, ready, use)
    for keep in range(2):
        for k in range(3):
            put(keep, k, 0).wait()
    for step in range(2 * n):
        pltpu.make_async_copy(buf.at[0], all_ref.at[0], s_out.at[step]).wait()


def gather_mlp(n, cid, x, w, cot, wd):
    rows, depth = x.shape
    units = wd.shape[0]
    dma = pltpu.SemaphoreType.DMA
    out = jax.ShapeDtypeStruct((2 * n, rows, units), BF16)
    res = pl.pallas_call(
        functools.partial(gather_mlp_kernel, n),
        out_shape=(jax.ShapeDtypeStruct((2 * n, rows, depth), x.dtype), out, out, out),
        in_specs=[pl.BlockSpec(memory_space=HBM)] * 4,
        out_specs=[pl.BlockSpec(memory_space=HBM)] * 4,
        scratch_shapes=[
            pltpu.VMEM((2 * n, rows, depth), x.dtype),
            pltpu.VMEM(w.shape, w.dtype),
            pltpu.VMEM(wd.shape, wd.dtype),
            pltpu.VMEM((rows, depth), BF16),
            pltpu.VMEM((2, 3, rows, units), BF16),
        ]
        + ring_sems(n)
        + [dma((3,)), dma, dma((2 * n,)), dma((2, 3))],
        compiler_params=pltpu.CompilerParams(
            collective_id=cid, has_side_effects=True, vmem_limit_bytes=60 * 2**20
        ),
        cost_estimate=cost(48, 12 * n * rows * depth * units),
        name="gather_mlp",
    )(x, w, cot.reshape(2 * n, rows, depth), wd)
    return [a.reshape(2 * n * rows, -1) for a in res]


def dot_scatter_kernel(
    n, count, trans, *refs
):
    a_refs, w_refs, out_ref = refs[:count], refs[count : 2 * count], refs[2 * count]
    avs, wvs = refs[2 * count + 1 : 3 * count + 1], refs[3 * count + 1 : 4 * count + 1]
    to_mate, from_mate, hop, from_ring, acc, s_a, s_w, s_part, r_part, s_ring, r_ring, s_o = refs[4 * count + 1 :]
    dp, core, at = plane_ids(n)
    rows = acc.shape[0]
    half = rows // 2
    mid = n // 2
    right, left, mate = {"dp": at(1)}, {"dp": at(-1)}, {"core": 1 - core}
    offsets = [mid]
    for d in range(mid - 1, 0, -1):
        offsets += [d, -d]
    offsets += [0]

    def offset_of(j):
        d = mid - (j + 1) // 2
        return jnp.where(j % 2 == 1, d, -d)

    loads = [pltpu.make_async_copy(w_refs[k], wvs[k], s_w.at[k]) for k in range(count)]
    for load in loads:
        load.start()

    def slot_of(step):
        j, own = step // 2, step % 2
        who = core + (1 - own) - 2 * core * (1 - own)
        return 2 * at(offset_of(j)) + who

    def load_a(step, k):
        return pltpu.make_async_copy(a_refs[k].at[slot_of(step)], avs[k].at[step], s_a.at[step, k])

    for step in range(2 * n):
        for k in range(count):
            load_a(step, k).start()
    greet((right, left, mate))
    for load in loads:
        load.wait()
    depth = out_ref.shape[-1]
    tile = col_tile(depth)
    top, low = pl.ds(0, half), pl.ds(half, half)
    waits = []

    def hand(j):
        return remote(to_mate.at[j], from_mate.at[j], s_part.at[j], r_part.at[j], mate)

    def ring(j, part, side, send, recv):
        src = hop.at[j] if part is None else hop.at[j, part]
        dst = from_ring.at[recv, side] if part is None else from_ring.at[recv, side, part]
        return remote(src, dst, s_ring.at[send, side], r_ring.at[recv, side], right if side == 0 else left)

    def body(step, carry):
        j, own = step // 2, step % 2
        for k in range(count):
            load_a(step, k).wait()

        def product(cols):
            total = None
            for k in range(count):
                block = avs[k][step]
                part = nt(block, wvs[k][cols, :]) if trans else nn(block, wvs[k][:, cols])
                total = part if total is None else total + part
            return total

        @pl.when(own == 0)
        def _():
            for c in range(depth // tile):
                cols = pl.ds(c * tile, tile)
                to_mate[j, :, cols] = product(cols).astype(BF16)
            hand(j).start()

        @pl.when(own == 1)
        def _():
            hand(j).wait_recv()
            for c in range(depth // tile):
                cols = pl.ds(c * tile, tile)
                part = product(cols) + from_mate[j, :, cols].astype(F32)
                acc[:, cols] = part
                hop[j, :, cols] = part.astype(BF16)

            @pl.when(j == 0)
            def _():
                ring(0, top, 0, 0, mid - 1).start()
                ring(0, low, 1, 0, mid - 1).start()

            for d in range(mid - 1, 0, -1):
                first = 1 + 2 * (mid - 1 - d)

                @pl.when(j == first + 1)
                def _():
                    for side in range(2):
                        k = first + side
                        if d == mid - 1:
                            part = top if side == 0 else low
                            ring(0, part, side, 0, d).wait_recv()
                            hop[k, part, :] = (
                                hop[k, part, :].astype(F32) + from_ring[d, side, part, :].astype(F32)
                            ).astype(BF16)
                        else:
                            ring(k - 2, None, side, 0, d).wait_recv()
                            hop[k] = (hop[k].astype(F32) + from_ring[d, side].astype(F32)).astype(BF16)
                        ring(k, None, side, mid - d, d - 1).start()

        return carry

    lax.fori_loop(0, 2 * n, body, 0)
    for side in range(2):
        ring(n - 2 + side - 1, None, side, mid - 1, 0).wait_recv()
    acc[...] += from_ring[0, 0].astype(F32) + from_ring[0, 1].astype(F32)
    put = pltpu.make_async_copy(acc, out_ref, s_o)
    put.start()
    for j in range(n):
        hand(j).wait_send()
    ring(0, top, 0, 0, mid - 1).wait_send()
    ring(0, low, 1, 0, mid - 1).wait_send()
    for d in range(mid - 1, 0, -1):
        for side in range(2):
            ring(1 + 2 * (mid - 1 - d) + side, None, side, mid - d, d - 1).wait_send()
    put.wait()


def dot_scatter(n, cid, terms, trans):
    depth = terms[0][1].shape[0] if trans else terms[0][1].shape[1]
    rows = terms[0][0].shape[0] // (2 * n)
    mid = n // 2
    count = len(terms)
    dma = pltpu.SemaphoreType.DMA
    lhs = [a.reshape(2 * n, rows, a.shape[1]) for a, _ in terms]
    rhs = [w for _, w in terms]
    return pl.pallas_call(
        functools.partial(dot_scatter_kernel, n, count, trans),
        out_shape=jax.ShapeDtypeStruct((rows, depth), F32),
        in_specs=[pl.BlockSpec(memory_space=HBM)] * (2 * count),
        out_specs=pl.BlockSpec(memory_space=HBM),
        scratch_shapes=[pltpu.VMEM(a.shape, BF16) for a in lhs]
        + [pltpu.VMEM(w.shape, BF16) for w in rhs]
        + [
            pltpu.VMEM((n, rows, depth), BF16),
            pltpu.VMEM((n, rows, depth), BF16),
            pltpu.VMEM((n, rows, depth), BF16),
            pltpu.VMEM((mid, 2, rows, depth), BF16),
            pltpu.VMEM((rows, depth), F32),
            dma((2 * n, count)),
            dma((count,)),
            dma((n,)),
            dma((n,)),
            dma((mid, 2)),
            dma((mid, 2)),
            dma,
        ],
        compiler_params=pltpu.CompilerParams(
            collective_id=cid, has_side_effects=True, vmem_limit_bytes=62 * 2**20
        ),
        cost_estimate=cost(45, 4 * n * rows * depth * sum(a.shape[2] for a in lhs)),
        name="dot_scatter",
    )(*lhs, *rhs)


def start_kernel(
    n, x_ref, w_ref, small_ref, block_ref, x_out, w_out, small_out, block_out, xv, wv, s_own, s_x, r_x, s_w, r_w, s_s, r_s, s_b, r_b
):
    dp, plane, core = (lax.axis_index(a) for a in EVERY)
    rows = w_ref.shape[0]
    width = w_ref.shape[1] // 3
    wide = width // (2 * n)
    away = dp != plane
    across = {"dp": plane, "pl": dp, "core": core}
    barrier = pltpu.get_barrier_semaphore()

    def knock(where):
        pl.semaphore_signal(barrier, inc=1, device_id=where, device_id_type=MESH_ID)

    def send_x():
        return remote(x_ref, x_out, s_x, r_x, across)

    def send_w(j, part):
        to = (dp + j) % n
        at = pl.multiple_of(part * width + to * (2 * wide) + core * wide, 128)
        dst = w_out.at[pl.ds(pl.multiple_of(dp * rows, 128), rows), pl.ds(part * wide, wide)]
        return remote(w_ref.at[:, pl.ds(at, wide)], dst, s_w.at[j, part], r_w.at[j, part], {"dp": to})

    def send_s(j):
        to = (dp + j) % n
        return remote(small_ref, small_out.at[dp], s_s.at[j], r_s.at[j], {"dp": to})

    def send_b(i, k):
        to = {"dp": (plane + i) % n, "pl": dp, "core": (core + k) % 2}
        return remote(block_ref, block_out.at[2 * plane + core], s_b.at[i, k], r_b.at[i, k], to)

    def own_w(part, back):
        at = pl.multiple_of(part * width + dp * (2 * wide) + core * wide, 128)
        src = w_ref.at[:, pl.ds(at, wide)]
        dst = w_out.at[pl.ds(pl.multiple_of(dp * rows, 128), rows), pl.ds(part * wide, wide)]
        if back:
            return pltpu.make_async_copy(wv.at[part], dst, s_own.at[part])
        return pltpu.make_async_copy(src, wv.at[part], s_own.at[part])

    own_s = pltpu.make_async_copy(small_ref, small_out.at[dp], s_own.at[3])
    own_b = pltpu.make_async_copy(block_ref, block_out.at[2 * plane + core], s_own.at[4])
    for part in range(3):
        own_w(part, False).start()
    own_s.start()
    for j in range(1, n):
        knock({"dp": (dp + n - j) % n})
    for i in range(n):
        for k in range(2):

            @pl.when(away | (i + k > 0))
            def _():
                knock({"dp": plane, "pl": (dp + n - i) % n, "core": (core + k) % 2})

    @pl.when(away)
    def _():
        knock(across)
        pl.semaphore_wait(barrier, 3 * n)
        send_x().start()
        send_b(0, 0).start()

    @pl.when(jnp.logical_not(away))
    def _():
        pl.semaphore_wait(barrier, 3 * n - 2)
        pltpu.make_async_copy(x_ref, xv, s_own.at[5]).start()
        own_b.start()

    for i in range(n):
        for k in range(2):
            if i + k > 0:
                send_b(i, k).start()
    for j in range(1, n):
        send_s(j).start()
    for j in range(1, n):
        for part in range(3):
            send_w(j, part).start()
    for part in range(3):
        own_w(part, False).wait()
        own_w(part, True).start()

    @pl.when(jnp.logical_not(away))
    def _():
        pltpu.make_async_copy(x_ref, xv, s_own.at[5]).wait()
        pltpu.make_async_copy(xv, x_out, s_own.at[5]).start()
        own_b.wait()
        pltpu.make_async_copy(xv, x_out, s_own.at[5]).wait()

    own_s.wait()
    for part in range(3):
        own_w(part, True).wait()
    for i in range(n):
        for k in range(2):
            if i + k > 0:
                send_b(i, k).wait()
    for j in range(1, n):
        send_s(j).wait()
        for part in range(3):
            send_w(j, part).wait()

    @pl.when(away)
    def _():
        send_b(0, 0).wait()
        send_x().wait()


def start(n, cid, x, w, small, block):
    rows, wide = w.shape[0], w.shape[1] // (6 * n)
    dma = pltpu.SemaphoreType.DMA
    return pl.pallas_call(
        functools.partial(start_kernel, n),
        out_shape=(
            jax.ShapeDtypeStruct(x.shape, x.dtype),
            jax.ShapeDtypeStruct((n * rows, 3 * wide), w.dtype),
            jax.ShapeDtypeStruct((n,) + small.shape, small.dtype),
            jax.ShapeDtypeStruct((2 * n,) + block.shape, block.dtype),
        ),
        in_specs=[pl.BlockSpec(memory_space=HBM)] * 4,
        out_specs=[pl.BlockSpec(memory_space=HBM)] * 4,
        scratch_shapes=[
            pltpu.VMEM(x.shape, x.dtype),
            pltpu.VMEM((3, rows, wide), w.dtype),
            dma((6,)),
            dma,
            dma,
            dma((n, 3)),
            dma((n, 3)),
            dma((n,)),
            dma((n,)),
            dma((n, 2)),
            dma((n, 2)),
        ],
        compiler_params=pltpu.CompilerParams(collective_id=cid, has_side_effects=True),
        cost_estimate=cost(75, 0),
        name="start",
    )(x, w, small, block)


def total_kernel(n, a_ref, o_ref, mine, others, part, sums, s_in, s_a, r_a, s_b, r_b, s_out):
    dp, plane, core = (lax.axis_index(a) for a in EVERY)
    barrier = pltpu.get_barrier_semaphore()
    load = pltpu.make_async_copy(a_ref, mine, s_in)
    load.start()
    peers = [{"dp": (dp + j) % n} for j in range(1, n)]
    stack = [(z, k) for z in range(n) for k in range(2) if z + k > 0]
    for j in range(1, n):
        pl.semaphore_signal(barrier, inc=1, device_id={"dp": (dp + n - j) % n}, device_id_type=MESH_ID)
    for z, k in stack:
        where = {"pl": (plane + n - z) % n, "core": (core + k) % 2}
        pl.semaphore_signal(barrier, inc=1, device_id=where, device_id_type=MESH_ID)
    pl.semaphore_wait(barrier, 3 * n - 2)
    load.wait()

    def send_a(j):
        to = (dp + j) % n
        return remote(mine.at[to], others.at[j], s_a.at[j], r_a.at[j], {"dp": to})

    def send_b(i):
        z, k = stack[i]
        where = {"pl": (plane + z) % n, "core": (core + k) % 2}
        return remote(part, sums.at[i], s_b.at[i], r_b.at[i], where)

    for j in range(1, n):
        send_a(j).start()
    value = mine[dp]
    for j in range(1, n):
        send_a(j).wait_recv()
        value = value + others[j]
    part[...] = value
    for i in range(len(stack)):
        send_b(i).start()
    for i in range(len(stack)):
        send_b(i).wait_recv()
        value = value + sums[i]
    for j in range(1, n):
        send_a(j).wait_send()
    for i in range(len(stack)):
        send_b(i).wait_send()
    mine[0] = value
    put = pltpu.make_async_copy(mine.at[0], o_ref, s_out)
    put.start()
    put.wait()


def total(n, cid, a):
    dma = pltpu.SemaphoreType.DMA
    shape = a.shape[1:]
    return pl.pallas_call(
        functools.partial(total_kernel, n),
        out_shape=jax.ShapeDtypeStruct(shape, F32),
        in_specs=[pl.BlockSpec(memory_space=HBM)],
        out_specs=pl.BlockSpec(memory_space=HBM),
        scratch_shapes=[
            pltpu.VMEM(a.shape, F32),
            pltpu.VMEM(a.shape, F32),
            pltpu.VMEM(shape, F32),
            pltpu.VMEM((2 * n - 1,) + shape, F32),
            dma,
            dma((n,)),
            dma((n,)),
            dma((2 * n - 1,)),
            dma((2 * n - 1,)),
            dma,
        ],
        compiler_params=pltpu.CompilerParams(collective_id=cid, has_side_effects=True),
        cost_estimate=cost(12, 0),
        name="total",
    )(a)


def assemble_kernel(wide, in_ref, out_ref):
    for k in range(2):
        out_ref[:, k * wide : (k + 1) * wide] = in_ref[k, 0, 0, 0].astype(F32)


def assemble(n, whole, parts, wide):
    sub = whole.shape[4]
    apart = whole.shape[3] == parts
    at = (lambda z, j, p: (0, z, j, p, 0, 0)) if apart else (lambda z, j, p: (0, z, j, 0, 0, p))
    return pl.pallas_call(
        functools.partial(assemble_kernel, wide),
        grid=(n, n, parts),
        out_shape=jax.ShapeDtypeStruct((n * sub, parts * n * 2 * wide), F32),
        in_specs=[pl.BlockSpec((2, 1, 1, 1, sub, wide), at)],
        out_specs=pl.BlockSpec((sub, 2 * wide), lambda z, j, p: (z, p * n + j)),
        cost_estimate=cost(12, 0),
        name="assemble",
    )(whole)


def split_columns_kernel(units, w_ref, o_ref):
    core = lax.axis_index("core")
    for k in range(2):

        @pl.when(core == k)
        def _():
            o_ref[0, 0] = w_ref[:, k * units : (k + 1) * units]


def split_columns(n, w):
    rows = w.shape[0]
    units = w.shape[1] // (4 * n)
    if (2 * units) % 128:
        mine = w.reshape(rows, 2, n, 2, units)
        return lax.dynamic_index_in_dim(mine, lax.axis_index("core"), 3, keepdims=False).transpose(2, 1, 0, 3)
    return pl.pallas_call(
        functools.partial(split_columns_kernel, units),
        grid=(n, 2),
        out_shape=jax.ShapeDtypeStruct((n, 2, rows, units), w.dtype),
        in_specs=[pl.BlockSpec((rows, 2 * units), lambda j, p: (0, p * n + j))],
        out_specs=pl.BlockSpec((1, 1, rows, units), lambda j, p: (j, p, 0, 0)),
        cost_estimate=cost(8, 0),
        name="split_columns",
    )(w)


def local(
    groups,
    inputs,
    block_of,
    first_gain,
    first_shift,
    w_qkv,
    qkv_bias,
    w_out,
    second_gain,
    second_shift,
    w_gateup,
    w_down,
    cotangent,
):
    n = groups
    blk = inputs.shape[2]
    slots = inputs.shape[1]
    toks = slots * blk
    width = inputs.shape[3]
    rows = w_qkv.shape[0]
    me, plane, core = (lax.axis_index(a) for a in EVERY)
    hw = width // (2 * n)
    units = w_down.shape[0] // 2
    swap_pairs = [(s * n + z, z * n + s) for s in range(n) for z in range(n)]
    swap = lambda a: lax.ppermute(a, ("dp", "pl"), swap_pairs)
    pick = lambda a, axis, at: lax.dynamic_index_in_dim(a, at, axis, keepdims=False)

    def rows_first(g):
        return lax.psum_scatter(g.astype(BF16), "pl", scatter_dimension=0, tiled=True)

    def last(part):
        return lax.all_gather(part, ("core", "pl"), axis=0, tiled=True).astype(F32)

    def columns_first(g):
        parts, _, wide = g.shape
        g = g.reshape(parts, n, n, rows // n, wide).transpose(2, 1, 0, 3, 4)
        part = lax.psum_scatter(g, "pl", scatter_dimension=0, tiled=True)
        part = part.reshape(n, parts * rows // n, wide)
        return lax.all_to_all(part, "dp", 0, 0, tiled=True)

    def columns_last(part, parts, wide):
        whole = lax.all_gather(part, ("core", "pl"), axis=0, tiled=True)
        whole = whole.reshape(2, n, n, -1, rows // n, part.shape[2])
        if (2 * wide) % 128 == 0:
            return assemble(n, whole, parts, wide)
        whole = whole.reshape(2, n, n, whole.shape[3], rows // n, -1, wide).transpose(1, 4, 3, 5, 2, 0, 6)
        return whole.reshape(rows, parts * n * 2 * wide).astype(F32)

    small = jnp.concatenate([first_gain, first_shift, second_gain, second_shift, qkv_bias]).reshape(-1, 128)
    ids = jnp.zeros((8, 128), jnp.int32).at[0, :slots].set(block_of.reshape(-1))
    x, wq, small, ids = start(n, 0, inputs.reshape(toks, width), w_qkv, small, ids)
    x, w_gateup, cotangent, w_out, w_down = lax.optimization_barrier((x, w_gateup, cotangent, w_out, w_down))
    token_rows = x.astype(F32)
    small = small.reshape(n, -1)
    gain_one, shift_one, gain_two, shift_two = (
        small[:, k * rows : (k + 1) * rows].reshape(width) for k in range(4)
    )
    bias = small[:, 4 * rows :].reshape(3, n, 2, hw)
    bias = pick(pick(bias, 1, me), 1, core).reshape(1, 3 * hw)
    blocks = ids[:, 0, :slots].reshape(-1)
    order = jnp.arange(blocks.shape[0], dtype=jnp.int32)
    slot_of = jnp.sum(jnp.where(blocks[None, :] == order[:, None], order[None, :], 0), axis=1)

    mine = split_columns(n, w_gateup)
    wgu = jnp.zeros((2, n, rows, units), BF16)
    wgu = lax.dynamic_update_index_in_dim(wgu, pick(mine, 0, me), me, 1)
    for j in range(1, n):
        got = lax.ppermute(pick(mine, 0, (me + j) % n), "dp", [(i, (i + j) % n) for i in range(n)])
        wgu = lax.dynamic_update_index_in_dim(wgu, got, (me + n - j) % n, 1)
    wgu = wgu.reshape(2, n * rows, units)
    wo = pick(w_out.reshape(2, hw, width), 0, core)
    wd = pick(w_down.reshape(2, units, width), 0, core)
    cot = swap(cotangent.reshape(toks, width))
    tables = rotary_tables(blocks.shape[0] * blk)

    normed_out, normed_one, inverse_one = layer_norm(token_rows, gain_one, shift_one)
    hidden_one, proj = gather_dot(n, 1, normed_out.astype(BF16), wq, False, F32)
    proj, cot = lax.optimization_barrier((proj, cot))
    cot_all = lax.all_gather(cot, PLANE, axis=0, tiled=True)
    qs, ks, vs, att, lse = attend(slot_of, proj, bias, tables, blk)
    middle = token_rows + dot_scatter(n, 2, [(att, wo)], False)
    normed_out_two, normed_two, inverse_two = layer_norm(middle, gain_two, shift_two)
    hidden_two, act, grad_gate, grad_up = gather_mlp(n, 3, normed_out_two.astype(BF16), wgu, cot_all, wd)
    grad_down = tn(act, cot_all).astype(BF16)
    grad_gateup = jnp.stack([tn(hidden_two, grad_gate), tn(hidden_two, grad_up)]).astype(BF16)
    grad_gate, grad_up, grad_down, grad_gateup = lax.optimization_barrier((grad_gate, grad_up, grad_down, grad_gateup))
    down_part = rows_first(grad_down)
    gateup_part = columns_first(grad_gateup)
    grad_hidden_two = dot_scatter(n, 4, [(grad_gate, wgu[0]), (grad_up, wgu[1])], True)
    gain_two_term = jnp.sum(grad_hidden_two * normed_two, axis=0)
    shift_two_term = jnp.sum(grad_hidden_two, axis=0)
    grad_middle = cot.astype(F32) + norm_back(grad_hidden_two, normed_two, inverse_two, gain_two)
    grad_middle_all, grad_att = gather_dot(n, 5, grad_middle.astype(BF16), wo, True, BF16)
    gq, gk, gv, bias_terms = attend_back(slot_of, qs, ks, vs, att, grad_att, lse, tables, blk)
    grad_proj = jnp.concatenate([gq, gk, gv], axis=1)
    grad_proj, gateup_part, down_part = lax.optimization_barrier((grad_proj, gateup_part, down_part))
    grad_hidden_one = dot_scatter(n, 6, [(grad_proj, wq)], True)
    gain_one_term = jnp.sum(grad_hidden_one * normed_one, axis=0)
    shift_one_term = jnp.sum(grad_hidden_one, axis=0)
    grad_inputs = grad_middle + norm_back(grad_hidden_one, normed_one, inverse_one, gain_one)
    grad_inputs = grad_inputs.astype(BF16)
    grad_inputs, act = lax.optimization_barrier((grad_inputs, act))
    outputs = swap((middle + dot_scatter(n, 8, [(act, wd)], False)).astype(BF16))
    grad_inputs = swap(grad_inputs).astype(F32)

    grad_down = last(down_part)
    grad_gateup = columns_last(gateup_part, 2, units)
    grad_out = last(rows_first(tn(att, grad_middle_all)))
    grad_qkv = columns_last(columns_first(tn(hidden_one, grad_proj).astype(BF16)[None]), 3, hw)
    bias_term = bias_terms[:3].reshape(3, 1, hw)
    at = me * 2 + core
    spots = (jnp.arange(2 * n, dtype=jnp.int32) == at)[None, :, None]
    bias_term = jnp.where(spots, bias_term, 0.0).reshape(n, -1)
    tiny = jnp.concatenate(
        [a.reshape(n, rows) for a in (gain_one_term, shift_one_term, gain_two_term, shift_two_term)] + [bias_term],
        axis=1,
    )
    tiny = total(n, 7, tiny.reshape(n, -1, 128)).reshape(-1)
    terms = [tiny[k * rows : (k + 1) * rows] for k in range(4)]
    return (
        outputs.reshape(inputs.shape),
        grad_inputs.reshape(inputs.shape),
        terms[0],
        terms[1],
        grad_qkv,
        tiny[4 * rows :],
        grad_out,
        terms[2],
        terms[3],
        grad_gateup,
        grad_down,
    )


def solution(mesh):
    n = mesh.shape["dp"]
    if mesh.shape["ctx"] != 2 * n:
        raise ValueError("unsupported mesh")
    grid = Mesh(mesh.devices.reshape(n, n, 2), EVERY)
    act = P("dp", ("pl", "core"), None, None)
    mat = P("dp", None)
    vec = P("dp")
    return jax.shard_map(
        functools.partial(local, n),
        mesh=grid,
        in_specs=(act, P("dp", ("pl", "core")), vec, vec, mat, vec, mat, vec, vec, mat, mat, act),
        out_specs=(act, act, vec, vec, mat, vec, mat, vec, vec, mat, mat),
        check_vma=False,
    )
```

```python
import functools

import jax
import jax.numpy as jnp
from jax import lax
from jax.experimental import pallas as pl
from jax.experimental.pallas import tpu as pltpu
from jax.sharding import Mesh
from jax.sharding import PartitionSpec as P

HEADS = 32
HEAD_DIM = 64
ROT = 16
PAIR = 2 * HEAD_DIM
SCALE = HEAD_DIM ** (-0.5)
epsilon = 1e-05
F32 = jnp.float32
BF16 = jnp.bfloat16
PLANE = ("dp", "core")
EVERY = ("dp", "pl", "core")


def layer_norm(token_rows, gain_vec, shift_vec):
    centre = jnp.mean(token_rows, axis=-1, keepdims=True)
    centred = token_rows - centre
    spread = jnp.mean(centred * centred, axis=-1, keepdims=True)
    inverse = lax.rsqrt(spread + epsilon)
    normed = centred * inverse
    return (normed * gain_vec + shift_vec, normed, inverse)


def norm_back(grad_rows, normed, inverse, gain_vec):
    scaled = grad_rows * gain_vec
    mean_plain = jnp.mean(scaled, axis=-1, keepdims=True)
    mean_cross = jnp.mean(scaled * normed, axis=-1, keepdims=True)
    return inverse * (scaled - mean_plain - normed * mean_cross)


def rotary_tables(length):
    half = ROT // 2
    lane = jnp.arange(PAIR, dtype=jnp.int32) % HEAD_DIM
    frequency = 10000.0 ** (-2.0 * (lane % half).astype(F32) / ROT)
    angles = jnp.arange(length, dtype=F32)[:, None] * frequency[None, :]
    cosine, sine = jnp.cos(angles), jnp.sin(angles)
    cos_t = jnp.where(lane < ROT, cosine, 1.0)
    low_t = jnp.where(lane < half, -sine, 0.0)
    high_t = jnp.where((lane >= half) & (lane < ROT), sine, 0.0)
    return cos_t, low_t, high_t


def head_mask(shape, head):
    lane = lax.broadcasted_iota(jnp.int32, shape, 1)
    return (lane < HEAD_DIM) if head == 0 else (lane >= HEAD_DIM)


def roll_pair(x, shift):
    return pltpu.roll(x, shift % PAIR, 1)


def nt(a, b):
    return lax.dot_general(a, b, (((1,), (1,)), ((), ())), preferred_element_type=F32)


def nn(a, b):
    return lax.dot_general(a, b, (((1,), (0,)), ((), ())), preferred_element_type=F32)


def tn(a, b):
    return lax.dot_general(a, b, (((0,), (0,)), ((), ())), preferred_element_type=F32)


def attend_kernel(
    blk, tile, slot_ref, pq, pk, pv, bq, bk, bv, cos_t, low_t, high_t, qs, ks, vs, att, lse, acc, top, osc
):
    length = pq.shape[0]

    def sort_block(b, carry):
        src = pl.ds(pl.multiple_of(slot_ref[b] * blk, blk), blk)
        dst = pl.ds(pl.multiple_of(b * blk, blk), blk)
        c, lo, hi = cos_t[dst, :], low_t[dst, :], high_t[dst, :]
        q = pq[src, :] + bq[...]
        k = pk[src, :] + bk[...]
        q = q * c + roll_pair(q, -(ROT // 2)) * lo + roll_pair(q, ROT // 2) * hi
        k = k * c + roll_pair(k, -(ROT // 2)) * lo + roll_pair(k, ROT // 2) * hi
        qs[dst, :] = q.astype(BF16)
        ks[dst, :] = k.astype(BF16)
        vs[dst, :] = (pv[src, :] + bv[...]).astype(BF16)
        return carry

    lax.fori_loop(0, length // blk, sort_block, 0)
    rows = lax.broadcasted_iota(jnp.int32, (tile, tile), 0)
    cols = lax.broadcasted_iota(jnp.int32, (tile, tile), 1)
    masks = [head_mask((tile, PAIR), h) for h in range(2)]

    def q_step(qi, carry):
        q_at = pl.ds(pl.multiple_of(qi * tile, tile), tile)
        q = qs[q_at, :]
        acc[...] = jnp.zeros_like(acc)
        top[...] = jnp.full(top.shape, -1e30, F32)

        def one(kj, diagonal):
            k_at = pl.ds(pl.multiple_of(kj * tile, tile), tile)
            k, v = ks[k_at, :], vs[k_at, :]
            for h in range(2):
                qm = jnp.where(masks[h], q, 0).astype(BF16)
                s = nt(qm, k) * SCALE
                if diagonal:
                    s = jnp.where(cols <= rows, s, -jnp.inf)
                old = top[h]
                new = jnp.maximum(old, jnp.max(s, axis=1, keepdims=True))
                p = jnp.exp(s - new[:, :1]).astype(BF16)
                ve = jnp.where(masks[h], v, 1).astype(BF16)
                acc[h] = acc[h] * jnp.exp(old - new) + nn(p, ve)
                top[h] = new

        def k_step(kj, c):
            one(kj, False)
            return c

        lax.fori_loop(0, qi, k_step, 0)
        one(qi, True)
        a0, a1 = acc[0], acc[1]
        sum0 = roll_pair(a0, HEAD_DIM)
        sum1 = roll_pair(a1, HEAD_DIM)
        total = jnp.where(masks[0], sum0, sum1)
        mixed = jnp.where(masks[0], a0, a1) / total
        osc[q_at, :] = mixed.astype(BF16)
        lse[q_at, :] = jnp.where(masks[0], top[0], top[1]) + jnp.log(total)
        return carry

    lax.fori_loop(0, length // tile, q_step, 0)

    def place_block(b, carry):
        dst = pl.ds(pl.multiple_of(slot_ref[b] * blk, blk), blk)
        att[dst, :] = osc[pl.ds(pl.multiple_of(b * blk, blk), blk), :]
        return carry

    lax.fori_loop(0, length // blk, place_block, 0)


def attend(slot_of, proj, bias, tables, blk):
    length, width = proj.shape
    pairs = width // (3 * PAIR)
    tile = min(512, length)
    whole = lambda f: pl.BlockSpec((length, PAIR), f)
    table = pl.BlockSpec((length, PAIR), lambda p, s: (0, 0), pipeline_mode=pl.Buffered(1))
    in_specs = (
        [whole(lambda p, s, o=o: (0, o * pairs + p)) for o in range(3)]
        + [pl.BlockSpec((1, PAIR), lambda p, s, o=o: (0, o * pairs + p)) for o in range(3)]
        + [table] * 3
    )
    out = jax.ShapeDtypeStruct((length, pairs * PAIR), BF16)
    own = whole(lambda p, s: (0, p))
    return pl.pallas_call(
        functools.partial(attend_kernel, blk, tile),
        out_shape=(out, out, out, out, jax.ShapeDtypeStruct((length, pairs * PAIR), F32)),
        grid_spec=pltpu.PrefetchScalarGridSpec(
            num_scalar_prefetch=1,
            grid=(pairs,),
            in_specs=in_specs,
            out_specs=[own] * 5,
            scratch_shapes=[
                pltpu.VMEM((2, tile, PAIR), F32),
                pltpu.VMEM((2, tile, PAIR), F32),
                pltpu.VMEM((length, PAIR), BF16),
            ],
        ),
        compiler_params=pltpu.CompilerParams(vmem_limit_bytes=56 * 2**20),
        cost_estimate=cost(41, 0),
        name="attend",
    )(slot_of, proj, proj, proj, bias, bias, bias, *tables)


def attend_back_kernel(
    blk, tile, slot_ref, qs, ks, vs, att, gat, lse, cos_t, low_t, high_t, gq, gk, gv, bias, dos, dlt, dq, dk, dv
):
    length = qs.shape[0]
    bmask = head_mask((blk, PAIR), 0)

    def sort_block(b, carry):
        src = pl.ds(pl.multiple_of(slot_ref[b] * blk, blk), blk)
        dst = pl.ds(pl.multiple_of(b * blk, blk), blk)
        g = gat[src, :]
        dos[dst, :] = g
        prod = g.astype(F32) * att[src, :].astype(F32)
        d0 = jnp.sum(jnp.where(bmask, prod, 0.0), axis=1, keepdims=True)
        d1 = jnp.sum(jnp.where(bmask, 0.0, prod), axis=1, keepdims=True)
        dlt[dst, :] = jnp.where(bmask, d0, d1)
        return carry

    lax.fori_loop(0, length // blk, sort_block, 0)
    dq[...] = jnp.zeros_like(dq)
    rows = lax.broadcasted_iota(jnp.int32, (tile, tile), 0)
    cols = lax.broadcasted_iota(jnp.int32, (tile, tile), 1)
    masks = [head_mask((tile, PAIR), h) for h in range(2)]
    steps = length // tile

    def k_step(kj, carry):
        k_at = pl.ds(pl.multiple_of(kj * tile, tile), tile)
        k, v = ks[k_at, :], vs[k_at, :]
        dk[...] = jnp.zeros_like(dk)
        dv[...] = jnp.zeros_like(dv)

        def one(qi, diagonal):
            q_at = pl.ds(pl.multiple_of(qi * tile, tile), tile)
            q, do = qs[q_at, :], dos[q_at, :]
            ls, dl = lse[q_at, :], dlt[q_at, :]
            for h in range(2):
                at = h * HEAD_DIM
                qm = jnp.where(masks[h], q, 0).astype(BF16)
                dm = jnp.where(masks[h], do, 0).astype(BF16)
                km = jnp.where(masks[h], k, 0).astype(BF16)
                p = jnp.exp(nt(qm, k) * SCALE - ls[:, at : at + 1])
                if diagonal:
                    p = jnp.where(cols <= rows, p, 0.0)
                ds = (p * (nt(dm, v) - dl[:, at : at + 1])).astype(BF16)
                dv[...] += tn(p.astype(BF16), dm)
                dk[...] += tn(ds, qm)
                dq[q_at, :] += nn(ds, km)

        one(kj, True)

        def q_step(qi, c):
            one(qi, False)
            return c

        lax.fori_loop(kj + 1, steps, q_step, 0)
        for part in range(tile // blk):
            b = kj * (tile // blk) + part
            sub = pl.ds(part * blk, blk)
            pos = pl.ds(pl.multiple_of(b * blk, blk), blk)
            dst = pl.ds(pl.multiple_of(slot_ref[b] * blk, blk), blk)
            g = dk[sub, :] * SCALE
            g = g * cos_t[pos, :] - roll_pair(g, -(ROT // 2)) * low_t[pos, :] - roll_pair(g, ROT // 2) * high_t[pos, :]
            gk[dst, :] = g.astype(BF16)
            bias[1:2, :] += jnp.sum(g, axis=0, keepdims=True)
            w = dv[sub, :]
            gv[dst, :] = w.astype(BF16)
            bias[2:3, :] += jnp.sum(w, axis=0, keepdims=True)
        return carry

    bias[...] = jnp.zeros_like(bias)
    lax.fori_loop(0, steps, k_step, 0)

    def place_block(b, carry):
        pos = pl.ds(pl.multiple_of(b * blk, blk), blk)
        dst = pl.ds(pl.multiple_of(slot_ref[b] * blk, blk), blk)
        g = dq[pos, :] * SCALE
        g = g * cos_t[pos, :] - roll_pair(g, -(ROT // 2)) * low_t[pos, :] - roll_pair(g, ROT // 2) * high_t[pos, :]
        gq[dst, :] = g.astype(BF16)
        bias[0:1, :] += jnp.sum(g, axis=0, keepdims=True)
        return carry

    lax.fori_loop(0, length // blk, place_block, 0)


def attend_back(slot_of, qs, ks, vs, att, gat, lse, tables, blk):
    length, width = qs.shape
    pairs = width // PAIR
    tile = min(512, length)
    own = pl.BlockSpec((length, PAIR), lambda p, s: (0, p))
    table = pl.BlockSpec((length, PAIR), lambda p, s: (0, 0), pipeline_mode=pl.Buffered(1))
    out = jax.ShapeDtypeStruct((length, width), BF16)
    return pl.pallas_call(
        functools.partial(attend_back_kernel, blk, tile),
        out_shape=(out, out, out, jax.ShapeDtypeStruct((8, width), F32)),
        grid_spec=pltpu.PrefetchScalarGridSpec(
            num_scalar_prefetch=1,
            grid=(pairs,),
            in_specs=[own] * 6 + [table] * 3,
            out_specs=[own] * 3 + [pl.BlockSpec((8, PAIR), lambda p, s: (0, p))],
            scratch_shapes=[
                pltpu.VMEM((length, PAIR), BF16),
                pltpu.VMEM((length, PAIR), F32),
                pltpu.VMEM((length, PAIR), F32),
                pltpu.VMEM((tile, PAIR), F32),
                pltpu.VMEM((tile, PAIR), F32),
            ],
        ),
        compiler_params=pltpu.CompilerParams(vmem_limit_bytes=56 * 2**20),
        cost_estimate=cost(50, 0),
        name="attend_back",
    )(slot_of, qs, ks, vs, att, gat, lse, *tables)


HBM = pltpu.MemorySpace.HBM
MESH_ID = pl.DeviceIdType.MESH


def ring_pos(dp, n):
    odd, half = dp % 2, dp // 2
    return odd * (half + 1) + (1 - odd) * ((n - half) % n)


def ring_dp(pos, n):
    far = ((pos + n - 1) % n) // (n // 2)
    return (1 - far) * (2 * pos - 1) + far * (2 * ((n - pos) % n))


def plane_ids(n):
    dp, core = lax.axis_index("dp"), lax.axis_index("core")
    pos = ring_pos(dp, n)
    at = lambda off: ring_dp((pos + off + n) % n, n)
    return dp, core, at


def greet(ids):
    barrier = pltpu.get_barrier_semaphore()
    for where in ids:
        pl.semaphore_signal(barrier, inc=1, device_id=where, device_id_type=MESH_ID)
    pl.semaphore_wait(barrier, len(ids))


def remote(src, dst, send, recv, where):
    return pltpu.make_async_remote_copy(
        src_ref=src, dst_ref=dst, send_sem=send, recv_sem=recv, device_id=where, device_id_type=MESH_ID
    )


def col_tile(width):
    for t in (512, 384, 256, 128):
        if width % t == 0:
            return t
    return width


class Gather:
    def __init__(self, n, x_ref, buf, s_in, s_ring, r_ring, s_part, r_part, use):
        self.n, self.mid, self.x_ref, self.buf, self.s_in, self.use = n, n // 2, x_ref, buf, s_in, use
        self.s_ring, self.r_ring, self.s_part, self.r_part = s_ring, r_ring, s_part, r_part
        self.dp, self.core, self.at = plane_ids(n)
        self.ends = ({"dp": self.at(1)}, {"dp": self.at(-1)}, {"core": 1 - self.core})
        half = x_ref.shape[0] // 2
        self.parts = (pl.ds(0, half), pl.ds(half, half))

    def slot(self, off, flip):
        return 2 * self.at(off) + (self.core if flip == 0 else 1 - self.core)

    def view(self, src, part):
        return self.buf.at[src] if part is None else self.buf.at[src, part]

    def push(self, src, part, where, send, recv):
        remote(self.view(src, part), self.view(src, part), send, recv, where).start()

    def sent(self, part, send):
        remote(self.view(0, part), self.view(0, part), send, self.r_ring.at[0, 0], self.ends[0]).wait_send()

    def arrive(self, src, part, sem):
        remote(self.view(src, part), self.view(src, part), self.s_ring.at[0, 0], sem, self.ends[0]).wait_recv()

    def begin(self):
        own = self.slot(0, 0)
        load = pltpu.make_async_copy(self.x_ref, self.buf.at[own], self.s_in)
        load.start()
        greet(self.ends)
        load.wait()
        self.push(own, None, self.ends[0], self.s_ring.at[0, 0], self.r_ring.at[1, 0])
        self.push(own, None, self.ends[1], self.s_ring.at[0, 1], self.r_ring.at[1, 1])
        self.push(own, None, self.ends[2], self.s_part.at[0, 0], self.r_part.at[0, 0])

    def ring_step(self, d):
        mid = self.mid
        for side, sign in ((0, -1), (1, 1)):
            src = self.slot(sign * d, 0)
            onward, part = self.ends[side], self.parts[side]
            if d < mid:
                self.arrive(src, None, self.r_ring.at[d, side])
                whole = None if d + 1 < mid else part
                self.push(src, whole, onward, self.s_ring.at[d, side], self.r_ring.at[d + 1, side])
                self.push(src, None, self.ends[2], self.s_part.at[d, side], self.r_part.at[d, side])
            else:
                self.arrive(src, part, self.r_ring.at[mid, side])
                self.push(src, part, self.ends[2], self.s_part.at[mid, side], self.r_part.at[mid, side])

    def mate_step(self, d):
        if d == 0:
            self.arrive(self.slot(0, 1), None, self.r_part.at[0, 0])
        elif d < self.mid:
            self.arrive(self.slot(-d, 1), None, self.r_part.at[d, 0])
            self.arrive(self.slot(d, 1), None, self.r_part.at[d, 1])
        else:
            self.arrive(self.slot(d, 1), self.parts[0], self.r_part.at[d, 0])
            self.arrive(self.slot(d, 1), self.parts[1], self.r_part.at[d, 1])

    def step(self, step):
        mid, core = self.mid, self.core
        for d in range(1, mid + 1):
            first = 2 + 4 * (d - 1)

            @pl.when(step == first)
            def _():
                self.ring_step(d)

            @pl.when(step == first + (2 if d < mid else 1))
            def _():
                self.mate_step(d)

        @pl.when(step == 1)
        def _():
            self.mate_step(0)

        later = jnp.maximum(step - 2, 0)
        d = jnp.where(step < 2, 0, 1 + later // 4)
        kind = jnp.where(step < 2, step, later % 4)
        last = jnp.where(step < 2, 1, d // mid)
        flip = jnp.where(last == 1, kind, kind // 2)
        off = jnp.where(kind % 2 == 0, -d, d)
        self.use(step, 2 * self.at(off) + core + flip - 2 * core * flip)

    def end(self):
        mid = self.mid
        for d in range(mid + 1):
            for side in range(2):
                part = self.parts[side]
                if d < mid:
                    self.sent(part if d + 1 == mid and d > 0 else None, self.s_ring.at[d, side])
                if d > 0 or side == 0:
                    self.sent(part if d == mid else None, self.s_part.at[d, side])


def gather_blocks(n, x_ref, buf, s_in, s_ring, r_ring, s_part, r_part, ready, use):
    run = Gather(n, x_ref, buf, s_in, s_ring, r_ring, s_part, r_part, use)
    run.begin()
    ready()

    def body(step, carry):
        run.step(step)
        return carry

    lax.fori_loop(0, 2 * n, body, 0)
    run.end()


class Swap:
    def __init__(self, n, pairs, relay, s_src, r_relay, s_fwd, r_dst):
        self.n, self.pairs, self.relay = n, pairs, relay
        self.s_src, self.r_relay, self.s_fwd, self.r_dst = s_src, r_relay, s_fwd, r_dst
        self.dp, self.plane = lax.axis_index("dp"), lax.axis_index("pl")
        self.away = self.dp != self.plane
        half = pairs[0][0].shape[0] // 2
        self.parts = (pl.ds(0, half), pl.ds(half, half))

    def knock(self, signal):
        @pl.when(self.away)
        def _():
            signal({"dp": self.plane})
            signal({"pl": self.dp})

        @pl.when(jnp.logical_not(self.away))
        def _():
            for j in range(1, self.n):
                signal({"dp": (self.dp + j) % self.n})
                signal({"pl": (self.dp + j) % self.n})

    def knocks(self):
        return jnp.where(self.away, 2, 2 * (self.n - 1))

    def first(self, i, path):
        src = self.pairs[i][0].at[self.parts[path]]
        dst = self.relay.at[i, path, self.dp if path == 0 else self.plane]
        to = {"dp": self.plane} if path == 0 else {"pl": self.dp}
        sem = self.r_relay.at[i, path, self.dp if path == 0 else self.plane]
        return remote(src, dst, self.s_src.at[i, path], sem, to)

    def landed(self, i, path, j):
        view = self.relay.at[i, path, j]
        return remote(view, view, self.s_src.at[i, path], self.r_relay.at[i, path, j], {"dp": j})

    def second(self, i, path, j):
        dst = self.pairs[i][1].at[self.parts[path]]
        to = {"pl": j} if path == 0 else {"dp": j}
        return remote(self.relay.at[i, path, j], dst, self.s_fwd.at[i, path, j], self.r_dst.at[i, path], to)

    def own(self, i, path, out):
        view = self.relay.at[i, path, self.dp]
        if out:
            return pltpu.make_async_copy(view, self.pairs[i][1].at[self.parts[path]], self.r_dst.at[i, path])
        return pltpu.make_async_copy(self.pairs[i][0].at[self.parts[path]], view, self.s_src.at[i, path])

    def send(self, i):
        for path in range(2):

            @pl.when(self.away)
            def _():
                self.first(i, path).start()

            @pl.when(jnp.logical_not(self.away))
            def _():
                self.own(i, path, False).start()

    def pass_on(self, i):
        @pl.when(jnp.logical_not(self.away))
        def _():
            for j in range(1, self.n):
                for path in range(2):
                    src = (self.dp + j) % self.n
                    self.landed(i, path, src).wait_recv()
                    self.second(i, path, src).start()
            for path in range(2):
                self.own(i, path, False).wait()
                self.own(i, path, True).start()

    def finish(self, i):
        @pl.when(self.away)
        def _():
            for path in range(2):
                self.second(i, path, 0).wait_recv()
                self.first(i, path).wait_send()

        @pl.when(jnp.logical_not(self.away))
        def _():
            for path in range(2):
                self.own(i, path, True).wait()
                for j in range(1, self.n):
                    self.second(i, path, (self.dp + j) % self.n).wait_send()


def swap_scratch(n, count, rows, depth):
    dma = pltpu.SemaphoreType.DMA
    return [
        pltpu.VMEM((count, 2, n, rows // 2, depth), BF16),
        dma((count, 2)),
        dma((count, 2, n)),
        dma((count, 2, n)),
        dma((count, 2)),
    ]


def swap_kernel(n, count, *refs):
    run = Swap(n, list(zip(refs[:count], refs[count : 2 * count])), *refs[2 * count :])
    barrier = pltpu.get_barrier_semaphore()
    run.knock(lambda where: pl.semaphore_signal(barrier, inc=1, device_id=where, device_id_type=MESH_ID))
    pl.semaphore_wait(barrier, run.knocks())
    for i in range(count):
        run.send(i)
    for i in range(count):
        run.pass_on(i)
    for i in range(count):
        run.finish(i)


def swap_blocks(n, cid, *items):
    count = len(items)
    rows, depth = items[0].shape
    return pl.pallas_call(
        functools.partial(swap_kernel, n, count),
        out_shape=tuple(jax.ShapeDtypeStruct(a.shape, a.dtype) for a in items),
        in_specs=[pl.BlockSpec(memory_space=HBM)] * count,
        out_specs=[pl.BlockSpec(memory_space=HBM)] * count,
        scratch_shapes=swap_scratch(n, count, rows, depth),
        compiler_params=pltpu.CompilerParams(collective_id=cid, has_side_effects=True),
        cost_estimate=cost(50 * count, 0),
        name="swap_blocks",
    )(*items)


def gather_dot_kernel(
    n, trans, x_ref, w_ref, all_ref, res_ref, buf, wv, stage, s_ring, r_ring, s_part, r_part, s_in, s_out, s_res
):
    load_w = pltpu.make_async_copy(w_ref, wv, s_in.at[0])
    load_w.start()
    width = res_ref.shape[-1]
    tile = col_tile(width)

    def put(keep, where):
        return pltpu.make_async_copy(stage.at[keep], res_ref.at[where], s_res.at[keep])

    def use(step, where):
        keep = step % 2

        @pl.when(step >= 2)
        def _():
            put(keep, where).wait()

        pltpu.make_async_copy(buf.at[where], all_ref.at[where], s_out.at[step]).start()
        block = buf[where]
        for c in range(width // tile):
            cols = pl.ds(c * tile, tile)
            part = nt(block, wv[cols, :]) if trans else nn(block, wv[:, cols])
            stage[keep, :, cols] = part.astype(stage.dtype)
        put(keep, where).start()

    gather_blocks(n, x_ref, buf, s_in.at[1], s_ring, r_ring, s_part, r_part, load_w.wait, use)
    for keep in range(2):
        put(keep, 0).wait()
    for step in range(2 * n):
        pltpu.make_async_copy(buf.at[0], all_ref.at[0], s_out.at[step]).wait()


def cost(us, flops):
    return pl.CostEstimate(flops=flops, bytes_accessed=int(us * 3.4e6), transcendentals=0)


def ring_sems(n):
    dma = pltpu.SemaphoreType.DMA
    mid = n // 2
    return [dma((mid, 2)), dma((mid + 1, 2)), dma((mid + 1, 2)), dma((mid + 1, 2))]


def gather_dot(n, cid, x, w, trans, dtype):
    rows, depth = x.shape
    width = w.shape[0] if trans else w.shape[1]
    dma = pltpu.SemaphoreType.DMA
    everything, result = pl.pallas_call(
        functools.partial(gather_dot_kernel, n, trans),
        out_shape=(
            jax.ShapeDtypeStruct((2 * n, rows, depth), x.dtype),
            jax.ShapeDtypeStruct((2 * n, rows, width), dtype),
        ),
        in_specs=[pl.BlockSpec(memory_space=HBM)] * 2,
        out_specs=[pl.BlockSpec(memory_space=HBM)] * 2,
        scratch_shapes=[
            pltpu.VMEM((2 * n, rows, depth), x.dtype),
            pltpu.VMEM(w.shape, w.dtype),
            pltpu.VMEM((2, rows, width), dtype),
        ]
        + ring_sems(n)
        + [dma((2,)), dma((2 * n,)), dma((2,))],
        compiler_params=pltpu.CompilerParams(
            collective_id=cid, has_side_effects=True, vmem_limit_bytes=60 * 2**20
        ),
        cost_estimate=cost(42, 4 * n * rows * depth * width),
        name="gather_dot",
    )(x, w)
    return everything.reshape(2 * n * rows, depth), result.reshape(2 * n * rows, width)


def gather_mlp_kernel(
    n, x_ref, w_ref, c_ref, d_ref, all_ref, act_ref, gg_ref, gu_ref, buf, wv, dv, cv, stage, s_ring, r_ring, s_part, r_part, s_in, s_c, s_out, s_res
):
    load_w = pltpu.make_async_copy(w_ref, wv, s_in.at[0])
    load_d = pltpu.make_async_copy(d_ref, dv, s_in.at[2])
    load_w.start()
    load_d.start()
    outs = (act_ref, gg_ref, gu_ref)

    def put(keep, k, where):
        return pltpu.make_async_copy(stage.at[keep, k], outs[k].at[where], s_res.at[keep, k])

    def ready():
        load_w.wait()
        load_d.wait()

    def use(step, where):
        keep = step % 2
        load_c = pltpu.make_async_copy(c_ref.at[where], cv, s_c)
        load_c.start()

        @pl.when(step >= 2)
        def _():
            for k in range(3):
                put(keep, k, where).wait()

        pltpu.make_async_copy(buf.at[where], all_ref.at[where], s_out.at[step]).start()
        block = buf[where]
        gate = nn(block, wv[0])
        upper = nn(block, wv[1])
        load_c.wait()
        back = nt(cv[...], dv[...])
        sig = 1.0 / (1.0 + jnp.exp(-gate))
        swish = gate * sig
        stage[keep, 0] = (swish * upper).astype(BF16)
        stage[keep, 1] = (back * upper * sig * (1.0 + gate * (1.0 - sig))).astype(BF16)
        stage[keep, 2] = (back * swish).astype(BF16)
        for k in range(3):
            put(keep, k, where).start()

    gather_blocks(n, x_ref, buf, s_in.at[1], s_ring, r_ring, s_part, r_part, ready, use)
    for keep in range(2):
        for k in range(3):
            put(keep, k, 0).wait()
    for step in range(2 * n):
        pltpu.make_async_copy(buf.at[0], all_ref.at[0], s_out.at[step]).wait()


def gather_mlp(n, cid, x, w, cot, wd):
    rows, depth = x.shape
    units = wd.shape[0]
    dma = pltpu.SemaphoreType.DMA
    out = jax.ShapeDtypeStruct((2 * n, rows, units), BF16)
    res = pl.pallas_call(
        functools.partial(gather_mlp_kernel, n),
        out_shape=(jax.ShapeDtypeStruct((2 * n, rows, depth), x.dtype), out, out, out),
        in_specs=[pl.BlockSpec(memory_space=HBM)] * 4,
        out_specs=[pl.BlockSpec(memory_space=HBM)] * 4,
        scratch_shapes=[
            pltpu.VMEM((2 * n, rows, depth), x.dtype),
            pltpu.VMEM(w.shape, w.dtype),
            pltpu.VMEM(wd.shape, wd.dtype),
            pltpu.VMEM((rows, depth), BF16),
            pltpu.VMEM((2, 3, rows, units), BF16),
        ]
        + ring_sems(n)
        + [dma((3,)), dma, dma((2 * n,)), dma((2, 3))],
        compiler_params=pltpu.CompilerParams(
            collective_id=cid, has_side_effects=True, vmem_limit_bytes=60 * 2**20
        ),
        cost_estimate=cost(48, 12 * n * rows * depth * units),
        name="gather_mlp",
    )(x, w, cot.reshape(2 * n, rows, depth), wd)
    return [a.reshape(2 * n * rows, -1) for a in res]


def dot_scatter_kernel(
    n, count, trans, *refs
):
    a_refs, w_refs, out_ref = refs[:count], refs[count : 2 * count], refs[2 * count]
    avs, wvs = refs[2 * count + 1 : 3 * count + 1], refs[3 * count + 1 : 4 * count + 1]
    to_mate, from_mate, hop, from_ring, acc, s_a, s_w, s_part, r_part, s_ring, r_ring, s_o = refs[4 * count + 1 :]
    dp, core, at = plane_ids(n)
    rows = acc.shape[0]
    half = rows // 2
    mid = n // 2
    right, left, mate = {"dp": at(1)}, {"dp": at(-1)}, {"core": 1 - core}
    offsets = [mid]
    for d in range(mid - 1, 0, -1):
        offsets += [d, -d]
    offsets += [0]

    def offset_of(j):
        d = mid - (j + 1) // 2
        return jnp.where(j % 2 == 1, d, -d)

    loads = [pltpu.make_async_copy(w_refs[k], wvs[k], s_w.at[k]) for k in range(count)]
    for load in loads:
        load.start()

    def slot_of(step):
        j, own = step // 2, step % 2
        who = core + (1 - own) - 2 * core * (1 - own)
        return 2 * at(offset_of(j)) + who

    def load_a(step, k):
        return pltpu.make_async_copy(a_refs[k].at[slot_of(step)], avs[k].at[step], s_a.at[step, k])

    for step in range(2 * n):
        for k in range(count):
            load_a(step, k).start()
    greet((right, left, mate))
    for load in loads:
        load.wait()
    depth = out_ref.shape[-1]
    tile = col_tile(depth)
    top, low = pl.ds(0, half), pl.ds(half, half)
    waits = []

    def hand(j):
        return remote(to_mate.at[j], from_mate.at[j], s_part.at[j], r_part.at[j], mate)

    def ring(j, part, side, send, recv):
        src = hop.at[j] if part is None else hop.at[j, part]
        dst = from_ring.at[recv, side] if part is None else from_ring.at[recv, side, part]
        return remote(src, dst, s_ring.at[send, side], r_ring.at[recv, side], right if side == 0 else left)

    def body(step, carry):
        j, own = step // 2, step % 2
        for k in range(count):
            load_a(step, k).wait()

        def product(cols):
            total = None
            for k in range(count):
                block = avs[k][step]
                part = nt(block, wvs[k][cols, :]) if trans else nn(block, wvs[k][:, cols])
                total = part if total is None else total + part
            return total

        @pl.when(own == 0)
        def _():
            for c in range(depth // tile):
                cols = pl.ds(c * tile, tile)
                to_mate[j, :, cols] = product(cols).astype(BF16)
            hand(j).start()

        @pl.when(own == 1)
        def _():
            hand(j).wait_recv()
            for c in range(depth // tile):
                cols = pl.ds(c * tile, tile)
                part = product(cols) + from_mate[j, :, cols].astype(F32)
                acc[:, cols] = part
                hop[j, :, cols] = part.astype(BF16)

            @pl.when(j == 0)
            def _():
                ring(0, top, 0, 0, mid - 1).start()
                ring(0, low, 1, 0, mid - 1).start()

            for d in range(mid - 1, 0, -1):
                first = 1 + 2 * (mid - 1 - d)

                @pl.when(j == first + 1)
                def _():
                    for side in range(2):
                        k = first + side
                        if d == mid - 1:
                            part = top if side == 0 else low
                            ring(0, part, side, 0, d).wait_recv()
                            hop[k, part, :] = (
                                hop[k, part, :].astype(F32) + from_ring[d, side, part, :].astype(F32)
                            ).astype(BF16)
                        else:
                            ring(k - 2, None, side, 0, d).wait_recv()
                            hop[k] = (hop[k].astype(F32) + from_ring[d, side].astype(F32)).astype(BF16)
                        ring(k, None, side, mid - d, d - 1).start()

        return carry

    lax.fori_loop(0, 2 * n, body, 0)
    for side in range(2):
        ring(n - 2 + side - 1, None, side, mid - 1, 0).wait_recv()
    acc[...] += from_ring[0, 0].astype(F32) + from_ring[0, 1].astype(F32)
    put = pltpu.make_async_copy(acc, out_ref, s_o)
    put.start()
    for j in range(n):
        hand(j).wait_send()
    ring(0, top, 0, 0, mid - 1).wait_send()
    ring(0, low, 1, 0, mid - 1).wait_send()
    for d in range(mid - 1, 0, -1):
        for side in range(2):
            ring(1 + 2 * (mid - 1 - d) + side, None, side, mid - d, d - 1).wait_send()
    put.wait()


def dot_scatter(n, cid, terms, trans):
    depth = terms[0][1].shape[0] if trans else terms[0][1].shape[1]
    rows = terms[0][0].shape[0] // (2 * n)
    mid = n // 2
    count = len(terms)
    dma = pltpu.SemaphoreType.DMA
    lhs = [a.reshape(2 * n, rows, a.shape[1]) for a, _ in terms]
    rhs = [w for _, w in terms]
    return pl.pallas_call(
        functools.partial(dot_scatter_kernel, n, count, trans),
        out_shape=jax.ShapeDtypeStruct((rows, depth), F32),
        in_specs=[pl.BlockSpec(memory_space=HBM)] * (2 * count),
        out_specs=pl.BlockSpec(memory_space=HBM),
        scratch_shapes=[pltpu.VMEM(a.shape, BF16) for a in lhs]
        + [pltpu.VMEM(w.shape, BF16) for w in rhs]
        + [
            pltpu.VMEM((n, rows, depth), BF16),
            pltpu.VMEM((n, rows, depth), BF16),
            pltpu.VMEM((n, rows, depth), BF16),
            pltpu.VMEM((mid, 2, rows, depth), BF16),
            pltpu.VMEM((rows, depth), F32),
            dma((2 * n, count)),
            dma((count,)),
            dma((n,)),
            dma((n,)),
            dma((mid, 2)),
            dma((mid, 2)),
            dma,
        ],
        compiler_params=pltpu.CompilerParams(
            collective_id=cid, has_side_effects=True, vmem_limit_bytes=62 * 2**20
        ),
        cost_estimate=cost(45, 4 * n * rows * depth * sum(a.shape[2] for a in lhs)),
        name="dot_scatter",
    )(*lhs, *rhs)


def start_kernel(
    n, x_ref, c_ref, w_ref, small_ref, block_ref, x_out, c_out, w_out, small_out, block_out, wv, s_own, s_w, r_w, s_s, r_s, s_b, r_b, *refs
):
    dp, plane, core = (lax.axis_index(a) for a in EVERY)
    rows = w_ref.shape[0]
    width = w_ref.shape[1] // 3
    wide = width // (2 * n)
    away = dp != plane
    move = Swap(n, [(x_ref, x_out), (c_ref, c_out)], *refs)
    barrier = pltpu.get_barrier_semaphore()

    def knock(where):
        pl.semaphore_signal(barrier, inc=1, device_id=where, device_id_type=MESH_ID)

    def send_w(j, part):
        to = (dp + j) % n
        at = pl.multiple_of(part * width + to * (2 * wide) + core * wide, 128)
        dst = w_out.at[pl.ds(pl.multiple_of(dp * rows, 128), rows), pl.ds(part * wide, wide)]
        return remote(w_ref.at[:, pl.ds(at, wide)], dst, s_w.at[j, part], r_w.at[j, part], {"dp": to})

    def send_s(j):
        to = (dp + j) % n
        return remote(small_ref, small_out.at[dp], s_s.at[j], r_s.at[j], {"dp": to})

    def send_b(i, k):
        to = {"dp": (plane + i) % n, "pl": dp, "core": (core + k) % 2}
        return remote(block_ref, block_out.at[2 * plane + core], s_b.at[i, k], r_b.at[i, k], to)

    def own_w(part, back):
        at = pl.multiple_of(part * width + dp * (2 * wide) + core * wide, 128)
        src = w_ref.at[:, pl.ds(at, wide)]
        dst = w_out.at[pl.ds(pl.multiple_of(dp * rows, 128), rows), pl.ds(part * wide, wide)]
        if back:
            return pltpu.make_async_copy(wv.at[part], dst, s_own.at[part])
        return pltpu.make_async_copy(src, wv.at[part], s_own.at[part])

    own_s = pltpu.make_async_copy(small_ref, small_out.at[dp], s_own.at[3])
    own_b = pltpu.make_async_copy(block_ref, block_out.at[2 * plane + core], s_own.at[4])
    for part in range(3):
        own_w(part, False).start()
    own_s.start()
    for j in range(1, n):
        knock({"dp": (dp + n - j) % n})
    for i in range(n):
        for k in range(2):

            @pl.when(away | (i + k > 0))
            def _():
                knock({"dp": plane, "pl": (dp + n - i) % n, "core": (core + k) % 2})

    move.knock(knock)
    pl.semaphore_wait(barrier, jnp.where(away, 3 * n - 1, 3 * n - 2) + move.knocks())
    move.send(0)

    @pl.when(away)
    def _():
        send_b(0, 0).start()

    @pl.when(jnp.logical_not(away))
    def _():
        own_b.start()

    for i in range(n):
        for k in range(2):
            if i + k > 0:
                send_b(i, k).start()
    for j in range(1, n):
        send_s(j).start()
    for j in range(1, n):
        for part in range(3):
            send_w(j, part).start()
    for part in range(3):
        own_w(part, False).wait()
        own_w(part, True).start()

    move.send(1)
    move.pass_on(0)
    move.pass_on(1)

    @pl.when(jnp.logical_not(away))
    def _():
        own_b.wait()

    own_s.wait()
    for part in range(3):
        own_w(part, True).wait()
    for i in range(n):
        for k in range(2):
            if i + k > 0:
                send_b(i, k).wait()
    for j in range(1, n):
        send_s(j).wait()
        for part in range(3):
            send_w(j, part).wait()

    @pl.when(away)
    def _():
        send_b(0, 0).wait()

    move.finish(0)
    move.finish(1)


def start(n, cid, x, c, w, small, block):
    rows, wide = w.shape[0], w.shape[1] // (6 * n)
    dma = pltpu.SemaphoreType.DMA
    return pl.pallas_call(
        functools.partial(start_kernel, n),
        out_shape=(
            jax.ShapeDtypeStruct(x.shape, x.dtype),
            jax.ShapeDtypeStruct(c.shape, c.dtype),
            jax.ShapeDtypeStruct((n * rows, 3 * wide), w.dtype),
            jax.ShapeDtypeStruct((n,) + small.shape, small.dtype),
            jax.ShapeDtypeStruct((2 * n,) + block.shape, block.dtype),
        ),
        in_specs=[pl.BlockSpec(memory_space=HBM)] * 5,
        out_specs=[pl.BlockSpec(memory_space=HBM)] * 5,
        scratch_shapes=[
            pltpu.VMEM((3, rows, wide), w.dtype),
            dma((6,)),
            dma((n, 3)),
            dma((n, 3)),
            dma((n,)),
            dma((n,)),
            dma((n, 2)),
            dma((n, 2)),
        ]
        + swap_scratch(n, 2, x.shape[0], x.shape[1]),
        compiler_params=pltpu.CompilerParams(
            collective_id=cid, has_side_effects=True, vmem_limit_bytes=56 * 2**20
        ),
        cost_estimate=cost(95, 0),
        name="start",
    )(x, c, w, small, block)


class Total:
    def __init__(self, n, a_ref, o_ref, mine, others, part, sums, s_in, s_a, r_a, s_b, r_b):
        self.n, self.a_ref, self.o_ref = n, a_ref, o_ref
        self.mine, self.others, self.part, self.sums = mine, others, part, sums
        self.s_in, self.s_a, self.r_a, self.s_b, self.r_b = s_in, s_a, r_a, s_b, r_b
        self.dp, self.plane, self.core = (lax.axis_index(a) for a in EVERY)
        self.stack = [(z, k) for z in range(n) for k in range(2) if z + k > 0]

    def send_a(self, j):
        to = (self.dp + j) % self.n
        return remote(self.mine.at[to], self.others.at[j], self.s_a.at[j], self.r_a.at[j], {"dp": to})

    def send_b(self, i):
        z, k = self.stack[i]
        where = {"pl": (self.plane + z) % self.n, "core": (self.core + k) % 2}
        return remote(self.part, self.sums.at[i], self.s_b.at[i], self.r_b.at[i], where)

    def knock(self, signal):
        for j in range(1, self.n):
            signal({"dp": (self.dp + self.n - j) % self.n})
        for z, k in self.stack:
            signal({"pl": (self.plane + self.n - z) % self.n, "core": (self.core + k) % 2})

    def knocks(self):
        return 3 * self.n - 2

    def begin(self):
        load = pltpu.make_async_copy(self.a_ref, self.mine, self.s_in)
        load.start()
        load.wait()
        for j in range(1, self.n):
            self.send_a(j).start()

    def middle(self):
        value = self.mine[self.dp]
        for j in range(1, self.n):
            self.send_a(j).wait_recv()
            value = value + self.others[j]
        self.part[...] = value
        for i in range(len(self.stack)):
            self.send_b(i).start()

    def end(self):
        value = self.part[...]
        for i in range(len(self.stack)):
            self.send_b(i).wait_recv()
            value = value + self.sums[i]
        for j in range(1, self.n):
            self.send_a(j).wait_send()
        for i in range(len(self.stack)):
            self.send_b(i).wait_send()
        self.mine[0] = value
        put = pltpu.make_async_copy(self.mine.at[0], self.o_ref, self.s_in)
        put.start()
        put.wait()


def total_scratch(n, shape):
    dma = pltpu.SemaphoreType.DMA
    return [
        pltpu.VMEM((n,) + shape, F32),
        pltpu.VMEM((n,) + shape, F32),
        pltpu.VMEM(shape, F32),
        pltpu.VMEM((2 * n - 1,) + shape, F32),
        dma,
        dma((n,)),
        dma((n,)),
        dma((2 * n - 1,)),
        dma((2 * n - 1,)),
    ]


def assemble_kernel(n, parts, wide, in_ref, out_ref):
    for p in range(parts):
        for j in range(n):
            for k in range(2):
                at = ((p * n + j) * 2 + k) * wide
                piece = in_ref[k, 0, j, p] if in_ref.shape[3] == parts else in_ref[k, 0, j, 0, :, p * wide : (p + 1) * wide]
                out_ref[:, at : at + wide] = piece.astype(F32)


def assemble(n, whole, parts, wide):
    chunks, sub = whole.shape[1], whole.shape[4]
    total_cols = parts * n * 2 * wide
    return pl.pallas_call(
        functools.partial(assemble_kernel, n, parts, wide),
        grid=(chunks,),
        out_shape=jax.ShapeDtypeStruct((chunks * sub, total_cols), F32),
        in_specs=[pl.BlockSpec((2, 1) + whole.shape[2:], lambda z: (0, z, 0, 0, 0, 0))],
        out_specs=pl.BlockSpec((sub, total_cols), lambda z: (z, 0)),
        compiler_params=pltpu.CompilerParams(vmem_limit_bytes=48 * 2**20),
        cost_estimate=cost(12, 0),
        name="assemble",
    )(whole)


def split_columns_kernel(units, w_ref, o_ref):
    core = lax.axis_index("core")
    for k in range(2):

        @pl.when(core == k)
        def _():
            o_ref[0, 0] = w_ref[:, k * units : (k + 1) * units]


def split_columns(n, w):
    rows = w.shape[0]
    units = w.shape[1] // (4 * n)
    if (2 * units) % 128:
        mine = w.reshape(rows, 2, n, 2, units)
        return lax.dynamic_index_in_dim(mine, lax.axis_index("core"), 3, keepdims=False).transpose(2, 1, 0, 3)
    return pl.pallas_call(
        functools.partial(split_columns_kernel, units),
        grid=(n, 2),
        out_shape=jax.ShapeDtypeStruct((n, 2, rows, units), w.dtype),
        in_specs=[pl.BlockSpec((rows, 2 * units), lambda j, p: (0, p * n + j))],
        out_specs=pl.BlockSpec((1, 1, rows, units), lambda j, p: (j, p, 0, 0)),
        cost_estimate=cost(8, 0),
        name="split_columns",
    )(w)


class Stack:
    def __init__(self, n, count, g_ref, h_ref, gres, hres, refs):
        self.n, self.count = n, count
        self.g_ref, self.h_ref, self.gres, self.hres = g_ref, h_ref, gres, hres
        self.g, self.gin, self.h, self.hin, self.sems, self.cross, self.sides = refs
        self.dp, self.plane, self.core = (lax.axis_index(a) for a in EVERY)
        self.mate = {"core": 1 - self.core}
        self.high = self.h_ref.shape[0]
        self.wide = self.h_ref.shape[1] // count

    LOAD, SENT, CAME, OWN, ON, BACK, GIVE, GOT = range(8)

    def sem(self, kind, c, which):
        return self.sems.at[kind, c, which]

    def load(self, c, which):
        if which == 0:
            return pltpu.make_async_copy(self.g_ref.at[:, :, c], self.g.at[c], self.sem(self.LOAD, c, 0))
        src = self.h_ref.at[:, pl.ds(pl.multiple_of(c * self.wide, 128), self.wide)]
        return pltpu.make_async_copy(src, self.h.at[c], self.sem(self.LOAD, c, 1))

    def hslot(self, c, core):
        rows = pl.ds(pl.multiple_of(core * self.high, 16), self.high)
        return self.hres.at[rows, pl.ds(pl.multiple_of(c * self.wide, 128), self.wide)]

    def along(self, c, which, up):
        to = {"pl": self.plane + (1 if up else -1)}
        src, dst = (self.g, self.gin) if which == 0 else (self.h, self.hin)
        return remote(src.at[c], dst.at[c], self.sem(self.SENT, c, which), self.sem(self.CAME, c, which), to)

    def owner(self, c, j):
        to = (self.dp + j) % self.n
        src, dst = self.g.at[c, :, to], self.gres.at[self.core, c, self.dp]
        if j == 0:
            return pltpu.make_async_copy(src, dst, self.sem(self.OWN, c, 0))
        return remote(src, dst, self.cross.at[0, c, j], self.cross.at[1, c, j], {"dp": to})

    def keep(self, c):
        return pltpu.make_async_copy(self.h.at[c], self.hslot(c, self.core), self.sem(self.OWN, c, 1))

    def back(self, c, which, up, first):
        to = {"pl": self.plane + (1 if up else -1)}
        if which == 0:
            src = dst = self.gres.at[self.core, c]
        else:
            dst = self.hslot(c, self.core)
            src = self.h.at[c] if first else dst
        return remote(src, dst, self.sem(self.ON, c, which), self.sem(self.BACK, c, which), to)

    def give(self, c, which, first):
        if which == 0:
            src = dst = self.gres.at[self.core, c]
        else:
            dst = self.hslot(c, self.core)
            src = self.h.at[c] if first else dst
        return remote(src, dst, self.sem(self.GIVE, c, which), self.sem(self.GOT, c, which), self.mate)

    def begin(self, knock):
        n = self.n
        for c in range(self.count // 2):
            for chunk in (c, self.count // 2 + c):
                for which in range(2):
                    self.load(chunk, which).start()
        for j in range(1, n):
            knock({"dp": (self.dp + j) % n})
        knock(self.mate)

        @pl.when(self.plane > 0)
        def _():
            knock({"pl": self.plane - 1})

        @pl.when(self.plane < n - 1)
        def _():
            knock({"pl": self.plane + 1})

    def knocks(self):
        ends = (self.plane == 0) | (self.plane == self.n - 1)
        return jnp.where(ends, self.n + 1, self.n + 2)

    def forward(self, c, place, up):
        last = place == self.n - 1
        for which in range(2):
            self.load(c, which).wait()

        @pl.when(place > 0)
        def _():
            for which in range(2):
                self.along(c, which, up).wait_recv()
            self.g[c] = (self.g[c].astype(F32) + self.gin[c].astype(F32)).astype(BF16)
            self.h[c] = (self.h[c].astype(F32) + self.hin[c].astype(F32)).astype(BF16)

        @pl.when(jnp.logical_not(last))
        def _():
            for which in range(2):
                self.along(c, which, up).start()

        @pl.when(last)
        def _():
            for j in range(self.n):
                self.owner(c, j).start()
            self.keep(c).start()
            self.back(c, 1, not up, True).start()
            self.give(c, 1, True).start()

    def homeward(self, c, place, up):
        @pl.when(place == self.n - 1)
        def _():
            self.owner(c, 0).wait()
            for j in range(1, self.n):
                self.owner(c, j).wait_recv()
            self.back(c, 0, up, True).start()
            self.give(c, 0, True).start()

        @pl.when(place < self.n - 1)
        def _():
            for which in (1, 0):
                self.back(c, which, up, False).wait_recv()

                @pl.when(place > 0)
                def _():
                    self.back(c, which, up, False).start()

                self.give(c, which, False).start()

    def steps(self):
        return self.count // 2 + 2 * self.n - 1

    def step(self, s):
        n, half = self.n, self.count // 2
        for up in (True, False):
            place = self.plane if up else n - 1 - self.plane
            base = half if up else 0
            c = s - place

            @pl.when((c >= 0) & (c < half))
            def _():
                self.forward(base + c, place, up)

        for up in (True, False):
            place = self.plane if up else n - 1 - self.plane
            base = half if up else 0
            c = s - n - (n - 1 - place)

            @pl.when((c >= 0) & (c < half))
            def _():
                self.homeward(base + c, place, not up)

    def end(self):
        n, half = self.n, self.count // 2
        for up in (True, False):
            place = self.plane if up else n - 1 - self.plane
            base = half if up else 0

            def drain(i, carry):
                c = base + i
                for which in range(2):
                    self.give(c, which, True).wait_recv()
                    self.give(c, which, True).wait_send()

                @pl.when(place < n - 1)
                def _():
                    for which in range(2):
                        self.along(c, which, up).wait_send()

                @pl.when(place == n - 1)
                def _():
                    for j in range(1, n):
                        self.owner(c, j).wait_send()
                    self.keep(c).wait()

                @pl.when(place > 0)
                def _():
                    for which in range(2):
                        self.back(c, which, not up, False).wait_send()

                return carry

            lax.fori_loop(0, half, drain, 0)


def stack_scratch(n, count, parts, sub, wide, high, width):
    dma = pltpu.SemaphoreType.DMA
    cols = width // count
    return [
        pltpu.VMEM((count, parts, n, sub, wide), BF16),
        pltpu.VMEM((count, parts, n, sub, wide), BF16),
        pltpu.VMEM((count, high, cols), BF16),
        pltpu.VMEM((count, high, cols), BF16),
        dma((8, count, 2)),
        dma((2, count, n)),
        dma((1,)),
    ]


def finish_kernel(n, count, g_ref, h_ref, t_ref, x_ref, c_ref, gres, hres, t_out, x_out, c_out, *refs):
    run = Stack(n, count, g_ref, h_ref, gres, hres, refs[:7])
    small = Total(n, t_ref, t_out, *refs[7:16])
    move = Swap(n, [(x_ref, x_out), (c_ref, c_out)], *refs[16:])
    barrier = pltpu.get_barrier_semaphore()

    def knock(where):
        pl.semaphore_signal(barrier, inc=1, device_id=where, device_id_type=MESH_ID)

    run.begin(knock)
    small.knock(knock)
    move.knock(knock)
    pl.semaphore_wait(barrier, run.knocks() + small.knocks() + move.knocks())
    small.begin()
    move.send(0)
    move.send(1)

    def body(s, carry):
        run.step(s)

        @pl.when(s == 2)
        def _():
            small.middle()

        for i in range(2):

            @pl.when(s == 4 + 2 * i)
            def _():
                move.pass_on(i)

        return carry

    lax.fori_loop(0, run.steps(), body, 0)
    small.end()
    move.finish(0)
    move.finish(1)
    run.end()


def finish(n, cid, g, h, t, x, c):
    parts, _, rows, wide = g.shape
    high, width = h.shape
    count = width // 128
    sub = rows // count
    return pl.pallas_call(
        functools.partial(finish_kernel, n, count),
        out_shape=(
            jax.ShapeDtypeStruct((2, count, n, parts, sub, wide), BF16),
            jax.ShapeDtypeStruct((2 * high, width), BF16),
            jax.ShapeDtypeStruct(t.shape[1:], F32),
            jax.ShapeDtypeStruct(x.shape, BF16),
            jax.ShapeDtypeStruct(c.shape, BF16),
        ),
        in_specs=[pl.BlockSpec(memory_space=HBM)] * 5,
        out_specs=[pl.BlockSpec(memory_space=HBM)] * 5,
        scratch_shapes=stack_scratch(n, count, parts, sub, wide, high, width)
        + total_scratch(n, t.shape[1:])
        + swap_scratch(n, 2, x.shape[0], x.shape[1]),
        compiler_params=pltpu.CompilerParams(
            collective_id=cid, has_side_effects=True, vmem_limit_bytes=60 * 2**20
        ),
        cost_estimate=cost(200, 0),
        name="finish",
    )(g.reshape(parts, n, count, sub, wide), h, t, x, c)


def local(
    groups,
    inputs,
    block_of,
    first_gain,
    first_shift,
    w_qkv,
    qkv_bias,
    w_out,
    second_gain,
    second_shift,
    w_gateup,
    w_down,
    cotangent,
):
    n = groups
    blk = inputs.shape[2]
    slots = inputs.shape[1]
    toks = slots * blk
    width = inputs.shape[3]
    rows = w_qkv.shape[0]
    me, plane, core = (lax.axis_index(a) for a in EVERY)
    hw = width // (2 * n)
    units = w_down.shape[0] // 2
    pick = lambda a, axis, at: lax.dynamic_index_in_dim(a, at, axis, keepdims=False)

    def rows_first(g):
        return lax.psum_scatter(g.astype(BF16), "pl", scatter_dimension=0, tiled=True)

    def last(part):
        return lax.all_gather(part, ("core", "pl"), axis=0, tiled=True).astype(F32)

    def columns_first(g):
        parts, _, wide = g.shape
        g = g.reshape(parts, n, n, rows // n, wide).transpose(2, 1, 0, 3, 4)
        part = lax.psum_scatter(g, "pl", scatter_dimension=0, tiled=True)
        return part.reshape(n, parts * rows // n, wide)

    def columns_last(part, parts, wide):
        whole = lax.all_gather(part, ("core", "pl"), axis=0, tiled=True)
        whole = whole.reshape(2, n, n, -1, rows // n, part.shape[2])
        if (2 * wide) % 128 == 0:
            return assemble(n, whole, parts, wide)
        whole = whole.reshape(2, n, n, whole.shape[3], rows // n, -1, wide).transpose(1, 4, 3, 5, 2, 0, 6)
        return whole.reshape(rows, parts * n * 2 * wide).astype(F32)

    small = jnp.concatenate([first_gain, first_shift, second_gain, second_shift, qkv_bias]).reshape(-1, 128)
    ids = jnp.zeros((8, 128), jnp.int32).at[0, :slots].set(block_of.reshape(-1))
    x, cot, wq, small, ids = start(n, 0, inputs.reshape(toks, width), cotangent.reshape(toks, width), w_qkv, small, ids)
    x, w_gateup, w_out, w_down = lax.optimization_barrier((x, w_gateup, w_out, w_down))
    token_rows = x.astype(F32)
    small = small.reshape(n, -1)
    gain_one, shift_one, gain_two, shift_two = (
        small[:, k * rows : (k + 1) * rows].reshape(width) for k in range(4)
    )
    bias = small[:, 4 * rows :].reshape(3, n, 2, hw)
    bias = pick(pick(bias, 1, me), 1, core).reshape(1, 3 * hw)
    blocks = ids[:, 0, :slots].reshape(-1)
    order = jnp.arange(blocks.shape[0], dtype=jnp.int32)
    slot_of = jnp.sum(jnp.where(blocks[None, :] == order[:, None], order[None, :], 0), axis=1)

    mine = split_columns(n, w_gateup)
    wgu = jnp.zeros((2, n, rows, units), BF16)
    wgu = lax.dynamic_update_index_in_dim(wgu, pick(mine, 0, me), me, 1)
    for j in range(1, n):
        got = lax.ppermute(pick(mine, 0, (me + j) % n), "dp", [(i, (i + j) % n) for i in range(n)])
        wgu = lax.dynamic_update_index_in_dim(wgu, got, (me + n - j) % n, 1)
    wgu = wgu.reshape(2, n * rows, units)
    wo = pick(w_out.reshape(2, hw, width), 0, core)
    wd = pick(w_down.reshape(2, units, width), 0, core)
    tables = rotary_tables(blocks.shape[0] * blk)

    normed_out, normed_one, inverse_one = layer_norm(token_rows, gain_one, shift_one)
    hidden_one, proj = gather_dot(n, 1, normed_out.astype(BF16), wq, False, F32)
    proj, cot = lax.optimization_barrier((proj, cot))
    cot_all = lax.all_gather(cot, PLANE, axis=0, tiled=True)
    qs, ks, vs, att, lse = attend(slot_of, proj, bias, tables, blk)
    middle = token_rows + dot_scatter(n, 2, [(att, wo)], False)
    normed_out_two, normed_two, inverse_two = layer_norm(middle, gain_two, shift_two)
    hidden_two, act, grad_gate, grad_up = gather_mlp(n, 3, normed_out_two.astype(BF16), wgu, cot_all, wd)
    grad_down = tn(act, cot_all).astype(BF16)
    grad_gateup = jnp.stack([tn(hidden_two, grad_gate), tn(hidden_two, grad_up)]).astype(BF16)
    grad_gate, grad_up, grad_down, grad_gateup = lax.optimization_barrier((grad_gate, grad_up, grad_down, grad_gateup))
    down_part = rows_first(grad_down)
    gateup_part = columns_first(grad_gateup)
    grad_hidden_two = dot_scatter(n, 4, [(grad_gate, wgu[0]), (grad_up, wgu[1])], True)
    gain_two_term = jnp.sum(grad_hidden_two * normed_two, axis=0)
    shift_two_term = jnp.sum(grad_hidden_two, axis=0)
    grad_middle = cot.astype(F32) + norm_back(grad_hidden_two, normed_two, inverse_two, gain_two)
    grad_middle_all, grad_att = gather_dot(n, 5, grad_middle.astype(BF16), wo, True, BF16)
    gq, gk, gv, bias_terms = attend_back(slot_of, qs, ks, vs, att, grad_att, lse, tables, blk)
    grad_proj = jnp.concatenate([gq, gk, gv], axis=1)
    grad_proj, gateup_part, down_part = lax.optimization_barrier((grad_proj, gateup_part, down_part))
    gateup_part = lax.all_to_all(gateup_part, "dp", 0, 0, tiled=True)
    grad_qkv = tn(hidden_one, grad_proj).astype(BF16)
    grad_out = tn(att, grad_middle_all).astype(BF16)
    grad_hidden_one = dot_scatter(n, 6, [(grad_proj, wq)], True)
    gain_one_term = jnp.sum(grad_hidden_one * normed_one, axis=0)
    shift_one_term = jnp.sum(grad_hidden_one, axis=0)
    grad_inputs = grad_middle + norm_back(grad_hidden_one, normed_one, inverse_one, gain_one)
    grad_inputs = grad_inputs.astype(BF16)
    grad_inputs, act = lax.optimization_barrier((grad_inputs, act))
    outputs = (middle + dot_scatter(n, 8, [(act, wd)], False)).astype(BF16)

    grad_down = last(down_part)
    grad_gateup = columns_last(gateup_part, 2, units)
    bias_term = bias_terms[:3].reshape(3, 1, hw)
    at = me * 2 + core
    spots = (jnp.arange(2 * n, dtype=jnp.int32) == at)[None, :, None]
    bias_term = jnp.where(spots, bias_term, 0.0).reshape(n, -1)
    tiny = jnp.concatenate(
        [a.reshape(n, rows) for a in (gain_one_term, shift_one_term, gain_two_term, shift_two_term)] + [bias_term],
        axis=1,
    )
    grad_qkv, grad_out, tiny, outputs, grad_inputs = finish(
        n, 7, grad_qkv.reshape(1, n, rows, 3 * hw), grad_out, tiny.reshape(n, -1, 128), outputs, grad_inputs
    )
    grad_qkv = assemble(n, grad_qkv, 3, hw)
    grad_out = grad_out.astype(F32)
    grad_inputs = grad_inputs.astype(F32)
    tiny = tiny.reshape(-1)
    terms = [tiny[k * rows : (k + 1) * rows] for k in range(4)]
    return (
        outputs.reshape(inputs.shape),
        grad_inputs.reshape(inputs.shape),
        terms[0],
        terms[1],
        grad_qkv,
        tiny[4 * rows :],
        grad_out,
        terms[2],
        terms[3],
        grad_gateup,
        grad_down,
    )


def solution(mesh):
    n = mesh.shape["dp"]
    if mesh.shape["ctx"] != 2 * n:
        raise ValueError("unsupported mesh")
    grid = Mesh(mesh.devices.reshape(n, n, 2), EVERY)
    act = P("dp", ("pl", "core"), None, None)
    mat = P("dp", None)
    vec = P("dp")
    return jax.shard_map(
        functools.partial(local, n),
        mesh=grid,
        in_specs=(act, P("dp", ("pl", "core")), vec, vec, mat, vec, mat, vec, vec, mat, mat, act),
        out_specs=(act, act, vec, vec, mat, vec, mat, vec, vec, mat, mat),
        check_vma=False,
    )
```

```python
import functools

import jax
import jax.numpy as jnp
from jax import lax
from jax.experimental import pallas as pl
from jax.experimental.pallas import tpu as pltpu
from jax.sharding import Mesh
from jax.sharding import PartitionSpec as P

HEADS = 32
HEAD_DIM = 64
ROT = 16
PAIR = 2 * HEAD_DIM
SCALE = HEAD_DIM ** (-0.5)
epsilon = 1e-05
F32 = jnp.float32
BF16 = jnp.bfloat16
PLANE = ("dp", "core")
EVERY = ("dp", "pl", "core")


def layer_norm(token_rows, gain_vec, shift_vec):
    centre = jnp.mean(token_rows, axis=-1, keepdims=True)
    centred = token_rows - centre
    spread = jnp.mean(centred * centred, axis=-1, keepdims=True)
    inverse = lax.rsqrt(spread + epsilon)
    normed = centred * inverse
    return (normed * gain_vec + shift_vec, normed, inverse)


def norm_back(grad_rows, normed, inverse, gain_vec):
    scaled = grad_rows * gain_vec
    mean_plain = jnp.mean(scaled, axis=-1, keepdims=True)
    mean_cross = jnp.mean(scaled * normed, axis=-1, keepdims=True)
    return inverse * (scaled - mean_plain - normed * mean_cross)


def rotary_tables(length):
    half = ROT // 2
    lane = jnp.arange(PAIR, dtype=jnp.int32) % HEAD_DIM
    frequency = 10000.0 ** (-2.0 * (lane % half).astype(F32) / ROT)
    angles = jnp.arange(length, dtype=F32)[:, None] * frequency[None, :]
    cosine, sine = jnp.cos(angles), jnp.sin(angles)
    cos_t = jnp.where(lane < ROT, cosine, 1.0)
    low_t = jnp.where(lane < half, -sine, 0.0)
    high_t = jnp.where((lane >= half) & (lane < ROT), sine, 0.0)
    return cos_t, low_t, high_t


def head_mask(shape, head):
    lane = lax.broadcasted_iota(jnp.int32, shape, 1)
    return (lane < HEAD_DIM) if head == 0 else (lane >= HEAD_DIM)


def roll_pair(x, shift):
    return pltpu.roll(x, shift % PAIR, 1)


def nt(a, b):
    return lax.dot_general(a, b, (((1,), (1,)), ((), ())), preferred_element_type=F32)


def nn(a, b):
    return lax.dot_general(a, b, (((1,), (0,)), ((), ())), preferred_element_type=F32)


def tn(a, b):
    return lax.dot_general(a, b, (((0,), (0,)), ((), ())), preferred_element_type=F32)


def attend_back_kernel(
    blk, tile, slot_ref, qs, ks, vs, att, gat, lse, cos_t, low_t, high_t, out, bias, dos, dlt, dq, dk, dv
):
    length = qs.shape[0]
    bmask = head_mask((blk, PAIR), 0)

    def sort_block(b, carry):
        src = pl.ds(pl.multiple_of(slot_ref[b] * blk, blk), blk)
        dst = pl.ds(pl.multiple_of(b * blk, blk), blk)
        g = gat[src, :]
        dos[dst, :] = g
        prod = g.astype(F32) * att[src, :].astype(F32)
        d0 = jnp.sum(jnp.where(bmask, prod, 0.0), axis=1, keepdims=True)
        d1 = jnp.sum(jnp.where(bmask, 0.0, prod), axis=1, keepdims=True)
        dlt[dst, :] = jnp.where(bmask, d0, d1)
        return carry

    lax.fori_loop(0, length // blk, sort_block, 0)
    dq[...] = jnp.zeros_like(dq)
    rows = lax.broadcasted_iota(jnp.int32, (tile, tile), 0)
    cols = lax.broadcasted_iota(jnp.int32, (tile, tile), 1)
    masks = [head_mask((tile, PAIR), h) for h in range(2)]
    steps = length // tile

    def k_step(kj, carry):
        k_at = pl.ds(pl.multiple_of(kj * tile, tile), tile)
        k, v = ks[k_at, :], vs[k_at, :]
        dk[...] = jnp.zeros_like(dk)
        dv[...] = jnp.zeros_like(dv)

        def one(qi, diagonal):
            q_at = pl.ds(pl.multiple_of(qi * tile, tile), tile)
            q, do = qs[q_at, :], dos[q_at, :]
            ls, dl = lse[q_at, :], dlt[q_at, :]
            for h in range(2):
                at = h * HEAD_DIM
                qm = jnp.where(masks[h], q, 0).astype(BF16)
                dm = jnp.where(masks[h], do, 0).astype(BF16)
                km = jnp.where(masks[h], k, 0).astype(BF16)
                p = jnp.exp(nt(qm, k) * SCALE - ls[:, at : at + 1])
                if diagonal:
                    p = jnp.where(cols <= rows, p, 0.0)
                ds = (p * (nt(dm, v) - dl[:, at : at + 1])).astype(BF16)
                dv[...] += tn(p.astype(BF16), dm)
                dk[...] += tn(ds, qm)
                dq[q_at, :] += nn(ds, km)

        one(kj, True)

        def q_step(qi, c):
            one(qi, False)
            return c

        lax.fori_loop(kj + 1, steps, q_step, 0)
        for part in range(tile // blk):
            b = kj * (tile // blk) + part
            sub = pl.ds(part * blk, blk)
            pos = pl.ds(pl.multiple_of(b * blk, blk), blk)
            dst = pl.ds(pl.multiple_of(slot_ref[b] * blk, blk), blk)
            g = dk[sub, :] * SCALE
            g = g * cos_t[pos, :] - roll_pair(g, -(ROT // 2)) * low_t[pos, :] - roll_pair(g, ROT // 2) * high_t[pos, :]
            out[1, dst, :] = g.astype(BF16)
            bias[1:2, :] += jnp.sum(g, axis=0, keepdims=True)
            w = dv[sub, :]
            out[2, dst, :] = w.astype(BF16)
            bias[2:3, :] += jnp.sum(w, axis=0, keepdims=True)
        return carry

    bias[...] = jnp.zeros_like(bias)
    lax.fori_loop(0, steps, k_step, 0)

    def place_block(b, carry):
        pos = pl.ds(pl.multiple_of(b * blk, blk), blk)
        dst = pl.ds(pl.multiple_of(slot_ref[b] * blk, blk), blk)
        g = dq[pos, :] * SCALE
        g = g * cos_t[pos, :] - roll_pair(g, -(ROT // 2)) * low_t[pos, :] - roll_pair(g, ROT // 2) * high_t[pos, :]
        out[0, dst, :] = g.astype(BF16)
        bias[0:1, :] += jnp.sum(g, axis=0, keepdims=True)
        return carry

    lax.fori_loop(0, length // blk, place_block, 0)


def attend_back(slot_of, qs, ks, vs, att, gat, lse, tables, blk):
    length, width = qs.shape
    pairs = width // PAIR
    tile = min(512, length)
    own = pl.BlockSpec((length, PAIR), lambda p, s: (0, p))
    table = pl.BlockSpec((length, PAIR), lambda p, s: (0, 0), pipeline_mode=pl.Buffered(1))
    return pl.pallas_call(
        functools.partial(attend_back_kernel, blk, tile),
        out_shape=(jax.ShapeDtypeStruct((3, length, width), BF16), jax.ShapeDtypeStruct((8, width), F32)),
        grid_spec=pltpu.PrefetchScalarGridSpec(
            num_scalar_prefetch=1,
            grid=(pairs,),
            in_specs=[own] * 6 + [table] * 3,
            out_specs=[
                pl.BlockSpec((3, length, PAIR), lambda p, s: (0, 0, p)),
                pl.BlockSpec((8, PAIR), lambda p, s: (0, p)),
            ],
            scratch_shapes=[
                pltpu.VMEM((length, PAIR), BF16),
                pltpu.VMEM((length, PAIR), F32),
                pltpu.VMEM((length, PAIR), F32),
                pltpu.VMEM((tile, PAIR), F32),
                pltpu.VMEM((tile, PAIR), F32),
            ],
        ),
        compiler_params=pltpu.CompilerParams(vmem_limit_bytes=56 * 2**20),
        cost_estimate=cost(50, 0),
        name="attend_back",
    )(slot_of, qs, ks, vs, att, gat, lse, *tables)


HBM = pltpu.MemorySpace.HBM
MESH_ID = pl.DeviceIdType.MESH


def ring_pos(dp, n):
    odd, half = dp % 2, dp // 2
    return odd * (half + 1) + (1 - odd) * ((n - half) % n)


def ring_dp(pos, n):
    far = ((pos + n - 1) % n) // (n // 2)
    return (1 - far) * (2 * pos - 1) + far * (2 * ((n - pos) % n))


def plane_ids(n):
    dp, core = lax.axis_index("dp"), lax.axis_index("core")
    pos = ring_pos(dp, n)
    at = lambda off: ring_dp((pos + off + n) % n, n)
    return dp, core, at


def greet(ids, more=None):
    barrier = pltpu.get_barrier_semaphore()

    def knock(where):
        pl.semaphore_signal(barrier, inc=1, device_id=where, device_id_type=MESH_ID)

    for where in ids:
        knock(where)
    if more is None:
        pl.semaphore_wait(barrier, len(ids))
    else:
        more.knock(knock)
        pl.semaphore_wait(barrier, len(ids) + more.knocks())


def remote(src, dst, send, recv, where):
    return pltpu.make_async_remote_copy(
        src_ref=src, dst_ref=dst, send_sem=send, recv_sem=recv, device_id=where, device_id_type=MESH_ID
    )


def col_tile(width):
    for t in (512, 384, 256, 128):
        if width % t == 0:
            return t
    return width


class Gather:
    def __init__(self, n, x_ref, buf, s_in, s_ring, r_ring, s_part, r_part, use):
        self.n, self.mid, self.x_ref, self.buf, self.s_in, self.use = n, n // 2, x_ref, buf, s_in, use
        self.s_ring, self.r_ring, self.s_part, self.r_part = s_ring, r_ring, s_part, r_part
        self.dp, self.core, self.at = plane_ids(n)
        self.ends = ({"dp": self.at(1)}, {"dp": self.at(-1)}, {"core": 1 - self.core})
        half = x_ref.shape[0] // 2
        self.parts = (pl.ds(0, half), pl.ds(half, half))

    def slot(self, off, flip):
        return 2 * self.at(off) + (self.core if flip == 0 else 1 - self.core)

    def view(self, src, part):
        return self.buf.at[src] if part is None else self.buf.at[src, part]

    def push(self, src, part, where, send, recv):
        remote(self.view(src, part), self.view(src, part), send, recv, where).start()

    def sent(self, part, send):
        remote(self.view(0, part), self.view(0, part), send, self.r_ring.at[0, 0], self.ends[0]).wait_send()

    def arrive(self, src, part, sem):
        remote(self.view(src, part), self.view(src, part), self.s_ring.at[0, 0], sem, self.ends[0]).wait_recv()

    def begin(self, more=None):
        own = self.slot(0, 0)
        load = pltpu.make_async_copy(self.x_ref, self.buf.at[own], self.s_in)
        load.start()
        greet(self.ends, more)
        load.wait()
        self.push(own, None, self.ends[0], self.s_ring.at[0, 0], self.r_ring.at[1, 0])
        self.push(own, None, self.ends[1], self.s_ring.at[0, 1], self.r_ring.at[1, 1])
        self.push(own, None, self.ends[2], self.s_part.at[0, 0], self.r_part.at[0, 0])

    def ring_step(self, d):
        mid = self.mid
        for side, sign in ((0, -1), (1, 1)):
            src = self.slot(sign * d, 0)
            onward, part = self.ends[side], self.parts[side]
            if d < mid:
                self.arrive(src, None, self.r_ring.at[d, side])
                whole = None if d + 1 < mid else part
                self.push(src, whole, onward, self.s_ring.at[d, side], self.r_ring.at[d + 1, side])
                self.push(src, None, self.ends[2], self.s_part.at[d, side], self.r_part.at[d, side])
            else:
                self.arrive(src, part, self.r_ring.at[mid, side])
                self.push(src, part, self.ends[2], self.s_part.at[mid, side], self.r_part.at[mid, side])

    def mate_step(self, d):
        if d == 0:
            self.arrive(self.slot(0, 1), None, self.r_part.at[0, 0])
        elif d < self.mid:
            self.arrive(self.slot(-d, 1), None, self.r_part.at[d, 0])
            self.arrive(self.slot(d, 1), None, self.r_part.at[d, 1])
        else:
            self.arrive(self.slot(d, 1), self.parts[0], self.r_part.at[d, 0])
            self.arrive(self.slot(d, 1), self.parts[1], self.r_part.at[d, 1])

    def step(self, step):
        mid, core = self.mid, self.core
        for d in range(1, mid + 1):
            first = 2 + 4 * (d - 1)

            @pl.when(step == first)
            def _():
                self.ring_step(d)

            @pl.when(step == first + (2 if d < mid else 1))
            def _():
                self.mate_step(d)

        @pl.when(step == 1)
        def _():
            self.mate_step(0)

        later = jnp.maximum(step - 2, 0)
        d = jnp.where(step < 2, 0, 1 + later // 4)
        kind = jnp.where(step < 2, step, later % 4)
        last = jnp.where(step < 2, 1, d // mid)
        flip = jnp.where(last == 1, kind, kind // 2)
        off = jnp.where(kind % 2 == 0, -d, d)
        self.use(step, 2 * self.at(off) + core + flip - 2 * core * flip)

    def end(self):
        mid = self.mid
        for d in range(mid + 1):
            for side in range(2):
                part = self.parts[side]
                if d < mid:
                    self.sent(part if d + 1 == mid and d > 0 else None, self.s_ring.at[d, side])
                if d > 0 or side == 0:
                    self.sent(part if d == mid else None, self.s_part.at[d, side])


def gather_blocks(n, x_ref, buf, s_in, s_ring, r_ring, s_part, r_part, ready, use, move=None):
    run = Gather(n, x_ref, buf, s_in, s_ring, r_ring, s_part, r_part, use)
    run.begin(move)
    if move is not None:
        move.send(0)
    ready()

    def body(step, carry):
        run.step(step)
        if move is not None:

            @pl.when(step == n)
            def _():
                move.pass_on(0)

        return carry

    lax.fori_loop(0, 2 * n, body, 0)
    run.end()
    if move is not None:
        move.finish(0)


class Swap:
    def __init__(self, n, pairs, relay, s_src, r_relay, s_fwd, r_dst):
        self.n, self.pairs, self.relay = n, pairs, relay
        self.s_src, self.r_relay, self.s_fwd, self.r_dst = s_src, r_relay, s_fwd, r_dst
        self.dp, self.plane = lax.axis_index("dp"), lax.axis_index("pl")
        self.away = self.dp != self.plane
        half = pairs[0][0].shape[0] // 2
        self.parts = (pl.ds(0, half), pl.ds(half, half))

    def knock(self, signal):
        @pl.when(self.away)
        def _():
            signal({"dp": self.plane})
            signal({"pl": self.dp})

        @pl.when(jnp.logical_not(self.away))
        def _():
            for j in range(1, self.n):
                signal({"dp": (self.dp + j) % self.n})
                signal({"pl": (self.dp + j) % self.n})

    def knocks(self):
        return jnp.where(self.away, 2, 2 * (self.n - 1))

    def first(self, i, path):
        src = self.pairs[i][0].at[self.parts[path]]
        dst = self.relay.at[i, path, self.dp if path == 0 else self.plane]
        to = {"dp": self.plane} if path == 0 else {"pl": self.dp}
        sem = self.r_relay.at[i, path, self.dp if path == 0 else self.plane]
        return remote(src, dst, self.s_src.at[i, path], sem, to)

    def landed(self, i, path, j):
        view = self.relay.at[i, path, j]
        return remote(view, view, self.s_src.at[i, path], self.r_relay.at[i, path, j], {"dp": j})

    def second(self, i, path, j):
        dst = self.pairs[i][1].at[self.parts[path]]
        to = {"pl": j} if path == 0 else {"dp": j}
        return remote(self.relay.at[i, path, j], dst, self.s_fwd.at[i, path, j], self.r_dst.at[i, path], to)

    def own(self, i, path, out):
        view = self.relay.at[i, path, self.dp]
        if out:
            return pltpu.make_async_copy(view, self.pairs[i][1].at[self.parts[path]], self.r_dst.at[i, path])
        return pltpu.make_async_copy(self.pairs[i][0].at[self.parts[path]], view, self.s_src.at[i, path])

    def send(self, i):
        for path in range(2):

            @pl.when(self.away)
            def _():
                self.first(i, path).start()

            @pl.when(jnp.logical_not(self.away))
            def _():
                self.own(i, path, False).start()

    def pass_on(self, i):
        @pl.when(jnp.logical_not(self.away))
        def _():
            for j in range(1, self.n):
                for path in range(2):
                    src = (self.dp + j) % self.n
                    self.landed(i, path, src).wait_recv()
                    self.second(i, path, src).start()
            for path in range(2):
                self.own(i, path, False).wait()
                self.own(i, path, True).start()

    def finish(self, i):
        @pl.when(self.away)
        def _():
            for path in range(2):
                self.second(i, path, 0).wait_recv()
                self.first(i, path).wait_send()

        @pl.when(jnp.logical_not(self.away))
        def _():
            for path in range(2):
                self.own(i, path, True).wait()
                for j in range(1, self.n):
                    self.second(i, path, (self.dp + j) % self.n).wait_send()


def swap_scratch(n, count, rows, depth):
    dma = pltpu.SemaphoreType.DMA
    return [
        pltpu.VMEM((count, 2, n, rows // 2, depth), BF16),
        dma((count, 2)),
        dma((count, 2, n)),
        dma((count, 2, n)),
        dma((count, 2)),
    ]


def swap_kernel(n, count, *refs):
    run = Swap(n, list(zip(refs[:count], refs[count : 2 * count])), *refs[2 * count :])
    barrier = pltpu.get_barrier_semaphore()
    run.knock(lambda where: pl.semaphore_signal(barrier, inc=1, device_id=where, device_id_type=MESH_ID))
    pl.semaphore_wait(barrier, run.knocks())
    for i in range(count):
        run.send(i)
    for i in range(count):
        run.pass_on(i)
    for i in range(count):
        run.finish(i)


def swap_blocks(n, cid, *items):
    count = len(items)
    rows, depth = items[0].shape
    return pl.pallas_call(
        functools.partial(swap_kernel, n, count),
        out_shape=tuple(jax.ShapeDtypeStruct(a.shape, a.dtype) for a in items),
        in_specs=[pl.BlockSpec(memory_space=HBM)] * count,
        out_specs=[pl.BlockSpec(memory_space=HBM)] * count,
        scratch_shapes=swap_scratch(n, count, rows, depth),
        compiler_params=pltpu.CompilerParams(collective_id=cid, has_side_effects=True),
        cost_estimate=cost(50 * count, 0),
        name="swap_blocks",
    )(*items)


def gather_dot_kernel(
    n, trans, moving, *refs
):
    move = None
    if moving:
        move = Swap(n, [(refs[2], refs[5])], *refs[-5:])
        refs = refs[:2] + refs[3:5] + refs[6:-5]
    x_ref, w_ref, all_ref, res_ref, buf, wv, stage, s_ring, r_ring, s_part, r_part, s_in, s_out, s_res = refs
    load_w = pltpu.make_async_copy(w_ref, wv, s_in.at[0])
    load_w.start()
    count = res_ref.shape[0]

    def put(keep, k, where):
        return pltpu.make_async_copy(stage.at[keep, k], res_ref.at[k, where], s_res.at[keep, k])

    def use(step, where):
        keep = step % 2

        @pl.when(step >= 2)
        def _():
            for k in range(count):
                put(keep, k, where).wait()

        pltpu.make_async_copy(buf.at[where], all_ref.at[where], s_out.at[step]).start()
        block = buf[where]
        for k in range(count):
            part = nt(block, wv[k]) if trans else nn(block, wv[k])
            stage[keep, k] = part.astype(stage.dtype)
            put(keep, k, where).start()

    gather_blocks(n, x_ref, buf, s_in.at[1], s_ring, r_ring, s_part, r_part, load_w.wait, use, move)
    for keep in range(2):
        for k in range(count):
            put(keep, k, 0).wait()
    for step in range(2 * n):
        pltpu.make_async_copy(buf.at[0], all_ref.at[0], s_out.at[step]).wait()


def cost(us, flops):
    return pl.CostEstimate(flops=flops, bytes_accessed=int(us * 3.4e6), transcendentals=0)


def ring_sems(n):
    dma = pltpu.SemaphoreType.DMA
    mid = n // 2
    return [dma((mid, 2)), dma((mid + 1, 2)), dma((mid + 1, 2)), dma((mid + 1, 2))]


def gather_dot(n, cid, x, w, trans, dtype, moved=None):
    rows, depth = x.shape
    count = w.shape[0]
    width = w.shape[1] if trans else w.shape[2]
    dma = pltpu.SemaphoreType.DMA
    extra = [] if moved is None else [moved]
    everything, result, *moved = pl.pallas_call(
        functools.partial(gather_dot_kernel, n, trans, len(extra)),
        out_shape=[
            jax.ShapeDtypeStruct((2 * n, rows, depth), x.dtype),
            jax.ShapeDtypeStruct((count, 2 * n, rows, width), dtype),
        ]
        + [jax.ShapeDtypeStruct(a.shape, a.dtype) for a in extra],
        in_specs=[pl.BlockSpec(memory_space=HBM)] * (2 + len(extra)),
        out_specs=[pl.BlockSpec(memory_space=HBM)] * (2 + len(extra)),
        scratch_shapes=[
            pltpu.VMEM((2 * n, rows, depth), x.dtype),
            pltpu.VMEM(w.shape, w.dtype),
            pltpu.VMEM((2, count, rows, width), dtype),
        ]
        + ring_sems(n)
        + [dma((2,)), dma((2 * n,)), dma((2, count))]
        + [a for b in extra for a in swap_scratch(n, 1, b.shape[0], b.shape[1])],
        compiler_params=pltpu.CompilerParams(
            collective_id=cid, has_side_effects=True, vmem_limit_bytes=60 * 2**20
        ),
        cost_estimate=cost(42, 4 * n * rows * depth * width * count),
        name="gather_dot",
    )(x, w, *extra)
    out = (everything.reshape(2 * n * rows, depth), result.reshape(count, 2 * n * rows, width))
    return out + tuple(moved)


def place_rows(n, refs, wv, sem):
    dp, side = lax.axis_index("dp"), lax.axis_index("pl") % 2
    rows = refs[0].shape[1]
    half = rows // 2
    at = pl.ds(pl.multiple_of(dp * rows, 128), rows)
    copies = [pltpu.make_async_copy(refs[0], wv.at[:, at], sem.at[0])]
    for j in range(1, n):
        for other in range(2):
            first = ((dp + n - j) % n) * rows + half * (side + other - 2 * side * other)
            at = pl.ds(pl.multiple_of(first, 128), half)
            k = 2 * j - 1 + other
            copies.append(pltpu.make_async_copy(refs[k], wv.at[:, at], sem.at[k]))
    return copies


def gather_mlp_kernel(
    n, x_ref, c_ref, d_ref, *refs
):
    count = 2 * n - 1
    w_refs = refs[:count]
    all_ref, act_ref, gu_ref, buf, wv, dv, cv, act, grad = refs[count : count + 9]
    s_ring, r_ring, s_part, r_part, s_in, s_w, s_c, s_out, s_res = refs[count + 9 :]
    load_d = pltpu.make_async_copy(d_ref, dv, s_in.at[0])
    load_d.start()
    for load in place_rows(n, w_refs, wv, s_w):
        load.start()

    def put(keep, k, where):
        src, dst = (act, act_ref) if k == 0 else (grad, gu_ref)
        return pltpu.make_async_copy(src.at[keep], dst.at[where], s_res.at[keep, k])

    def ready():
        for load in place_rows(n, w_refs, wv, s_w):
            load.wait()
        load_d.wait()

    def use(step, where):
        keep = step % 2
        load_c = pltpu.make_async_copy(c_ref.at[where], cv, s_c)
        load_c.start()

        @pl.when(step >= 2)
        def _():
            for k in range(2):
                put(keep, k, where).wait()

        pltpu.make_async_copy(buf.at[where], all_ref.at[where], s_out.at[step]).start()
        both = nn(buf[where], wv[0])
        units = act.shape[-1]
        gate, upper = both[:, :units], both[:, units:]
        load_c.wait()
        back = nt(cv[...], dv[...])
        sig = 1.0 / (1.0 + jnp.exp(-gate))
        swish = gate * sig
        act[keep] = (swish * upper).astype(BF16)
        grad[keep, :, :units] = (back * upper * sig * (1.0 + gate * (1.0 - sig))).astype(BF16)
        grad[keep, :, units:] = (back * swish).astype(BF16)
        for k in range(2):
            put(keep, k, where).start()

    gather_blocks(n, x_ref, buf, s_in.at[1], s_ring, r_ring, s_part, r_part, ready, use)
    for keep in range(2):
        for k in range(2):
            put(keep, k, 0).wait()
    for step in range(2 * n):
        pltpu.make_async_copy(buf.at[0], all_ref.at[0], s_out.at[step]).wait()


def gather_mlp(n, cid, x, pieces, cot, wd):
    rows, depth = x.shape
    units = wd.shape[0]
    dma = pltpu.SemaphoreType.DMA
    everything, act, grad = pl.pallas_call(
        functools.partial(gather_mlp_kernel, n),
        out_shape=(
            jax.ShapeDtypeStruct((2 * n, rows, depth), x.dtype),
            jax.ShapeDtypeStruct((2 * n, rows, units), BF16),
            jax.ShapeDtypeStruct((2 * n, rows, 2 * units), BF16),
        ),
        in_specs=[pl.BlockSpec(memory_space=HBM)] * (3 + len(pieces)),
        out_specs=[pl.BlockSpec(memory_space=HBM)] * 3,
        scratch_shapes=[
            pltpu.VMEM((2 * n, rows, depth), x.dtype),
            pltpu.VMEM((1, depth, 2 * units), BF16),
            pltpu.VMEM(wd.shape, wd.dtype),
            pltpu.VMEM((rows, depth), BF16),
            pltpu.VMEM((2, rows, units), BF16),
            pltpu.VMEM((2, rows, 2 * units), BF16),
        ]
        + ring_sems(n)
        + [dma((2,)), dma((2 * n,)), dma, dma((2 * n,)), dma((2, 2))],
        compiler_params=pltpu.CompilerParams(
            collective_id=cid, has_side_effects=True, vmem_limit_bytes=60 * 2**20
        ),
        cost_estimate=cost(48, 12 * n * rows * depth * units),
        name="gather_mlp",
    )(x, cot.reshape(2 * n, rows, depth), wd, *pieces)
    toks = 2 * n * rows
    return everything.reshape(toks, depth), act.reshape(toks, units), grad.reshape(1, toks, 2 * units)


class Scatter:
    def __init__(self, n, trans, a_ref, loads, wv, refs):
        self.n, self.trans, self.a_ref, self.loads, self.wv = n, trans, a_ref, loads, wv
        self.av, self.hop, self.from_mate, self.from_ring, self.acc = refs[:5]
        self.s_a, self.s_part, self.r_part, self.s_ring, self.r_ring = refs[5:]
        self.dp, self.core, self.at = plane_ids(n)
        self.ends = ({"dp": self.at(1)}, {"dp": self.at(-1)})
        self.mate = {"core": 1 - self.core}
        self.mid = n // 2
        half = self.acc.shape[0] // 2
        self.parts = (pl.ds(0, half), pl.ds(half, half))

    def load_a(self, step):
        j, own = step // 2, step % 2
        d = self.mid - (j + 1) // 2
        off = jnp.where(j % 2 == 1, d, -d)
        who = self.core + (1 - own) - 2 * self.core * (1 - own)
        return pltpu.make_async_copy(self.a_ref.at[:, 2 * self.at(off) + who], self.av.at[step], self.s_a.at[step])

    def hand(self, j):
        return remote(self.hop.at[j], self.from_mate.at[j], self.s_part.at[j], self.r_part.at[j], self.mate)

    def ring(self, j, part, side, send, recv):
        src = self.hop.at[j] if part is None else self.hop.at[j, part]
        dst = self.from_ring.at[recv, side] if part is None else self.from_ring.at[recv, side, part]
        return remote(src, dst, self.s_ring.at[send, side], self.r_ring.at[recv, side], self.ends[side])

    def begin(self):
        for load in self.loads:
            load.start()
        for step in range(2 * self.n):
            self.load_a(step).start()

    def knock(self, signal):
        for where in self.ends + (self.mate,):
            signal(where)

    def ready(self):
        for load in self.loads:
            load.wait()

    def product(self, step, cols):
        total = None
        for p in range(self.av.shape[1]):
            block = self.av[step, p]
            part = nt(block, self.wv[p, cols, :]) if self.trans else nn(block, self.wv[p, :, cols])
            total = part if total is None else total + part
        return total

    def step(self, step):
        mid = self.mid
        j, own = step // 2, step % 2
        self.load_a(step).wait()
        depth = self.acc.shape[1]
        tile = col_tile(depth)

        @pl.when(own == 0)
        def _():
            for c in range(depth // tile):
                cols = pl.ds(c * tile, tile)
                self.hop[j, :, cols] = self.product(step, cols).astype(BF16)
            self.hand(j).start()

        @pl.when(own == 1)
        def _():
            self.hand(j).wait()
            for c in range(depth // tile):
                cols = pl.ds(c * tile, tile)
                part = self.product(step, cols) + self.from_mate[j, :, cols].astype(F32)
                self.acc[:, cols] = part
                self.hop[j, :, cols] = part.astype(BF16)

            @pl.when(j == 0)
            def _():
                for side in range(2):
                    self.ring(0, self.parts[side], side, 0, mid - 1).start()

            for d in range(mid - 1, 0, -1):
                first = 1 + 2 * (mid - 1 - d)

                @pl.when(j == first + 1)
                def _():
                    for side in range(2):
                        self.add(first + side, d, side)

    def add(self, k, d, side):
        if d == self.mid - 1:
            part = self.parts[side]
            self.ring(0, part, side, 0, d).wait_recv()
            both = self.hop[k, part, :].astype(F32) + self.from_ring[d, side, part, :].astype(F32)
            self.hop[k, part, :] = both.astype(BF16)
        else:
            self.ring(k - 2, None, side, 0, d).wait_recv()
            self.hop[k] = (self.hop[k].astype(F32) + self.from_ring[d, side].astype(F32)).astype(BF16)
        self.ring(k, None, side, self.mid - d, d - 1).start()

    def result(self):
        for side in range(2):
            self.ring(self.n - 3 + side, None, side, self.mid - 1, 0).wait_recv()
        self.acc[...] += self.from_ring[0, 0].astype(F32) + self.from_ring[0, 1].astype(F32)

    def end(self):
        mid = self.mid
        for side in range(2):
            self.ring(0, self.parts[side], side, 0, mid - 1).wait_send()
        for d in range(mid - 1, 0, -1):
            for side in range(2):
                self.ring(1 + 2 * (mid - 1 - d) + side, None, side, mid - d, d - 1).wait_send()


def scatter_scratch(n, parts, rows, inner, depth):
    dma = pltpu.SemaphoreType.DMA
    mid = n // 2
    return [
        pltpu.VMEM((2 * n, parts, rows, inner), BF16),
        pltpu.VMEM((n, rows, depth), BF16),
        pltpu.VMEM((n, rows, depth), BF16),
        pltpu.VMEM((mid, 2, rows, depth), BF16),
        pltpu.VMEM((rows, depth), F32),
        dma((2 * n,)),
        dma((n,)),
        dma((n,)),
        dma((mid, 2)),
        dma((mid, 2)),
    ]


def dot_scatter_kernel(n, count, trans, *refs):
    a_refs, w_refs = refs[0], refs[1 : 1 + count]
    out_ref, wv, s_w, s_o = refs[1 + count : 5 + count]
    loads = place_rows(n, w_refs, wv, s_w) if count > 1 else [pltpu.make_async_copy(w_refs[0], wv, s_w.at[0])]
    run = Scatter(n, trans, a_refs, loads, wv, refs[5 + count :])
    run.begin()
    greet(run.ends + (run.mate,))
    run.ready()

    def body(step, carry):
        run.step(step)
        return carry

    lax.fori_loop(0, 2 * n, body, 0)
    run.result()
    put = pltpu.make_async_copy(run.acc, out_ref, s_o)
    put.start()
    run.end()
    put.wait()


def dot_scatter(n, cid, a, pieces, trans):
    parts, toks, inner = a.shape
    rows = toks // (2 * n)
    count = len(pieces)
    w_rows = pieces[0].shape[1] * (n if count > 1 else 1)
    w_shape = (parts, w_rows, pieces[0].shape[2])
    depth = w_rows if trans else w_shape[2]
    dma = pltpu.SemaphoreType.DMA
    return pl.pallas_call(
        functools.partial(dot_scatter_kernel, n, count, trans),
        out_shape=jax.ShapeDtypeStruct((rows, depth), F32),
        in_specs=[pl.BlockSpec(memory_space=HBM)] * (1 + count),
        out_specs=pl.BlockSpec(memory_space=HBM),
        scratch_shapes=[pltpu.VMEM(w_shape, BF16), dma((2 * n,)), dma] + scatter_scratch(n, parts, rows, inner, depth),
        compiler_params=pltpu.CompilerParams(
            collective_id=cid, has_side_effects=True, vmem_limit_bytes=62 * 2**20
        ),
        cost_estimate=cost(45, 2 * parts * toks * inner * depth),
        name="dot_scatter",
    )(a.reshape(parts, 2 * n, rows, inner), *pieces)


def start_kernel(
    n, x_ref, w_ref, small_ref, block_ref, x_out, w_out, small_out, block_out, wv, s_own, s_w, r_w, s_s, r_s, s_b, r_b, *refs
):
    dp, plane, core = (lax.axis_index(a) for a in EVERY)
    rows = w_ref.shape[0]
    width = w_ref.shape[1] // 3
    wide = width // (2 * n)
    away = dp != plane
    move = Swap(n, [(x_ref, x_out)], *refs)
    barrier = pltpu.get_barrier_semaphore()

    def knock(where):
        pl.semaphore_signal(barrier, inc=1, device_id=where, device_id_type=MESH_ID)

    def send_w(j, part):
        to = (dp + j) % n
        at = pl.multiple_of(part * width + to * (2 * wide) + core * wide, 128)
        dst = w_out.at[part, pl.ds(pl.multiple_of(dp * rows, 128), rows)]
        return remote(w_ref.at[:, pl.ds(at, wide)], dst, s_w.at[j, part], r_w.at[j, part], {"dp": to})

    def send_s(j):
        to = (dp + j) % n
        return remote(small_ref, small_out.at[dp], s_s.at[j], r_s.at[j], {"dp": to})

    def send_b(i, k):
        to = {"dp": (plane + i) % n, "pl": dp, "core": (core + k) % 2}
        return remote(block_ref, block_out.at[2 * plane + core], s_b.at[i, k], r_b.at[i, k], to)

    def own_w(part, back):
        at = pl.multiple_of(part * width + dp * (2 * wide) + core * wide, 128)
        src = w_ref.at[:, pl.ds(at, wide)]
        dst = w_out.at[part, pl.ds(pl.multiple_of(dp * rows, 128), rows)]
        if back:
            return pltpu.make_async_copy(wv.at[part], dst, s_own.at[part])
        return pltpu.make_async_copy(src, wv.at[part], s_own.at[part])

    own_s = pltpu.make_async_copy(small_ref, small_out.at[dp], s_own.at[3])
    own_b = pltpu.make_async_copy(block_ref, block_out.at[2 * plane + core], s_own.at[4])
    for part in range(3):
        own_w(part, False).start()
    own_s.start()
    for j in range(1, n):
        knock({"dp": (dp + n - j) % n})
    for i in range(n):
        for k in range(2):

            @pl.when(away | (i + k > 0))
            def _():
                knock({"dp": plane, "pl": (dp + n - i) % n, "core": (core + k) % 2})

    move.knock(knock)
    pl.semaphore_wait(barrier, jnp.where(away, 3 * n - 1, 3 * n - 2) + move.knocks())
    move.send(0)

    @pl.when(away)
    def _():
        send_b(0, 0).start()

    @pl.when(jnp.logical_not(away))
    def _():
        own_b.start()

    for i in range(n):
        for k in range(2):
            if i + k > 0:
                send_b(i, k).start()
    for j in range(1, n):
        send_s(j).start()
    for j in range(1, n):
        for part in range(3):
            send_w(j, part).start()
    move.pass_on(0)
    for part in range(3):
        own_w(part, False).wait()
        own_w(part, True).start()


    @pl.when(jnp.logical_not(away))
    def _():
        own_b.wait()

    own_s.wait()
    for part in range(3):
        own_w(part, True).wait()
    for i in range(n):
        for k in range(2):
            if i + k > 0:
                send_b(i, k).wait()
    for j in range(1, n):
        send_s(j).wait()
        for part in range(3):
            send_w(j, part).wait()

    @pl.when(away)
    def _():
        send_b(0, 0).wait()

    move.finish(0)


def start(n, cid, x, w, small, block):
    rows, wide = w.shape[0], w.shape[1] // (6 * n)
    dma = pltpu.SemaphoreType.DMA
    return pl.pallas_call(
        functools.partial(start_kernel, n),
        out_shape=(
            jax.ShapeDtypeStruct(x.shape, x.dtype),
            jax.ShapeDtypeStruct((3, n * rows, wide), w.dtype),
            jax.ShapeDtypeStruct((n,) + small.shape, small.dtype),
            jax.ShapeDtypeStruct((2 * n,) + block.shape, block.dtype),
        ),
        in_specs=[pl.BlockSpec(memory_space=HBM)] * 4,
        out_specs=[pl.BlockSpec(memory_space=HBM)] * 4,
        scratch_shapes=[
            pltpu.VMEM((3, rows, wide), w.dtype),
            dma((6,)),
            dma((n, 3)),
            dma((n, 3)),
            dma((n,)),
            dma((n,)),
            dma((n, 2)),
            dma((n, 2)),
        ]
        + swap_scratch(n, 1, x.shape[0], x.shape[1]),
        compiler_params=pltpu.CompilerParams(
            collective_id=cid, has_side_effects=True, vmem_limit_bytes=56 * 2**20
        ),
        cost_estimate=cost(95, 0),
        name="start",
    )(x, w, small, block)


class Total:
    def __init__(self, n, a_ref, o_ref, mine, others, part, sums, s_in, s_a, r_a, s_b, r_b):
        self.n, self.a_ref, self.o_ref = n, a_ref, o_ref
        self.mine, self.others, self.part, self.sums = mine, others, part, sums
        self.s_in, self.s_a, self.r_a, self.s_b, self.r_b = s_in, s_a, r_a, s_b, r_b
        self.dp, self.plane, self.core = (lax.axis_index(a) for a in EVERY)
        self.stack = [(z, k) for z in range(n) for k in range(2) if z + k > 0]

    def send_a(self, j):
        to = (self.dp + j) % self.n
        return remote(self.mine.at[to], self.others.at[j], self.s_a.at[j], self.r_a.at[j], {"dp": to})

    def send_b(self, i):
        z, k = self.stack[i]
        where = {"pl": (self.plane + z) % self.n, "core": (self.core + k) % 2}
        return remote(self.part, self.sums.at[i], self.s_b.at[i], self.r_b.at[i], where)

    def knock(self, signal):
        for j in range(1, self.n):
            signal({"dp": (self.dp + self.n - j) % self.n})
        for z, k in self.stack:
            signal({"pl": (self.plane + self.n - z) % self.n, "core": (self.core + k) % 2})

    def knocks(self):
        return 3 * self.n - 2

    def begin(self):
        load = pltpu.make_async_copy(self.a_ref, self.mine, self.s_in)
        load.start()
        load.wait()
        for j in range(1, self.n):
            self.send_a(j).start()

    def middle(self):
        value = self.mine[self.dp]
        for j in range(1, self.n):
            self.send_a(j).wait_recv()
            value = value + self.others[j]
        self.part[...] = value
        for i in range(len(self.stack)):
            self.send_b(i).start()

    def end(self):
        value = self.part[...]
        for i in range(len(self.stack)):
            self.send_b(i).wait_recv()
            value = value + self.sums[i]
        for j in range(1, self.n):
            self.send_a(j).wait_send()
        for i in range(len(self.stack)):
            self.send_b(i).wait_send()
        self.mine[0] = value
        put = pltpu.make_async_copy(self.mine.at[0], self.o_ref, self.s_in)
        put.start()
        put.wait()


def total_scratch(n, shape):
    dma = pltpu.SemaphoreType.DMA
    return [
        pltpu.VMEM((n,) + shape, F32),
        pltpu.VMEM((n,) + shape, F32),
        pltpu.VMEM(shape, F32),
        pltpu.VMEM((2 * n - 1,) + shape, F32),
        dma,
        dma((n,)),
        dma((n,)),
        dma((2 * n - 1,)),
        dma((2 * n - 1,)),
    ]


def assemble_kernel(n, parts, wide, lead, in_ref, out_ref):
    me = lax.axis_index("dp")
    for p in range(parts):
        for j in range(n):
            for k in range(2):
                at = ((p * n + j) * 2 + k) * wide
                if lead == 0:
                    piece = in_ref[k, 0, j, p]
                else:
                    piece = in_ref[0, k, (me + n - j) % n, :, p * wide : (p + 1) * wide]
                out_ref[:, at : at + wide] = piece.astype(F32)


def assemble(n, whole, parts, wide, lead):
    chunks, sub = whole.shape[1 - lead], whole.shape[4 - lead]
    total_cols = parts * n * 2 * wide
    block = (2, 1) if lead == 0 else (1, 2)
    at = (lambda z: (0, z, 0, 0, 0, 0)) if lead == 0 else (lambda z: (z, 0, 0, 0, 0))
    return pl.pallas_call(
        functools.partial(assemble_kernel, n, parts, wide, lead),
        grid=(chunks,),
        out_shape=jax.ShapeDtypeStruct((chunks * sub, total_cols), F32),
        in_specs=[pl.BlockSpec(block + whole.shape[2:], at)],
        out_specs=pl.BlockSpec((sub, total_cols), lambda z: (z, 0)),
        compiler_params=pltpu.CompilerParams(vmem_limit_bytes=56 * 2**20),
        cost_estimate=cost(12, 0),
        name="assemble",
    )(whole)


def split_columns_kernel(units, to_ref, gate_ref, up_ref, o_ref):
    core = lax.axis_index("core")
    for k in range(2):

        @pl.when(core == k)
        def _():
            o_ref[0, :, :units] = gate_ref[:, k * units : (k + 1) * units]
            o_ref[0, :, units:] = up_ref[:, k * units : (k + 1) * units]


def split_columns(n, w, to, half=None):
    rows = w.shape[0]
    units = w.shape[1] // (4 * n)
    if (2 * units) % 128:
        mine = w.reshape(rows, 2, n, 2, units)
        mine = lax.dynamic_index_in_dim(mine, lax.axis_index("core"), 3, keepdims=False)
        mine = lax.dynamic_index_in_dim(mine, to, 2, keepdims=False).reshape(1, rows, 2 * units)
        if half is None:
            return mine
        return lax.dynamic_slice_in_dim(mine, half * (rows // 2), rows // 2, 1)
    if half is None:
        half = jnp.zeros((), jnp.int32)
    else:
        rows = rows // 2
    return pl.pallas_call(
        functools.partial(split_columns_kernel, units),
        grid_spec=pltpu.PrefetchScalarGridSpec(
            num_scalar_prefetch=1,
            grid=(1,),
            in_specs=[
                pl.BlockSpec((rows, 2 * units), lambda i, t: (t[1], t[0])),
                pl.BlockSpec((rows, 2 * units), lambda i, t: (t[1], n + t[0])),
            ],
            out_specs=pl.BlockSpec((1, rows, 2 * units), lambda i, t: (0, 0, 0)),
        ),
        out_shape=jax.ShapeDtypeStruct((1, rows, 2 * units), w.dtype),
        cost_estimate=cost(2, 0),
        name="split_columns",
    )(jnp.stack([to, half]).astype(jnp.int32), w, w)


def weight_grad_kernel(planes, h_ref, g_ref, o_ref):
    parts, _, wide = g_ref.shape
    sub = h_ref.shape[1] // planes
    for p in range(parts):
        out = tn(h_ref[...], g_ref[p]).astype(BF16)
        if planes == 1:
            o_ref[p, 0] = out
        else:
            for z in range(planes):
                o_ref[z, 0, :, p * wide : (p + 1) * wide] = out[z * sub : (z + 1) * sub]


def weight_grad(n, planes, h, g):
    parts, toks, wide = g.shape
    rows = h.shape[1] // n
    if planes == 1:
        shape, block, at = (parts, n, rows, wide), (parts, 1, rows, wide), lambda r: (0, r, 0, 0)
    else:
        sub = rows // planes
        shape, block, at = (planes, n, sub, parts * wide), (planes, 1, sub, parts * wide), lambda r: (0, r, 0, 0)
    return pl.pallas_call(
        functools.partial(weight_grad_kernel, planes),
        grid=(n,),
        in_specs=[
            pl.BlockSpec((toks, rows), lambda r: (0, r)),
            pl.BlockSpec((parts, toks, wide), lambda r: (0, 0, 0), pipeline_mode=pl.Buffered(1)),
        ],
        out_specs=pl.BlockSpec(block, at),
        out_shape=jax.ShapeDtypeStruct(shape, BF16),
        compiler_params=pltpu.CompilerParams(vmem_limit_bytes=56 * 2**20),
        cost_estimate=cost(16, 2 * parts * toks * h.shape[1] * wide),
        name="weight_grad",
    )(h, g)


class Stack:
    def __init__(self, n, count, g_ref, h_ref, gres, hres, refs):
        self.n, self.count = n, count
        self.g_ref, self.h_ref, self.gres, self.hres = g_ref, h_ref, gres, hres
        self.g, self.gin, self.h, self.hin, self.sems, self.cross, self.sides = refs
        self.dp, self.plane, self.core = (lax.axis_index(a) for a in EVERY)
        self.mate = {"core": 1 - self.core}
        self.high = self.h_ref.shape[0]
        self.wide = 2 * self.h_ref.shape[1] // count

    LOAD, SENT, CAME, OWN, ON, BACK, GIVE, GOT = range(8)

    def sem(self, kind, c, which):
        return self.sems.at[kind, c, which]

    def load(self, c, which):
        if which == 0:
            return pltpu.make_async_copy(self.g_ref.at[:, :, c], self.g.at[c], self.sem(self.LOAD, c, 0))
        src = self.h_ref.at[self.corner(c, 0)]
        return pltpu.make_async_copy(src, self.h.at[c], self.sem(self.LOAD, c, 1))

    def corner(self, c, core):
        half = self.high // 2
        first = pl.multiple_of(core * self.high + (c % 2) * half, 16)
        return pl.ds(first, half), pl.ds(pl.multiple_of((c // 2) * self.wide, 128), self.wide)

    def hslot(self, c, core):
        return self.hres.at[self.corner(c, core)]

    def along(self, c, which, up):
        to = {"pl": self.plane + (1 if up else -1)}
        src, dst = (self.g, self.gin) if which == 0 else (self.h, self.hin)
        return remote(src.at[c], dst.at[c], self.sem(self.SENT, c, which), self.sem(self.CAME, c, which), to)

    def owner(self, c, j):
        to = (self.dp + j) % self.n
        src, dst = self.g.at[c, :, to], self.gres.at[self.core, c, self.dp]
        if j == 0:
            return pltpu.make_async_copy(src, dst, self.sem(self.OWN, c, 0))
        return remote(src, dst, self.cross.at[0, c, j], self.cross.at[1, c, j], {"dp": to})

    def keep(self, c):
        return pltpu.make_async_copy(self.h.at[c], self.hslot(c, self.core), self.sem(self.OWN, c, 1))

    def back(self, c, which, up, first):
        to = {"pl": self.plane + (1 if up else -1)}
        if which == 0:
            src = dst = self.gres.at[self.core, c]
        else:
            dst = self.hslot(c, self.core)
            src = self.h.at[c] if first else dst
        return remote(src, dst, self.sem(self.ON, c, which), self.sem(self.BACK, c, which), to)

    def give(self, c, which, first):
        if which == 0:
            src = dst = self.gres.at[self.core, c]
        else:
            dst = self.hslot(c, self.core)
            src = self.h.at[c] if first else dst
        return remote(src, dst, self.sem(self.GIVE, c, which), self.sem(self.GOT, c, which), self.mate)

    def begin(self, knock):
        n = self.n
        for c in range(self.count // 2):
            for chunk in (c, self.count // 2 + c):
                for which in range(2):
                    self.load(chunk, which).start()
        for j in range(1, n):
            knock({"dp": (self.dp + j) % n})
        knock(self.mate)

        @pl.when(self.plane > 0)
        def _():
            knock({"pl": self.plane - 1})

        @pl.when(self.plane < n - 1)
        def _():
            knock({"pl": self.plane + 1})

    def knocks(self):
        ends = (self.plane == 0) | (self.plane == self.n - 1)
        return jnp.where(ends, self.n + 1, self.n + 2)

    def forward(self, c, place, up):
        last = place == self.n - 1
        for which in range(2):
            self.load(c, which).wait()

        @pl.when(place > 0)
        def _():
            for which in range(2):
                self.along(c, which, up).wait_recv()
            self.g[c] = (self.g[c].astype(F32) + self.gin[c].astype(F32)).astype(BF16)
            self.h[c] = (self.h[c].astype(F32) + self.hin[c].astype(F32)).astype(BF16)

        @pl.when(jnp.logical_not(last))
        def _():
            for which in range(2):
                self.along(c, which, up).start()

        @pl.when(last)
        def _():
            for j in range(self.n):
                self.owner(c, j).start()
            self.keep(c).start()
            self.back(c, 1, not up, True).start()
            self.give(c, 1, True).start()

    def homeward(self, c, place, up):
        @pl.when(place == self.n - 1)
        def _():
            self.owner(c, 0).wait()
            for j in range(1, self.n):
                self.owner(c, j).wait_recv()
            self.back(c, 0, up, True).start()
            self.give(c, 0, True).start()

        @pl.when(place < self.n - 1)
        def _():
            for which in (1, 0):
                self.back(c, which, up, False).wait_recv()

                @pl.when(place > 0)
                def _():
                    self.back(c, which, up, False).start()

                self.give(c, which, False).start()

    def steps(self):
        return self.count // 2 + 2 * self.n - 1

    def step(self, s):
        n, half = self.n, self.count // 2
        for up in (True, False):
            place = self.plane if up else n - 1 - self.plane
            base = half if up else 0
            c = s - place

            @pl.when((c >= 0) & (c < half))
            def _():
                self.forward(base + c, place, up)

        for up in (True, False):
            place = self.plane if up else n - 1 - self.plane
            base = half if up else 0
            c = s - n - (n - 1 - place)

            @pl.when((c >= 0) & (c < half))
            def _():
                self.homeward(base + c, place, not up)

    def end(self):
        n, half = self.n, self.count // 2
        for up in (True, False):
            place = self.plane if up else n - 1 - self.plane
            base = half if up else 0

            def drain(i, carry):
                c = base + i
                for which in range(2):
                    self.give(c, which, True).wait_recv()
                    self.give(c, which, True).wait_send()

                @pl.when(place < n - 1)
                def _():
                    for which in range(2):
                        self.along(c, which, up).wait_send()

                @pl.when(place == n - 1)
                def _():
                    for j in range(1, n):
                        self.owner(c, j).wait_send()
                    self.keep(c).wait()

                @pl.when(place > 0)
                def _():
                    for which in range(2):
                        self.back(c, which, not up, False).wait_send()

                return carry

            lax.fori_loop(0, half, drain, 0)


def stack_scratch(n, count, parts, sub, wide, high, width):
    dma = pltpu.SemaphoreType.DMA
    cols = 2 * width // count
    return [
        pltpu.VMEM((count, parts, n, sub, wide), BF16),
        pltpu.VMEM((count, parts, n, sub, wide), BF16),
        pltpu.VMEM((count, high // 2, cols), BF16),
        pltpu.VMEM((count, high // 2, cols), BF16),
        dma((8, count, 2)),
        dma((2, count, n)),
        dma((1,)),
    ]


def finish_kernel(
    n, count, g_ref, h_ref, t_ref, x_ref, a_ref, w_ref, m_ref, gres, hres, t_out, x_out, c_out, wv, base, s_own, *refs
):
    run = Stack(n, count, g_ref, h_ref, gres, hres, refs[:7])
    small = Total(n, t_ref, t_out, *refs[7:16])
    load_m = pltpu.make_async_copy(m_ref, base, s_own.at[0])
    load_m.start()
    down = Scatter(n, False, a_ref, [pltpu.make_async_copy(w_ref, wv, s_own.at[1])], wv, refs[21:])
    result = down.hop.at[n - 1]
    move = Swap(n, [(x_ref, x_out), (result, c_out)], *refs[16:21])
    down.begin()
    barrier = pltpu.get_barrier_semaphore()

    def knock(where):
        pl.semaphore_signal(barrier, inc=1, device_id=where, device_id_type=MESH_ID)

    run.begin(knock)
    small.knock(knock)
    move.knock(knock)
    down.knock(knock)
    pl.semaphore_wait(barrier, run.knocks() + small.knocks() + move.knocks() + 3)
    down.ready()
    small.begin()
    move.send(0)

    def body(s, carry):
        run.step(s)

        @pl.when(s == 2)
        def _():
            small.middle()

        @pl.when(s < 2 * n)
        def _():
            down.step(s)

        @pl.when(s == 4)
        def _():
            move.pass_on(0)

        @pl.when(s == 2 * n)
        def _():
            down.result()
            load_m.wait()
            result[...] = (base[...] + down.acc[...]).astype(BF16)
            move.send(1)

        @pl.when(s == 2 * n + 3)
        def _():
            move.pass_on(1)

        return carry

    lax.fori_loop(0, run.steps(), body, 0)
    small.end()
    move.finish(0)
    move.finish(1)
    run.end()
    down.end()


def finish(n, cid, g, h, t, x, a, w, m):
    parts, _, rows, wide = g.shape
    high, width = h.shape
    count = width // 128
    sub = rows // count
    toks, inner = a.shape
    own, depth = m.shape
    return pl.pallas_call(
        functools.partial(finish_kernel, n, count),
        out_shape=(
            jax.ShapeDtypeStruct((2, count, n, parts, sub, wide), BF16),
            jax.ShapeDtypeStruct((2 * high, width), BF16),
            jax.ShapeDtypeStruct(t.shape[1:], F32),
            jax.ShapeDtypeStruct(x.shape, BF16),
            jax.ShapeDtypeStruct(m.shape, BF16),
        ),
        in_specs=[pl.BlockSpec(memory_space=HBM)] * 7,
        out_specs=[pl.BlockSpec(memory_space=HBM)] * 5,
        scratch_shapes=[
            pltpu.VMEM((1,) + w.shape, BF16),
            pltpu.VMEM((own, depth), F32),
            pltpu.SemaphoreType.DMA((2,)),
        ]
        + stack_scratch(n, count, parts, sub, wide, high, width)
        + total_scratch(n, t.shape[1:])
        + swap_scratch(n, 2, x.shape[0], x.shape[1])
        + scatter_scratch(n, 1, own, inner, depth),
        compiler_params=pltpu.CompilerParams(
            collective_id=cid, has_side_effects=True, vmem_limit_bytes=63 * 2**20
        ),
        cost_estimate=cost(200, 0),
        name="finish",
    )(g.reshape(parts, n, count, sub, wide), h, t, x, a.reshape(1, 2 * n, own, inner), w.reshape((1,) + w.shape), m)


def attend_kernel(
    n, tile, qs, ks, vs, cot_ref, att, lse, cot_all, acc, top, buf, s_ring, r_ring, s_part, r_part, s_in, s_out
):
    length = qs.shape[0]
    pair, pairs = pl.program_id(0), pl.num_programs(0)

    def use(step, where):
        pltpu.make_async_copy(buf.at[where], cot_all.at[where], s_out.at[step]).start()

    run = Gather(n, cot_ref, buf, s_in, s_ring, r_ring, s_part, r_part, use)

    @pl.when(pair == 0)
    def _():
        run.begin()

    rows = lax.broadcasted_iota(jnp.int32, (tile, tile), 0)
    cols = lax.broadcasted_iota(jnp.int32, (tile, tile), 1)
    masks = [head_mask((tile, PAIR), h) for h in range(2)]
    steps = length // tile
    half = steps * pairs // 2

    def q_step(qi, carry):
        at = pair * steps + qi
        for when, first, count in ((half, 0, n), (half + half // 2, n, n // 2)):

            @pl.when(at == when)
            def _():
                for r in range(count):
                    run.step(first + r)

        q_at = pl.ds(pl.multiple_of(qi * tile, tile), tile)
        q = qs[q_at, :]
        acc[...] = jnp.zeros_like(acc)
        top[...] = jnp.full(top.shape, -1e30, F32)

        def one(kj, diagonal):
            k_at = pl.ds(pl.multiple_of(kj * tile, tile), tile)
            k, v = ks[k_at, :], vs[k_at, :]
            for h in range(2):
                qm = jnp.where(masks[h], q * SCALE, 0).astype(BF16)
                s = nt(qm, k)
                if diagonal:
                    s = jnp.where(cols <= rows, s, -jnp.inf)
                old = top[h]
                new = jnp.maximum(old, jnp.max(s, axis=1, keepdims=True))
                p = jnp.exp(s - new[:, :1]).astype(BF16)
                ve = jnp.where(masks[h], v, 1).astype(BF16)
                acc[h] = acc[h] * jnp.exp(old - new) + nn(p, ve)
                top[h] = new

        def k_step(kj, c):
            one(kj, False)
            return c

        lax.fori_loop(0, qi, k_step, 0)
        one(qi, True)
        a0, a1 = acc[0], acc[1]
        total = jnp.where(masks[0], roll_pair(a0, HEAD_DIM), roll_pair(a1, HEAD_DIM))
        att[q_at, :] = (jnp.where(masks[0], a0, a1) / total).astype(BF16)
        lse[q_at, :] = jnp.where(masks[0], top[0], top[1]) + jnp.log(total)
        return carry

    lax.fori_loop(0, steps, q_step, 0)

    @pl.when(pair == pairs - 1)
    def _():
        for r in range(n + n // 2, 2 * n):
            run.step(r)
        run.end()
        for step in range(2 * n):
            pltpu.make_async_copy(buf.at[0], cot_all.at[0], s_out.at[step]).wait()


def attend(n, cid, qs, ks, vs, cot):
    length, width = qs.shape
    pairs = width // PAIR
    tile = min(512, length)
    rows, depth = cot.shape
    dma = pltpu.SemaphoreType.DMA
    hbm = pl.BlockSpec(memory_space=HBM)
    own = pl.BlockSpec((length, PAIR), lambda p: (0, p))
    return pl.pallas_call(
        functools.partial(attend_kernel, n, tile),
        grid=(pairs,),
        out_shape=(
            jax.ShapeDtypeStruct((length, width), BF16),
            jax.ShapeDtypeStruct((length, width), F32),
            jax.ShapeDtypeStruct((2 * n, rows, depth), BF16),
        ),
        in_specs=[own] * 3 + [hbm],
        out_specs=[own] * 2 + [hbm],
        scratch_shapes=[
            pltpu.VMEM((2, tile, PAIR), F32),
            pltpu.VMEM((2, tile, PAIR), F32),
            pltpu.VMEM((2 * n, rows, depth), BF16),
        ]
        + ring_sems(n)
        + [dma, dma((2 * n,))],
        compiler_params=pltpu.CompilerParams(
            collective_id=cid, has_side_effects=True, vmem_limit_bytes=60 * 2**20
        ),
        cost_estimate=cost(42, 0),
        name="attend",
    )(qs, ks, vs, cot)


def prepare_kernel(blk, slot_ref, proj, bias, cos_t, low_t, high_t, qs, ks, vs):
    def sort_block(b, carry):
        src = pl.ds(pl.multiple_of(slot_ref[b] * blk, blk), blk)
        dst = pl.ds(pl.multiple_of(b * blk, blk), blk)
        c, lo, hi = cos_t[dst, :], low_t[dst, :], high_t[dst, :]
        q = proj[0, src, :] + bias[0]
        k = proj[1, src, :] + bias[1]
        q = q * c + roll_pair(q, -(ROT // 2)) * lo + roll_pair(q, ROT // 2) * hi
        k = k * c + roll_pair(k, -(ROT // 2)) * lo + roll_pair(k, ROT // 2) * hi
        qs[dst, :] = q.astype(BF16)
        ks[dst, :] = k.astype(BF16)
        vs[dst, :] = (proj[2, src, :] + bias[2]).astype(BF16)
        return carry

    lax.fori_loop(0, proj.shape[1] // blk, sort_block, 0)


def prepare(slot_of, proj, bias, tables, blk):
    _, length, width = proj.shape
    table = pl.BlockSpec((length, PAIR), lambda p, s: (0, 0), pipeline_mode=pl.Buffered(1))
    out = jax.ShapeDtypeStruct((length, width), BF16)
    return pl.pallas_call(
        functools.partial(prepare_kernel, blk),
        out_shape=(out, out, out),
        grid_spec=pltpu.PrefetchScalarGridSpec(
            num_scalar_prefetch=1,
            grid=(width // PAIR,),
            in_specs=[
                pl.BlockSpec((3, length, PAIR), lambda p, s: (0, 0, p)),
                pl.BlockSpec((3, 1, PAIR), lambda p, s: (0, 0, p)),
                table,
                table,
                table,
            ],
            out_specs=[pl.BlockSpec((length, PAIR), lambda p, s: (0, p))] * 3,
        ),
        compiler_params=pltpu.CompilerParams(vmem_limit_bytes=48 * 2**20),
        cost_estimate=cost(6, 0),
        name="prepare",
    )(slot_of, proj, bias, *tables)


def reorder_kernel(blk, from_ref, in_ref, out_ref):
    def move(j, carry):
        src = pl.ds(pl.multiple_of(from_ref[j] * blk, blk), blk)
        out_ref[pl.ds(pl.multiple_of(j * blk, blk), blk), :] = in_ref[src, :]
        return carry

    lax.fori_loop(0, in_ref.shape[0] // blk, move, 0)


def reorder(blocks, rows, blk):
    whole = pl.BlockSpec(rows.shape, lambda i, s: (0, 0))
    return pl.pallas_call(
        functools.partial(reorder_kernel, blk),
        out_shape=jax.ShapeDtypeStruct(rows.shape, rows.dtype),
        grid_spec=pltpu.PrefetchScalarGridSpec(num_scalar_prefetch=1, grid=(1,), in_specs=[whole], out_specs=whole),
        cost_estimate=cost(2, 0),
        name="reorder",
    )(blocks, rows)


def local(
    groups,
    inputs,
    block_of,
    first_gain,
    first_shift,
    w_qkv,
    qkv_bias,
    w_out,
    second_gain,
    second_shift,
    w_gateup,
    w_down,
    cotangent,
):
    n = groups
    blk = inputs.shape[2]
    slots = inputs.shape[1]
    toks = slots * blk
    width = inputs.shape[3]
    rows = w_qkv.shape[0]
    me, plane, core = (lax.axis_index(a) for a in EVERY)
    hw = width // (2 * n)
    units = w_down.shape[0] // 2
    pick = lambda a, axis, at: lax.dynamic_index_in_dim(a, at, axis, keepdims=False)

    small = jnp.concatenate([first_gain, first_shift, second_gain, second_shift, qkv_bias]).reshape(-1, 128)
    ids = jnp.zeros((8, 128), jnp.int32).at[0, :slots].set(block_of.reshape(-1))
    x, wq, small, ids = start(n, 0, inputs.reshape(toks, width), w_qkv, small, ids)
    x, w_gateup, w_out, w_down = lax.optimization_barrier((x, w_gateup, w_out, w_down))
    token_rows = x.astype(F32)
    small = small.reshape(n, -1)
    gain_one, shift_one, gain_two, shift_two = (
        small[:, k * rows : (k + 1) * rows].reshape(width) for k in range(4)
    )
    bias = small[:, 4 * rows :].reshape(3, n, 2, hw)
    bias = pick(pick(bias, 1, me), 1, core).reshape(3, 1, hw)
    blocks = ids[:, 0, :slots].reshape(-1)
    order = jnp.arange(blocks.shape[0], dtype=jnp.int32)
    slot_of = jnp.sum(jnp.where(blocks[None, :] == order[:, None], order[None, :], 0), axis=1)

    pieces = [split_columns(n, w_gateup, me)]
    side = plane % 2
    near = [
        lax.ppermute(split_columns(n, w_gateup, (me + j) % n, side), "dp", [(i, (i + j) % n) for i in range(n)])
        for j in range(1, n)
    ]
    wo = pick(w_out.reshape(2, hw, width), 0, core)
    wd = pick(w_down.reshape(2, units, width), 0, core)
    tables = rotary_tables(blocks.shape[0] * blk)

    normed_out, normed_one, inverse_one = layer_norm(token_rows, gain_one, shift_one)
    hidden_one, proj, cot = gather_dot(n, 1, normed_out.astype(BF16), wq, False, F32, cotangent.reshape(toks, width))
    proj, *near = lax.optimization_barrier((proj, *near))
    far = [lax.ppermute(a, "pl", [(i, i + 1 - 2 * (i % 2)) for i in range(n)]) for a in near]
    qs, ks, vs = prepare(slot_of, proj, bias, tables, blk)
    att, lse, cot_all = attend(n, 8, qs, ks, vs, cot)
    att = reorder(blocks, att, blk)
    cot_all = cot_all.reshape(-1, width)
    att, *far = lax.optimization_barrier((att, *far))
    for a, b in zip(near, far):
        pieces += [a, b]
    middle = token_rows + dot_scatter(n, 2, att[None], [wo[None]], False)
    normed_out_two, normed_two, inverse_two = layer_norm(middle, gain_two, shift_two)
    hidden_two, act, grad_gu = gather_mlp(n, 3, normed_out_two.astype(BF16), pieces, cot_all, wd)
    grad_gateup = weight_grad(n, n, hidden_two, grad_gu)
    grad_gu, grad_gateup = lax.optimization_barrier((grad_gu, grad_gateup))
    gateup_part = lax.psum_scatter(grad_gateup, "pl", scatter_dimension=0, tiled=True)
    grad_hidden_two = dot_scatter(n, 4, grad_gu, pieces, True)
    gain_two_term = jnp.sum(grad_hidden_two * normed_two, axis=0)
    shift_two_term = jnp.sum(grad_hidden_two, axis=0)
    grad_middle = cot.astype(F32) + norm_back(grad_hidden_two, normed_two, inverse_two, gain_two)
    grad_middle_all, grad_att = gather_dot(n, 5, grad_middle.astype(BF16), wo[None], True, BF16)
    grad_att, gateup_part = lax.optimization_barrier((grad_att, gateup_part))
    gateup_part = gateup_part.reshape(n, rows // n, 2 * units)
    shares = [pick(gateup_part, 0, me)]
    for j in range(1, n):
        share = pick(gateup_part, 0, (me + j) % n)
        shares.append(lax.ppermute(share, "dp", [(i, (i + j) % n) for i in range(n)]))
    grad_att, *shares = lax.optimization_barrier((grad_att, *shares))
    grad_proj, bias_terms = attend_back(slot_of, qs, ks, vs, att, grad_att[0], lse, tables, blk)
    grad_hidden_one = dot_scatter(n, 6, grad_proj, [wq], True)
    gain_one_term = jnp.sum(grad_hidden_one * normed_one, axis=0)
    shift_one_term = jnp.sum(grad_hidden_one, axis=0)
    grad_inputs = grad_middle + norm_back(grad_hidden_one, normed_one, inverse_one, gain_one)
    grad_inputs = grad_inputs.astype(BF16)
    whole = lax.all_gather(jnp.stack(shares), ("pl", "core"), axis=0, tiled=True)
    whole = whole.reshape(n, 2, n, rows // n, 2 * units)
    if (2 * units) % 128 == 0:
        grad_gateup = assemble(n, whole, 2, units, 1)
    else:
        whole = jnp.take(whole, (me + n - jnp.arange(n)) % n, axis=2).reshape(n, 2, n, rows // n, 2, units)
        grad_gateup = whole.transpose(0, 3, 4, 2, 1, 5).reshape(rows, -1).astype(F32)
    grad_qkv = weight_grad(n, 1, hidden_one, grad_proj)
    grad_rows = jnp.concatenate([tn(att, grad_middle_all).astype(BF16), tn(act, cot_all).astype(BF16)], axis=0)
    bias_term = bias_terms[:3].reshape(3, 1, hw)
    at = me * 2 + core
    spots = (jnp.arange(2 * n, dtype=jnp.int32) == at)[None, :, None]
    bias_term = jnp.where(spots, bias_term, 0.0).reshape(n, -1)
    tiny = jnp.concatenate(
        [a.reshape(n, rows) for a in (gain_one_term, shift_one_term, gain_two_term, shift_two_term)] + [bias_term],
        axis=1,
    )
    grad_qkv, grad_rows, tiny, grad_inputs, outputs = finish(
        n, 7, grad_qkv, grad_rows, tiny.reshape(n, -1, 128), grad_inputs, act, wd, middle
    )
    grad_qkv = assemble(n, grad_qkv, 3, hw, 0)
    grad_rows = grad_rows.reshape(2, -1, width)
    grad_out = grad_rows[:, :hw].astype(F32).reshape(-1, width)
    grad_down = grad_rows[:, hw:].astype(F32).reshape(-1, width)
    grad_inputs = grad_inputs.astype(F32)
    tiny = tiny.reshape(-1)
    terms = [tiny[k * rows : (k + 1) * rows] for k in range(4)]
    return (
        outputs.reshape(inputs.shape),
        grad_inputs.reshape(inputs.shape),
        terms[0],
        terms[1],
        grad_qkv,
        tiny[4 * rows :],
        grad_out,
        terms[2],
        terms[3],
        grad_gateup,
        grad_down,
    )


def solution(mesh):
    n = mesh.shape["dp"]
    if mesh.shape["ctx"] != 2 * n:
        raise ValueError("unsupported mesh")
    grid = Mesh(mesh.devices.reshape(n, n, 2), EVERY)
    act = P("dp", ("pl", "core"), None, None)
    mat = P("dp", None)
    vec = P("dp")
    return jax.shard_map(
        functools.partial(local, n),
        mesh=grid,
        in_specs=(act, P("dp", ("pl", "core")), vec, vec, mat, vec, mat, vec, vec, mat, mat, act),
        out_specs=(act, act, vec, vec, mat, vec, mat, vec, vec, mat, mat),
        check_vma=False,
    )
```
